32 devices in a mesh: lat: 4 (over x, core), lon: 2 (over y), lev: 4 (over z).
Axes of the slice: x: 2, y: 2, z: 4, core: 2. Of those that a mesh axis runs over, the one named last changes fastest.
Arguments:
- outer_increment: bfloat16 [16, 256, 1024], P('lev', 'lat', 'lon'), may hold values from -6 to 6
- courant: bfloat16 [3, 16, 64, 256], P(None, 'lev', 'lat', 'lon'), may hold values from -0.29882812 to 0.29882812
- obs_column: int32 [16384], P(('lat', 'lon')), may hold values from 0 to 2047
- obs_level: int32 [16384], P(('lat', 'lon')), may hold values from 0 to 15
- obs_value: float32 [16384], P(('lat', 'lon')), may hold values from -6 to 6
Outputs:
- inner_state: float32 [16, 64, 256], P('lev', 'lat', 'lon')
- adjoint: float32 [16, 64, 256], P('lev', 'lat', 'lon')
- outer_next: bfloat16 [16, 256, 1024], P('lev', 'lat', 'lon')
The draws below stay inside these ranges and needn't reach their ends.
Inputs may be any that keep to these rules, and one draw needn't show every extreme that they name: obs_column numbers a column of the 16 x 512 / 4 inner block of its latitude-longitude block, row by row.
All inputs are finite; a program needn't handle non-finite values.
Results may differ from the reference program's by a relative error of at most 0.001.
Values sent between devices are 32-bit elements; how exact they have to be, the bound alone decides.
A program may use at most 64 MiB of HBM per device.

```python
import jax
import jax.numpy as jnp

CLAT = 64
CLON = 512
OBS_COL = 2048
NLAT = 256
NLON = 1024
NLEV = 16
NOBS = 16384
N_LON = 2


def with_ends(drawn, rng, low, top_value):
    index_at = [jax.random.randint(jax.random.fold_in(rng, axis), (), 0, length) for axis, length in enumerate(drawn.shape)]
    widest = drawn.shape.index(max(drawn.shape))
    neighbour = index_at[:widest] + [(index_at[widest] + 1) % drawn.shape[widest]] + index_at[widest + 1:]
    return drawn.at[tuple(index_at)].set(low).at[tuple(neighbour)].set(top_value)


def block_levels(rng, extent, shards, smallest, high):
    gain = 1.0
    for dim, blocks in shards:
        draws = jax.random.uniform(jax.random.fold_in(jax.random.fold_in(rng, 6), dim), (blocks,), jnp.float32, smallest / len(shards), high / len(shards))
        gain = gain * jnp.repeat(jnp.exp(draws), extent[dim] // blocks).reshape((-1,) + (1,) * (len(extent) - 1 - dim))
    return gain


def noise(rng, shape, scale, limit, pieces=(), kind=jnp.bfloat16):
    entries = jax.random.normal(rng, shape, jnp.float32) * scale
    if len(pieces) > 0:
        entries = block_levels(rng, shape, pieces, -0.22, 0.18) * entries
    return jnp.clip(entries, min=-limit, max=limit).astype(kind)


def setup_inputs(seed: int = 0) -> dict:
    keys = jax.random.split(jax.random.key(seed), 6)
    outer_increment = noise(keys[0], (NLEV, NLAT, NLON), 1.0, 6.0, ((0, 4), (1, 4), (2, 2)))
    courant = jnp.clip(jax.random.uniform(keys[1], (3, NLEV, NLAT // 4, NLON // 4), jnp.float32, -0.29882812, 0.29882812) * block_levels(keys[1], (3, NLEV, NLAT // 4, NLON // 4), ((1, 4), (2, 4), (3, 2)), -0.4, 0.0), -0.29882812, 0.29882812).astype(jnp.bfloat16)
    obs_column = with_ends(jax.random.randint(keys[2], (NOBS,), 0, CLAT * CLON // 16), jax.random.fold_in(keys[2], 1), 0, (CLAT * CLON // 16) - 1).astype(jnp.int32)
    obs_level = with_ends(jax.random.randint(keys[3], (NOBS,), 0, NLEV), jax.random.fold_in(keys[3], 1), 0, NLEV - 1).astype(jnp.int32)
    obs_value = noise(keys[4], (NOBS,), 1.0, 6.0, ((0, 8),), jnp.float32)
    return {"outer_increment": outer_increment, "courant": courant, "obs_column": obs_column, "obs_level": obs_level, "obs_value": obs_value}


def extend(field):
    wrapped = jnp.pad(field, ((0, 0), (0, 0), (0, 0), (1, 1)), mode="wrap")
    return jnp.pad(wrapped, ((0, 0), (1, 1), (1, 1), (0, 0)))


def window_of(field, axis, shift):
    sizes = [field.shape[1] - 2, field.shape[2] - 2, field.shape[3] - 2]
    begins = [1, 1, 1]
    begins[axis - 1] = begins[axis - 1] + shift
    return field[:, begins[0]:begins[0] + sizes[0], begins[1]:begins[1] + sizes[1], begins[2]:begins[2] + sizes[2]]


def forward(state, rims_courant):
    numbers = window_of(rims_courant, 1, 0)
    result = (1.0 - jnp.sum(jnp.abs(numbers), axis=0, keepdims=True)) * state
    padded = extend(state)
    for direction in range(3):
        lower = jnp.maximum(numbers[direction:direction + 1], 0.0)
        upper = jnp.maximum(-numbers[direction:direction + 1], 0.0)
        result = result + lower * window_of(padded, direction + 1, -1) + upper * window_of(padded, direction + 1, 1)
    return result


def backward(adjoint, rims_courant):
    numbers = window_of(rims_courant, 1, 0)
    result = (1.0 - jnp.sum(jnp.abs(numbers), axis=0, keepdims=True)) * adjoint
    padded = extend(adjoint)
    for direction in range(3):
        lower = jnp.maximum(rims_courant[direction:direction + 1], 0.0)
        upper = jnp.maximum(-rims_courant[direction:direction + 1], 0.0)
        result = result + window_of(lower * padded, direction + 1, 1) + window_of(upper * padded, direction + 1, -1)
    return result


def reference(outer_increment, courant, obs_column, obs_level, obs_value):
    levels, rows, columns = outer_increment.shape
    inner_rows = rows // 4
    inner_cols = columns // 4
    blocked = outer_increment.reshape(levels, inner_rows, 4, inner_cols, 4)
    coarse = jnp.mean(blocked, axis=(2, 4), dtype=jnp.float32).astype(jnp.float32)
    rims_courant = extend(courant.astype(jnp.float32))
    state = coarse[None]
    for turn in range(2):
        state = forward(state, rims_courant)
    block_rows = CLAT // 4
    block_cols = CLON // 4
    blocks = jnp.arange(obs_column.shape[0], dtype=jnp.int32) // OBS_COL
    row_index = (blocks // N_LON) * block_rows + obs_column // block_cols
    col_index = (blocks % N_LON) * block_cols + obs_column % block_cols
    flat = ((obs_level * inner_rows + row_index) * inner_cols + col_index).astype(jnp.int32)
    innovation = state.reshape(-1)[flat] - obs_value
    forcing = jnp.zeros((levels * inner_rows * inner_cols,), jnp.float32).at[flat].add(innovation)
    adjoint = forcing.reshape(1, levels, inner_rows, inner_cols)
    for turn in range(2):
        adjoint = backward(adjoint, rims_courant)
    spread = jnp.broadcast_to(adjoint[0][:, :, None, :, None], (levels, inner_rows, 4, inner_cols, 4)).reshape(levels, rows, columns)
    outer_next = (outer_increment.astype(jnp.float32) - spread).astype(jnp.bfloat16)
    return state[0], adjoint[0], outer_next
```

```python
import functools

import jax
import jax.numpy as jnp
from jax import lax
from jax.experimental import pallas as pl
from jax.experimental.pallas import tpu as pltpu
from jax.sharding import PartitionSpec as P

MESH = pl.DeviceIdType.MESH
ROUNDS = 3


def bf16_parts(x, count):
    parts = []
    for _ in range(count):
        part = x.astype(jnp.bfloat16).astype(jnp.float32)
        parts.append(part)
        x = x - part
    return parts


def kernel(
    ends, outer_hbm, courant_hbm, col_hbm, lvl_hbm, val_hbm,
    state_v, adj_v, outer,
    courant, col, lvl, val, sums,
    lev_out, lat_out, lon_out, lev_in, lat_in, lon_in,
    lev2_out, lat2_out, edge_out, pack_out, lev2_in, lat2_in, edge_in, pack_in,
    units, in_sem, send_sem, recv_sem,
):
    n_lat, n_lon, n_lev = ends
    levels, rows, cols = state_v.shape
    flat_rows = levels * rows
    wide_cols = outer.shape[1]
    fine = wide_cols // cols

    loads = [
        pltpu.make_async_copy(src, dst, in_sem.at[i])
        for i, (src, dst) in enumerate(
            ((outer_hbm, outer), (courant_hbm, courant), (col_hbm, col), (lvl_hbm, lvl), (val_hbm, val))
        )
    ]
    for load in loads:
        load.start()

    me_lat, me_lon, me_lev = (lax.axis_index(a) for a in ("lat", "lon", "lev"))
    links = (
        ("lev", me_lev + 1, me_lev < n_lev - 1),
        ("lev", me_lev - 1, me_lev > 0),
        ("lat", me_lat + 1, me_lat < n_lat - 1),
        ("lat", me_lat - 1, me_lat > 0),
        ("lon", lax.rem(me_lon + 1, n_lon), None),
        ("lon", lax.rem(me_lon + n_lon - 1, n_lon), None),
    )
    side_lev = (links[0], links[1])
    side_lat = (links[2], links[3])
    side_lon = (links[4], links[5])

    def joined(*sides):
        exists = [e for _, _, e in sides if e is not None]
        target = {axis: who for axis, who, _ in sides}
        return target, functools.reduce(jnp.logical_and, exists) if exists else None

    wide_links = []

    def add(sides, opposite, source, landing):
        target, exists = joined(*sides)
        needs = tuple(w for w in range(4) if any(links[w] is side for side in sides))
        wide_links.append((target, exists, joined(*opposite)[1], source, landing, needs))

    for s in range(2):
        add([side_lev[s]], [side_lev[1 - s]], lambda q, s=s: lev2_out.at[q, s], lambda q, s=s: lev2_in.at[q, s])
        add([side_lat[s]], [side_lat[1 - s]], lambda q, s=s: lat2_out.at[q, s], lambda q, s=s: lat2_in.at[q, s])
    for s in range(2):
        for t in range(2):
            add([side_lev[s], side_lat[t]], [side_lev[1 - s], side_lat[1 - t]],
                lambda q, e=2 * s + t: edge_out.at[q, e], lambda q, e=2 * s + t: edge_in.at[q, e])
    faces_end = len(wide_links)
    for u in range(2):
        add([side_lon[u]], [side_lon[1 - u]], lambda q: pack_out.at[q], lambda q, e=u: pack_in.at[q, e])
    for base, sides in ((2, side_lev), (6, side_lat)):
        for s in range(2):
            for u in range(2):
                add([sides[s], side_lon[u]], [sides[1 - s], side_lon[1 - u]],
                    lambda q: pack_out.at[q], lambda q, e=base + 2 * s + u: pack_in.at[q, e])
    outs = {"lev": lev_out, "lat": lat_out, "lon": lon_out}
    ins = {"lev": lev_in, "lat": lat_in, "lon": lon_in}

    def guarded(exists, action):
        if exists is None:
            action()
        else:
            pl.when(exists)(action)

    barrier = pltpu.get_barrier_semaphore()
    for target, exists, _, _, _, _ in wide_links:
        guarded(
            exists,
            lambda target=target: pl.semaphore_signal(
                barrier, inc=1, device_id=target, device_id_type=MESH
            ),
        )

    def wide_message(q, i):
        target, _, _, source, landing, _ = wide_links[i]
        return pltpu.make_async_remote_copy(
            src_ref=source(q),
            dst_ref=landing(q),
            send_sem=send_sem,
            recv_sem=recv_sem.at[q],
            device_id=target,
            device_id_type=MESH,
        )

    def clear(landing):
        for q in range(2):
            ref = landing(q)
            ref[...] = jnp.zeros(ref.shape, jnp.float32)

    for _, _, arrives, _, landing, _ in wide_links:
        if arrives is not None:
            pl.when(jnp.logical_not(arrives))(lambda landing=landing: clear(landing))

    def message(turn, which):
        axis, who, _ = links[which]
        side = which % 2
        source = outs[axis].at[turn] if axis == "lon" else outs[axis].at[turn, side]
        return pltpu.make_async_remote_copy(
            src_ref=source,
            dst_ref=ins[axis].at[turn, side],
            send_sem=send_sem,
            recv_sem=recv_sem.at[0],
            device_id={axis: who},
            device_id_type=MESH,
        )

    def blank(ref, side):
        for turn in range(ROUNDS):
            ref[turn, side] = jnp.zeros(ref.shape[2:], jnp.float32)

    pl.when(me_lev == 0)(lambda: blank(lev_in, 0))
    pl.when(me_lev == n_lev - 1)(lambda: blank(lev_in, 1))
    pl.when(me_lat == 0)(lambda: blank(lat_in, 0))
    pl.when(me_lat == n_lat - 1)(lambda: blank(lat_in, 1))

    lane = lax.broadcasted_iota(jnp.int32, (flat_rows, cols), 1)
    flat = lax.broadcasted_iota(jnp.int32, (flat_rows, cols), 0)
    lane3 = lax.broadcasted_iota(jnp.int32, (levels, rows, cols), 2)
    row3 = lax.broadcasted_iota(jnp.int32, (levels, rows, cols), 1)

    pool = (
        lax.broadcasted_iota(jnp.int32, (wide_cols, cols), 0) // fine
        == lax.broadcasted_iota(jnp.int32, (wide_cols, cols), 1)
    ).astype(jnp.float32).astype(jnp.bfloat16)

    def pack(first, last):
        first = first.reshape(flat_rows, cols)[:, :1]
        last = last.reshape(flat_rows, cols)[:, cols - 1 :]
        spread = jnp.where(lane == flat, first, 0.0) + jnp.where(lane == flat + flat_rows, last, 0.0)
        return jnp.sum(spread, axis=0, keepdims=True)

    def column(row, begin, step, length):
        at = lax.broadcasted_iota(jnp.int32, (length, cols), 1)
        index = lax.broadcasted_iota(jnp.int32, (length, cols), 0)
        return jnp.sum(jnp.where(at == begin + step * index, row, 0.0), axis=1, keepdims=True)

    def either(from_previous, from_next):
        at = lax.broadcasted_iota(jnp.int32, from_next.shape, 1)
        return jnp.where(at < flat_rows, from_next, from_previous)

    def ends_of(row):
        return [column(row, b, 1, flat_rows).reshape(levels, rows, 1) for b in (flat_rows, 0)]

    def shifted(firsts, lasts, lev, lat, lon):
        below = [
            jnp.concatenate([lev[0][None], lasts[0][: levels - 1]], axis=0),
            jnp.where(row3 == 0, lat[0][:, None, :], pltpu.roll(lasts[1], 1, axis=1)),
            jnp.where(lane3 == 0, lon[0], pltpu.roll(lasts[2], 1, axis=2)),
        ]
        above = [
            jnp.concatenate([firsts[0][1:], lev[1][None]], axis=0),
            jnp.where(row3 == rows - 1, lat[1][:, None, :], pltpu.roll(firsts[1], rows - 1, axis=1)),
            jnp.where(lane3 == cols - 1, lon[1], pltpu.roll(firsts[2], cols - 1, axis=2)),
        ]
        return below, above

    def send(turn, firsts, lasts):
        lev_out[turn, 0] = lasts[0][levels - 1]
        lev_out[turn, 1] = firsts[0][0]
        lat_out[turn, 0] = lasts[1][:, rows - 1, :]
        lat_out[turn, 1] = firsts[1][:, 0, :]
        for which in range(4):
            guarded(links[which][2], lambda which=which: message(turn, which).start())
        lon_out[turn] = pack(firsts[2], lasts[2])
        for which in (4, 5):
            message(turn, which).start()

    def received(turn):
        return (
            [lev_in[turn, 0], lev_in[turn, 1]],
            [lat_in[turn, 0], lat_in[turn, 1]],
            either(lon_in[turn, 0], lon_in[turn, 1]),
        )

    expected = sum(1 if link[1] is None else link[1].astype(jnp.int32) for link in wide_links)
    loads[1].wait()
    numbers = courant[...].astype(jnp.float32)
    lower = [jnp.maximum(numbers[k], 0.0) for k in range(3)]
    upper = [jnp.maximum(-numbers[k], 0.0) for k in range(3)]
    centre = 1.0 - jnp.abs(numbers[0]) - jnp.abs(numbers[1]) - jnp.abs(numbers[2])

    loads[0].wait()
    sums[...] = jnp.dot(outer[...], pool, preferred_element_type=jnp.float32)
    coarse = sums[pl.ds(0, flat_rows, stride=fine), :]
    for k in range(1, fine):
        coarse = coarse + sums[pl.ds(k, flat_rows, stride=fine), :]
    coarse = (coarse * (1.0 / (fine * fine))).reshape(levels, rows, cols)

    lev3 = lax.broadcasted_iota(jnp.int32, (levels, rows, cols), 0)
    last_lev, last_row = levels - 1, rows - 1
    lev_edge = (last_lev, 0)
    row_edge = (last_row, 0)
    none_lev = jnp.zeros((rows, cols), jnp.float32)
    none_lat = jnp.zeros((levels, cols), jnp.float32)

    def step(values, lev, lat, lon):
        below, above = shifted([values] * 3, [values] * 3, lev, lat, lon)
        result = centre * values
        for k in range(3):
            result = result + lower[k] * below[k] + upper[k] * above[k]
        return result

    partial = step(coarse, [none_lev] * 2, [none_lat] * 2, [0.0, 0.0])
    pl.semaphore_wait(barrier, expected)
    for s in range(2):
        lev2_out[0, s, 0] = partial[lev_edge[s]]
        lev2_out[0, s, 1] = coarse[lev_edge[s]]
        lat2_out[0, s, 0] = partial[:, row_edge[s], :]
        lat2_out[0, s, 1] = coarse[:, row_edge[s], :]
        for t in range(2):
            for i in range(2):
                edge_out[0, 2 * s + t, i : i + 1] = coarse[lev_edge[s], row_edge[t] : row_edge[t] + 1, :]
    for i in range(faces_end):
        guarded(wide_links[i][1], lambda i=i: wide_message(0, i).start())
    own_pack = pack(coarse, coarse)
    pack_out[0, 0:1] = pack(partial, partial)
    pack_out[0, 1:2] = own_pack
    pack_out[0, 2:3] = own_pack
    pack_out[0, 3:4] = own_pack
    for i in range(faces_end, len(wide_links)):
        guarded(wide_links[i][1], lambda i=i: wide_message(0, i).start())

    for k in range(3):
        send(k, [numbers[k]] * 3, [numbers[k]] * 3)

    for load in loads[2:]:
        load.wait()
    where_row = (lvl[...] - me_lev * levels) * rows + col[...] // cols
    where_col = col[...] % cols
    parts = bf16_parts(val[...], 3)
    pieces, width = col.shape
    row_id = lax.broadcasted_iota(jnp.int32, (flat_rows, width), 0)
    col_id = lax.broadcasted_iota(jnp.int32, (cols, width), 0)
    hits = [[] for _ in range(4)]
    tables = []
    for k in range(pieces):
        match = where_row[k : k + 1] == row_id
        hits[0].append(jnp.where(match, 1.0, 0.0).astype(jnp.bfloat16))
        for i, part in enumerate(parts):
            hits[i + 1].append(jnp.where(match, part[k : k + 1], 0.0).astype(jnp.bfloat16))
        tables.append(jnp.where(where_col[k : k + 1] == col_id, 1.0, 0.0).astype(jnp.bfloat16))
    left_side = jnp.concatenate([jnp.concatenate(h, axis=1) for h in hits], axis=0)
    totals = lax.dot_general(
        left_side, jnp.concatenate(tables, axis=1), (((1,), (1,)), ((), ())),
        preferred_element_type=jnp.float32,
    )
    count = totals[:flat_rows].reshape(levels, rows, cols)
    observed = (
        totals[flat_rows : 2 * flat_rows]
        + totals[2 * flat_rows : 3 * flat_rows]
        + totals[3 * flat_rows :]
    ).reshape(levels, rows, cols)

    plane_row = lax.broadcasted_iota(jnp.int32, (rows, cols), 0)
    plane_lane = lax.broadcasted_iota(jnp.int32, (rows, cols), 1)
    line_lev = lax.broadcasted_iota(jnp.int32, (levels, cols), 0)
    line_lane = lax.broadcasted_iota(jnp.int32, (levels, cols), 1)
    at_lane = lax.broadcasted_iota(jnp.int32, (1, cols), 1)
    at = lax.rem(at_lane, flat_rows)
    at_lev, at_row = lax.div(at, rows), lax.rem(at, rows)

    def packs(q):
        return (
            either(pack_in[q, 0], pack_in[q, 1]),
            [either(pack_in[q, 2 + 2 * s], pack_in[q, 3 + 2 * s]) for s in range(2)],
            [either(pack_in[q, 6 + 2 * s], pack_in[q, 7 + 2 * s]) for s in range(2)],
        )


    def low(x):
        return jnp.maximum(x, 0.0)

    def up(x):
        return jnp.maximum(-x, 0.0)

    def lines(ref):
        total = 1
        for n in ref.shape:
            total = total * n
        return total // cols

    def settle(groups, sem, known=()):
        if len(known) < 4:
            for has in (True, False):
                flag = links[len(known)][2]
                pl.when(flag if has else jnp.logical_not(flag))(
                    lambda has=has: settle(groups, sem, known + (has,))
                )
            return
        total = sum(amount for needs, amount in groups if all(known[w] for w in needs))
        view = units.at[pl.ds(0, total)]
        pltpu.make_async_copy(view, view, sem).wait()

    def narrow_lines(flip):
        sizes = {"lev": rows, "lat": levels, "lon": 1}
        return [((w ^ flip,) if w < 4 else (), ROUNDS * sizes[links[w][0]]) for w in range(6)]

    def wide_lines(q, flip):
        return [(tuple(w ^ flip for w in link[5]), lines(link[4](q))) for link in wide_links]

    settle(narrow_lines(1) + wide_lines(0, 1), recv_sem.at[0])
    speeds = [received(k) for k in range(3)]
    side_pack, lev_pack, lat_pack = packs(0)
    beside_lev, beside_lat = [], []
    for s in range(2):
        near, far = (up, low) if s == 0 else (low, up)
        c = [speeds[k][0][s] for k in range(3)]
        plane = lev2_in[0, s, 0] + near(c[0]) * coarse[(0, last_lev)[s]]
        plane = plane + jnp.where(plane_row == 0, low(c[1]) * edge_in[0, 2 * s, 0:1], 0.0)
        plane = plane + jnp.where(plane_row == last_row, up(c[1]) * edge_in[0, 2 * s + 1, 0:1], 0.0)
        begin = lev_edge[s] * rows
        moved = lev_pack[s][1:2]
        plane = plane + jnp.where(plane_lane == 0, low(c[2]) * column(moved, flat_rows + begin, 1, rows), 0.0)
        plane = plane + jnp.where(plane_lane == cols - 1, up(c[2]) * column(moved, begin, 1, rows), 0.0)
        beside_lev.append(plane)

        c = [speeds[k][1][s] for k in range(3)]
        plane = lat2_in[0, s, 0] + near(c[1]) * coarse[:, (0, last_row)[s], :]
        plane = plane + jnp.where(line_lev == 0, low(c[0]) * edge_in[0, s, 1:2], 0.0)
        plane = plane + jnp.where(line_lev == last_lev, up(c[0]) * edge_in[0, 2 + s, 1:2], 0.0)
        begin = row_edge[s]
        moved = lat_pack[s][1:2]
        plane = plane + jnp.where(
            line_lane == 0, low(c[2]) * column(moved, flat_rows + begin, rows, levels), 0.0
        )
        plane = plane + jnp.where(line_lane == cols - 1, up(c[2]) * column(moved, begin, rows, levels), 0.0)
        beside_lat.append(plane)
    c = [speeds[k][2] for k in range(3)]
    ring = side_pack[0:1] + jnp.where(at_lane < flat_rows, low(c[2]), up(c[2])) * pltpu.roll(
        own_pack, flat_rows, axis=1
    )
    turned = [pltpu.roll(lev_pack[0][1:2], cols - last_lev * rows, axis=1), pltpu.roll(lev_pack[1][1:2], last_lev * rows, axis=1)]
    ring = ring + jnp.where(at_lev == 0, low(c[0]) * turned[0], 0.0)
    ring = ring + jnp.where(at_lev == last_lev, up(c[0]) * turned[1], 0.0)
    turned = [pltpu.roll(lat_pack[0][1:2], cols - last_row, axis=1), pltpu.roll(lat_pack[1][1:2], last_row, axis=1)]
    ring = ring + jnp.where(at_row == 0, low(c[1]) * turned[0], 0.0)
    ring = ring + jnp.where(at_row == last_row, up(c[1]) * turned[1], 0.0)

    state = step(
        coarse, [lev2_in[0, s, 1] for s in range(2)], [lat2_in[0, s, 1] for s in range(2)],
        ends_of(side_pack[1:2]),
    )
    state = step(state, beside_lev, beside_lat, ends_of(ring))
    field = count * state - observed

    state_v[...] = state
    to_first = [lower[k] * field for k in range(3)]
    to_last = [upper[k] * field for k in range(3)]
    below, above = shifted(to_first, to_last, [none_lev] * 2, [none_lat] * 2, [0.0, 0.0])
    partial = centre * field
    for k in range(3):
        partial = partial + above[k] + below[k]

    last_lev, last_row = levels - 1, rows - 1
    lev_edge = (last_lev, 0)
    row_edge = (last_row, 0)
    for s in range(2):
        lev_move = (to_last, to_first)[s]
        lev2_out[1, s, 0] = partial[lev_edge[s]]
        lev2_out[1, s, 1] = lev_move[0][lev_edge[s]]
        lat2_out[1, s, 0] = partial[:, row_edge[s], :]
        lat2_out[1, s, 1] = lev_move[1][:, row_edge[s], :]
        for t in range(2):
            lat_move = (to_last, to_first)[t]
            r = row_edge[t]
            edge_out[1, 2 * s + t, 0:1] = lat_move[1][lev_edge[s], r : r + 1, :]
            edge_out[1, 2 * s + t, 1:2] = lev_move[0][lev_edge[s], r : r + 1, :]
    for i in range(faces_end):
        guarded(wide_links[i][1], lambda i=i: wide_message(1, i).start())
    moved_lon = pack(to_first[2], to_last[2])
    at_lev_ends = jnp.where(lev3 == 0, to_first[0], jnp.where(lev3 == last_lev, to_last[0], 0.0))
    at_row_ends = jnp.where(row3 == 0, to_first[1], jnp.where(row3 == last_row, to_last[1], 0.0))
    pack_out[1, 0:1] = pack(partial, partial)
    pack_out[1, 1:2] = moved_lon
    pack_out[1, 2:3] = pack(at_lev_ends, at_lev_ends)
    pack_out[1, 3:4] = pack(at_row_ends, at_row_ends)
    for i in range(faces_end, len(wide_links)):
        guarded(wide_links[i][1], lambda i=i: wide_message(1, i).start())

    speed_lev = [up(speeds[0][0][0]), low(speeds[0][0][1])]
    speed_lat = [up(speeds[1][1][0]), low(speeds[1][1][1])]
    speed_lon = jnp.where(at_lane < flat_rows, low(speeds[2][2]), up(speeds[2][2]))
    settle(wide_lines(1, 1), recv_sem.at[1])
    side_pack, lev_pack, lat_pack = packs(1)

    left, right = ends_of(side_pack[1:2])
    field = partial + jnp.where(lane3 == 0, left, 0.0) + jnp.where(lane3 == cols - 1, right, 0.0)
    field = field + jnp.where(lev3 == 0, lev2_in[1, 0, 1][None], 0.0)
    field = field + jnp.where(lev3 == last_lev, lev2_in[1, 1, 1][None], 0.0)
    field = field + jnp.where(row3 == 0, lat2_in[1, 0, 1][:, None, :], 0.0)
    field = field + jnp.where(row3 == last_row, lat2_in[1, 1, 1][:, None, :], 0.0)

    plane_row = lax.broadcasted_iota(jnp.int32, (rows, cols), 0)
    plane_lane = lax.broadcasted_iota(jnp.int32, (rows, cols), 1)
    line_lev = lax.broadcasted_iota(jnp.int32, (levels, cols), 0)
    line_lane = lax.broadcasted_iota(jnp.int32, (levels, cols), 1)
    beside_lev, beside_lat = [], []
    for s in range(2):
        own = (to_first[0][0], to_last[0][last_lev])[s]
        plane = lev2_in[1, s, 0] + own
        plane = plane + jnp.where(plane_row == 0, edge_in[1, 2 * s, 0:1], 0.0)
        plane = plane + jnp.where(plane_row == last_row, edge_in[1, 2 * s + 1, 0:1], 0.0)
        begin = lev_edge[s] * rows
        moved = lev_pack[s][1:2]
        plane = plane + jnp.where(plane_lane == 0, column(moved, flat_rows + begin, 1, rows), 0.0)
        plane = plane + jnp.where(plane_lane == cols - 1, column(moved, begin, 1, rows), 0.0)
        beside_lev.append(plane * speed_lev[s])

        own = (to_first[1][:, 0, :], to_last[1][:, last_row, :])[s]
        plane = lat2_in[1, s, 0] + own
        plane = plane + jnp.where(line_lev == 0, edge_in[1, s, 1:2], 0.0)
        plane = plane + jnp.where(line_lev == last_lev, edge_in[1, 2 + s, 1:2], 0.0)
        begin = row_edge[s]
        moved = lat_pack[s][1:2]
        plane = plane + jnp.where(line_lane == 0, column(moved, flat_rows + begin, rows, levels), 0.0)
        plane = plane + jnp.where(line_lane == cols - 1, column(moved, begin, rows, levels), 0.0)
        beside_lat.append(plane * speed_lat[s])
    at = lax.rem(lax.broadcasted_iota(jnp.int32, (1, cols), 1), flat_rows)
    at_lev, at_row = lax.div(at, rows), lax.rem(at, rows)
    ring = side_pack[0:1] + pltpu.roll(moved_lon, flat_rows, axis=1)
    ring = ring + jnp.where(at_lev == 0, pltpu.roll(lev_pack[0][2:3], cols - last_lev * rows, axis=1), 0.0)
    ring = ring + jnp.where(at_lev == last_lev, pltpu.roll(lev_pack[1][2:3], last_lev * rows, axis=1), 0.0)
    ring = ring + jnp.where(at_row == 0, pltpu.roll(lat_pack[0][3:4], cols - last_row, axis=1), 0.0)
    ring = ring + jnp.where(at_row == last_row, pltpu.roll(lat_pack[1][3:4], last_row, axis=1), 0.0)
    beside_lon = ends_of(ring * speed_lon)

    below, above = shifted(
        [lower[k] * field for k in range(3)], [upper[k] * field for k in range(3)],
        beside_lev, beside_lat, beside_lon,
    )
    result = centre * field
    for k in range(3):
        result = result + above[k] + below[k]
    field = result
    adj_v[...] = field

    settle(narrow_lines(0) + wide_lines(0, 0) + wide_lines(1, 0), send_sem)


def finish(state_v, adj_v, outer, state_hbm, adj_hbm, next_hbm, wide, nxt, out_sem):
    levels, rows, cols = state_v.shape
    flat_rows = levels * rows
    wide_cols = outer.shape[1]
    fine = wide_cols // cols
    outer_rows = outer.shape[0] // levels
    stores = [
        pltpu.make_async_copy(state_v, state_hbm, out_sem.at[0]),
        pltpu.make_async_copy(adj_v, adj_hbm, out_sem.at[1]),
    ]
    for store in stores:
        store.start()
    field = adj_v[...]

    table = (
        lax.broadcasted_iota(jnp.int32, (cols, wide_cols), 0)
        == lax.broadcasted_iota(jnp.int32, (cols, wide_cols), 1) // fine
    ).astype(jnp.float32).astype(jnp.bfloat16)
    halves = bf16_parts(field.reshape(flat_rows, cols), 2)
    spread = jnp.dot(
        jnp.concatenate([h.astype(jnp.bfloat16) for h in halves], axis=1),
        jnp.concatenate([table, table], axis=0),
        preferred_element_type=jnp.float32,
    )
    for k in range(fine):
        for c in range(fine):
            wide[c, pl.ds(k, flat_rows, stride=fine), :] = spread[:, c * cols : (c + 1) * cols]
    for level in range(levels):
        span = pl.ds(level * outer_rows, outer_rows)
        for c in range(fine):
            lanes = pl.ds(c * cols, cols)
            nxt[span, lanes] = (outer[span, lanes].astype(jnp.float32) - wide[c, span, :]).astype(jnp.bfloat16)
        store = pltpu.make_async_copy(nxt.at[span], next_hbm.at[span], out_sem.at[2 + level])
        store.start()
        stores.append(store)
    for store in stores:
        store.wait()


def shards(ends, outer_increment, courant, obs_column, obs_level, obs_value):
    levels, outer_rows, wide_cols = outer_increment.shape
    _, _, rows, cols = courant.shape
    flat_rows = levels * rows
    fine = wide_cols // cols
    lanes = 128
    observed = (obs_column.shape[0] // lanes, lanes)
    assert 2 * flat_rows == cols and levels > 1 and rows > 1
    f32, bf16 = jnp.float32, jnp.bfloat16
    outer_shape = (levels * outer_rows, wide_cols)
    vmem = pl.BlockSpec(memory_space=pltpu.VMEM)
    hbm = pl.BlockSpec(memory_space=pl.ANY)
    held = pl.pallas_call(
        functools.partial(kernel, ends),
        out_shape=(
            pltpu.VMEM((levels, rows, cols), f32),
            pltpu.VMEM((levels, rows, cols), f32),
            pltpu.VMEM(outer_shape, bf16),
        ),
        in_specs=[hbm] * 5,
        out_specs=(vmem,) * 3,
        scratch_shapes=[
            pltpu.VMEM(courant.shape, bf16),
            pltpu.VMEM(observed, jnp.int32),
            pltpu.VMEM(observed, jnp.int32),
            pltpu.VMEM(observed, f32),
            pltpu.VMEM((levels * outer_rows, cols), f32),
            pltpu.VMEM((ROUNDS, 2, rows, cols), f32),
            pltpu.VMEM((ROUNDS, 2, levels, cols), f32),
            pltpu.VMEM((ROUNDS, 1, cols), f32),
            pltpu.VMEM((ROUNDS, 2, rows, cols), f32),
            pltpu.VMEM((ROUNDS, 2, levels, cols), f32),
            pltpu.VMEM((ROUNDS, 2, 1, cols), f32),
            pltpu.VMEM((2, 2, 2, rows, cols), f32),
            pltpu.VMEM((2, 2, 2, levels, cols), f32),
            pltpu.VMEM((2, 4, 2, cols), f32),
            pltpu.VMEM((2, 4, cols), f32),
            pltpu.VMEM((2, 2, 2, rows, cols), f32),
            pltpu.VMEM((2, 2, 2, levels, cols), f32),
            pltpu.VMEM((2, 4, 2, cols), f32),
            pltpu.VMEM((2, 10, 4, cols), f32),
            pltpu.VMEM((1024, 1, cols), f32),
            pltpu.SemaphoreType.DMA((5,)),
            pltpu.SemaphoreType.DMA,
            pltpu.SemaphoreType.DMA((2,)),
        ],
        compiler_params=pltpu.CompilerParams(collective_id=0, has_side_effects=True),
    )(
        outer_increment.reshape(outer_shape),
        courant,
        obs_column.reshape(observed),
        obs_level.reshape(observed),
        obs_value.reshape(observed),
    )
    state, adjoint, following = pl.pallas_call(
        finish,
        out_shape=(
            jax.ShapeDtypeStruct((levels, rows, cols), f32),
            jax.ShapeDtypeStruct((levels, rows, cols), f32),
            jax.ShapeDtypeStruct(outer_shape, bf16),
        ),
        in_specs=[vmem] * 3,
        out_specs=(hbm,) * 3,
        scratch_shapes=[
            pltpu.VMEM((fine, levels * outer_rows, cols), f32),
            pltpu.VMEM(outer_shape, bf16),
            pltpu.SemaphoreType.DMA((2 + levels,)),
        ],
    )(*[pltpu.with_memory_space_constraint(x, pltpu.VMEM) for x in held])
    return state, adjoint, following.reshape(outer_increment.shape)


def solution(mesh):
    ends = tuple(mesh.shape[a] for a in ("lat", "lon", "lev"))
    block = P("lev", "lat", "lon")
    observed = P(("lat", "lon"))
    return jax.shard_map(
        functools.partial(shards, ends),
        mesh=mesh,
        in_specs=(block, P(None, "lev", "lat", "lon"), observed, observed, observed),
        out_specs=(block, block, block),
        check_vma=False,
    )
```

```python
import functools

import jax
import jax.numpy as jnp
from jax import lax
from jax.experimental import pallas as pl
from jax.experimental.pallas import tpu as pltpu
from jax.sharding import PartitionSpec as P

MESH = pl.DeviceIdType.MESH
REACH = 4
GROUP = 2 * REACH
TILE = 8


def bf16_parts(x, count):
    parts = []
    for _ in range(count):
        part = x.astype(jnp.bfloat16).astype(jnp.float32)
        parts.append(part)
        x = x - part
    return parts


def forward(v, c, minus, plus):
    sizes = [jnp.abs(n) for n in c]
    result = (1.0 - sizes[0] - sizes[1] - sizes[2]) * v
    for k in range(3):
        result = result + sizes[k] * jnp.where(c[k] > 0.0, minus[k], plus[k])
    return result


def shares(p, c):
    low, up = [], []
    for n in c:
        moved = jnp.abs(n) * p
        low.append(jnp.where(n > 0.0, moved, 0.0))
        up.append(jnp.where(n > 0.0, 0.0, moved))
    return low, up


def centre_of(c):
    return 1.0 - jnp.abs(c[0]) - jnp.abs(c[1]) - jnp.abs(c[2])


def kernel(
    ends, outer_hbm, courant_hbm, col_hbm, lvl_hbm, val_hbm,
    state_v, adj_v, outer,
    courant, col, lvl, val, sums,
    own, face_in, last_in, side_in, edge_out, edge_in, halo,
    strip, strip_full, strip_half,
    seen, seen_in, seen_strip, seen_full, seen_half, units,
    in_sem, send_sem, recv_sem,
):
    n_lat, n_lon, n_lev = ends
    levels, rows, cols = state_v.shape
    flat_rows = levels * rows
    wide_cols = outer.shape[1]
    fine = wide_cols // cols
    near = REACH - 1
    span = seen.shape[0]
    beyond = (span - levels) // 2

    me_lat, me_lon, me_lev = (lax.axis_index(a) for a in ("lat", "lon", "lev"))
    links = (
        ("lev", me_lev + 1, me_lev < n_lev - 1),
        ("lev", me_lev - 1, me_lev > 0),
        ("lat", me_lat + 1, me_lat < n_lat - 1),
        ("lat", me_lat - 1, me_lat > 0),
        ("lon", lax.rem(me_lon + 1, n_lon), None),
        ("lon", lax.rem(me_lon + n_lon - 1, n_lon), None),
    )
    turns = (0, 1) if n_lon > 2 else (0,)
    bands = ((rows - TILE, TILE), (0, TILE))

    def both(flags):
        return functools.reduce(jnp.logical_and, flags) if flags else None

    def guarded(exists, action):
        if exists is None:
            action()
        else:
            pl.when(exists)(action)

    class Message:
        def __init__(self, which, source, landing, sem):
            self.needs = tuple(w for w in which if w < 4)
            self.target = {links[w][0]: links[w][1] for w in which}
            self.exists = both([links[w][2] for w in self.needs])
            self.arrives = both([links[w ^ 1][2] for w in self.needs])
            self.source, self.landing, self.sem = source, landing, sem

        def start(self):
            def begin():
                pltpu.make_async_remote_copy(
                    src_ref=self.source, dst_ref=self.landing, send_sem=send_sem, recv_sem=recv_sem.at[self.sem],
                    device_id=self.target, device_id_type=MESH,
                ).start()

            guarded(self.exists, begin)

        def lines(self):
            total = 1
            for n in self.landing.shape:
                total = total * n
            return total // cols

    partners, first, second = [], [], []
    for a in (2, 1, 0):
        for t in (0, 1, None):
            for u in turns + (None,):
                which = [a - 1] if a else []
                which = which + ([2 + t] if t is not None else []) + ([4 + u] if u is not None else [])
                if not which:
                    continue
                partners.append(which)
                b = 0 if u is None else u + 1
                if t is None:
                    first.append(Message(which, strip, strip_full.at[a, b], 0))
                else:
                    first.append(Message(which, strip.at[pl.ds(*bands[t])], strip_half.at[a, t, b], 0))
                if u is None:
                    if a and t is None:
                        begin = levels - near if a == 1 else 0
                        furthest = levels - REACH if a == 1 else near
                        first.append(Message(which, own.at[pl.ds(begin, near)], face_in.at[a - 1], 0))
                        first.append(Message(which, own.at[furthest, 0], last_in.at[a - 1], 0))
                    elif a:
                        first.append(Message(which, edge_out.at[a - 1, t], edge_in.at[a - 1, t], 0))
                    else:
                        first.append(Message(which, own.at[:, :, pl.ds(*bands[t])], side_in.at[t], 0))
                if not a:
                    if t is None:
                        second.append(Message(which, seen_strip, seen_full.at[u], 1))
                    else:
                        second.append(Message(which, seen_strip.at[:, pl.ds(*bands[t])], seen_half.at[t, b], 1))
                    if u is None:
                        kept = pl.ds(1, span - 2)
                        second.append(Message(which, seen.at[kept, :, pl.ds(*bands[t])], seen_in.at[t], 1))
    first.sort(key=lambda m: m.lines() - 64 * len(m.target))

    barrier = pltpu.get_barrier_semaphore()
    expected = 0
    for which in partners:
        exists = both([links[w][2] for w in which if w < 4])
        target = {links[w][0]: links[w][1] for w in which}
        guarded(exists, lambda target=target: pl.semaphore_signal(barrier, inc=1, device_id=target, device_id_type=MESH))
        expected = expected + (1 if exists is None else exists.astype(jnp.int32))

    loads = [
        pltpu.make_async_copy(src, dst, in_sem.at[i])
        for i, (src, dst) in enumerate(
            ((outer_hbm, outer), (courant_hbm, courant), (col_hbm, col), (lvl_hbm, lvl), (val_hbm, val))
        )
    ]
    for load in loads:
        load.start()

    def settle(messages, flip, sem, known=()):
        if len(known) < 4:
            for has in (True, False):
                flag = links[len(known)][2]
                pl.when(flag if has else jnp.logical_not(flag))(
                    lambda has=has: settle(messages, flip, sem, known + (has,))
                )
            return
        total = sum(m.lines() for m in messages if all(known[w ^ flip] for w in m.needs))
        view = units.at[pl.ds(0, total)]
        pltpu.make_async_copy(view, view, sem).wait()

    def clear(ref):
        ref[...] = jnp.zeros(ref.shape, jnp.float32)

    for m in first + second:
        if m.arrives is not None:
            pl.when(jnp.logical_not(m.arrives))(lambda m=m: clear(m.landing))
    clear(halo)

    lane = lax.broadcasted_iota(jnp.int32, (rows, cols), 1)
    group = lane // GROUP
    pool = (
        lax.broadcasted_iota(jnp.int32, (wide_cols, cols), 0) // fine
        == lax.broadcasted_iota(jnp.int32, (wide_cols, cols), 1)
    ).astype(jnp.float32).astype(jnp.bfloat16)

    loads[1].wait()
    for k in range(3):
        own[:, k + 1] = courant[k].astype(jnp.float32)
    loads[0].wait()
    sums[...] = jnp.dot(outer[...], pool, preferred_element_type=jnp.float32)
    coarse = sums[pl.ds(0, flat_rows, stride=fine), :]
    for k in range(1, fine):
        coarse = coarse + sums[pl.ds(k, flat_rows, stride=fine), :]
    own[:, 0] = (coarse * (1.0 / (fine * fine))).reshape(levels, rows, cols)

    ends_only = jnp.zeros((rows, cols), jnp.float32)
    for f in (1, 2, 3, 0):
        for l in range(levels):
            place = f * levels + l
            ends_only = jnp.where(group == place, pltpu.roll(own[l, f], (REACH + GROUP * place) % cols, axis=1), ends_only)
    strip[...] = ends_only

    entries = [(0, i, j) for i in range(1, REACH) for j in range(1, REACH + 1 - i)]
    entries = entries + [(f, i, j) for f in (1, 2, 3) for i in range(1, near) for j in range(1, near + 1 - i)]
    for s in range(2):
        for t in range(2):
            for n, (f, i, j) in enumerate(entries):
                l = levels - i if s == 0 else i - 1
                r = rows - j if t == 0 else j - 1
                edge_out[s, t, n : n + 1, :] = own[l, f, r : r + 1, :]

    pl.semaphore_wait(barrier, expected)
    for m in first:
        m.start()

    for load in loads[2:]:
        load.wait()
    where_row = (lvl[...] - me_lev * levels + beyond) * rows + col[...] // cols
    where_col = col[...] % cols
    parts = bf16_parts(val[...], 2)
    pieces, width = col.shape
    row_id = lax.broadcasted_iota(jnp.int32, (span * rows, width), 0)
    col_id = lax.broadcasted_iota(jnp.int32, (cols, width), 0)
    hits = [[] for _ in range(3)]
    tables = []
    for k in range(pieces):
        match = where_row[k : k + 1] == row_id
        hits[0].append(jnp.where(match, 1.0, 0.0).astype(jnp.bfloat16))
        for i, part in enumerate(parts):
            hits[i + 1].append(jnp.where(match, part[k : k + 1], 0.0).astype(jnp.bfloat16))
        tables.append(jnp.where(where_col[k : k + 1] == col_id, 1.0, 0.0).astype(jnp.bfloat16))
    left_side = jnp.concatenate([jnp.concatenate(h, axis=1) for h in hits], axis=0)
    totals = lax.dot_general(
        left_side, jnp.concatenate(tables, axis=1), (((1,), (1,)), ((), ())),
        preferred_element_type=jnp.float32,
    )
    wide_rows = span * rows
    counted = totals[:wide_rows].reshape(span, rows, cols)
    summed = (totals[wide_rows : 2 * wide_rows] + totals[2 * wide_rows :]).reshape(span, rows, cols)
    seen[:, 0] = counted
    seen[:, 1] = summed
    for i, values in enumerate((counted, summed)):
        ends_only = jnp.zeros((rows, cols), jnp.float32)
        for g in range(span):
            place = g + REACH - beyond
            ends_only = jnp.where(group == place, pltpu.roll(values[g], (REACH + GROUP * place) % cols, axis=1), ends_only)
        seen_strip[i] = ends_only
    for m in second:
        m.start()

    settle(first, 1, recv_sem.at[0])

    tall = rows + TILE
    half = lax.broadcasted_iota(jnp.int32, (TILE, cols), 0) < TILE // 2
    lanes = lax.broadcasted_iota(jnp.int32, (tall, cols), 1)
    slot = lanes % GROUP
    left_half = slot < REACH
    blank = jnp.zeros((TILE, cols), jnp.float32)

    def joined(full, before, after):
        return jnp.concatenate([full, jnp.where(half, after, before)], axis=0)

    for s in range(2):
        for t in range(2):
            for n, (f, i, j) in enumerate(entries):
                r = TILE - j if t == 0 else j - 1
                halo[s, i - 1, f, r : r + 1, :] = edge_in[s, t, n : n + 1, :]

    def cell(l, f):
        if 0 <= l < levels:
            return joined(own[l, f], side_in[0, l, f], side_in[1, l, f])
        s, i = (0, -l) if l < 0 else (1, l - levels + 1)
        if i == REACH:
            return jnp.concatenate([last_in[s], blank], axis=0)
        full = face_in[s, near - i, f] if s == 0 else face_in[s, i - 1, f]
        return jnp.concatenate([full, halo[s, i - 1, f]], axis=0)

    def down(x):
        return pltpu.roll(x, 1, axis=0)

    def up_row(x):
        return pltpu.roll(x, tall - 1, axis=0)

    def right(x, by=1):
        return pltpu.roll(x, by, axis=1)

    def left(x, by=1):
        return pltpu.roll(x, cols - by, axis=1)

    before_b, after_b = 1, (2 if n_lon > 2 else 1)

    def strip_block(a, b):
        full = strip[...] if a == 0 and b == 0 else strip_full[a, b]
        return joined(full, strip_half[a, 0, b], strip_half[a, 1, b])

    def placed(blocks, f):
        turned = [right(blocks[a], (GROUP * levels * (n - f)) % cols) if n != f else blocks[a] for n, a in enumerate((1, 0, 2))]
        width = GROUP * levels
        return jnp.where(lanes < width, turned[0], jnp.where(lanes < 2 * width, turned[1], turned[2]))

    mine = [strip_block(a, 0) for a in range(3)]
    sides = []
    sides.append([jnp.where(left_half, strip_block(a, before_b), mine[a]) for a in range(3)])
    sides.append([jnp.where(left_half, mine[a], strip_block(a, after_b)) for a in range(3)])
    side_c, side_v = [], []
    for blocks in sides:
        c = [placed(blocks, k + 1) for k in range(3)]
        v = placed(blocks, 0)
        for _ in range(2):
            v = forward(v, c, [right(v, GROUP), down(v), right(v)], [left(v, GROUP), up_row(v), left(v)])
        side_c.append(c)
        side_v.append(v)

    def inserted(z, l):
        return right(z, (cols - REACH - GROUP * (l + REACH)) % cols)

    speeds = {l: [cell(l, k + 1) for k in range(3)] for l in range(-near, levels + near)}
    v = {l: cell(l, 0) for l in range(-REACH, levels + REACH)}
    for reach in (near, near - 1):
        v = {
            l: forward(v[l], speeds[l], [v[l - 1], down(v[l]), right(v[l])], [v[l + 1], up_row(v[l]), left(v[l])])
            for l in range(-reach, levels + reach)
        }
    fix = jnp.where(left_half, side_v[1], side_v[0])
    rim = (lanes < 2) | (lanes >= cols - 2)
    v = {l: jnp.where(rim, inserted(fix, l), v[l]) for l in v}
    for l in range(levels):
        state_v[l] = v[l][:rows]

    settle(second, 1, recv_sem.at[1])

    def seen_cell(l, i):
        g = l + beyond
        if 0 < g < span - 1:
            return joined(seen[g, i], seen_in[0, g - 1, i], seen_in[1, g - 1, i])
        return jnp.concatenate([seen[g, i], blank], axis=0)

    def seen_block(b, i):
        full = seen_strip[i] if b == 0 else seen_full[b - 1, i]
        return joined(full, seen_half[0, b, i], seen_half[1, b, i])

    side_q = []
    for side in range(2):
        known = []
        for i in range(2):
            if side == 0:
                known.append(jnp.where(left_half, seen_block(before_b, i), seen_block(0, i)))
            else:
                known.append(jnp.where(left_half, seen_block(0, i), seen_block(after_b, i)))
        p = known[0] * side_v[side] - known[1]
        c = side_c[side]
        low, up = shares(p, c)
        q = centre_of(c) * p + left(low[0], GROUP) + right(up[0], GROUP)
        q = q + up_row(low[1]) + down(up[1]) + left(low[2]) + right(up[2])
        low, up = shares(q, c)
        side_q.append((q, right(up[2]) if side == 0 else left(low[2])))
    fix = jnp.where(left_half, side_q[1][0], side_q[0][0])
    crossing = jnp.where(left_half, side_q[1][1], side_q[0][1])

    p = {l: seen_cell(l, 0) * v[l] - seen_cell(l, 1) for l in v}
    low, up = {}, {}
    for l in p:
        low[l], up[l] = shares(p[l], speeds[l])
    rim = (lanes < 1) | (lanes >= cols - 1)
    q = {}
    for l in range(-1, levels + 1):
        total = centre_of(speeds[l]) * p[l] + low[l + 1][0] + up[l - 1][0]
        total = total + up_row(low[l][1]) + down(up[l][1]) + left(low[l][2]) + right(up[l][2])
        q[l] = jnp.where(rim, inserted(fix, l), total)
    for l in q:
        low[l], up[l] = shares(q[l], speeds[l])
    for l in range(levels):
        total = centre_of(speeds[l]) * q[l] + low[l + 1][0] + up[l - 1][0]
        total = total + up_row(low[l][1]) + down(up[l][1])
        total = total + jnp.where(rim, inserted(crossing, l), 0.0)
        total = total + jnp.where(lanes >= cols - 1, 0.0, left(low[l][2])) + jnp.where(lanes < 1, 0.0, right(up[l][2]))
        adj_v[l] = total[:rows]

    settle(first + second, 0, send_sem)


def finish(state_v, adj_v, outer, state_hbm, adj_hbm, next_hbm, wide, nxt, out_sem):
    levels, rows, cols = state_v.shape
    flat_rows = levels * rows
    wide_cols = outer.shape[1]
    fine = wide_cols // cols
    outer_rows = outer.shape[0] // levels
    stores = [
        pltpu.make_async_copy(state_v, state_hbm, out_sem.at[0]),
        pltpu.make_async_copy(adj_v, adj_hbm, out_sem.at[1]),
    ]
    for store in stores:
        store.start()
    field = adj_v[...]

    table = (
        lax.broadcasted_iota(jnp.int32, (cols, wide_cols), 0)
        == lax.broadcasted_iota(jnp.int32, (cols, wide_cols), 1) // fine
    ).astype(jnp.float32).astype(jnp.bfloat16)
    halves = bf16_parts(field.reshape(flat_rows, cols), 2)
    spread = jnp.dot(
        jnp.concatenate([h.astype(jnp.bfloat16) for h in halves], axis=1),
        jnp.concatenate([table, table], axis=0),
        preferred_element_type=jnp.float32,
    )
    for k in range(fine):
        for c in range(fine):
            wide[c, pl.ds(k, flat_rows, stride=fine), :] = spread[:, c * cols : (c + 1) * cols]
    for level in range(levels):
        span = pl.ds(level * outer_rows, outer_rows)
        for c in range(fine):
            lanes = pl.ds(c * cols, cols)
            nxt[span, lanes] = (outer[span, lanes].astype(jnp.float32) - wide[c, span, :]).astype(jnp.bfloat16)
        store = pltpu.make_async_copy(nxt.at[span], next_hbm.at[span], out_sem.at[2 + level])
        store.start()
        stores.append(store)
    for store in stores:
        store.wait()


def shards(ends, outer_increment, courant, obs_column, obs_level, obs_value):
    levels, outer_rows, wide_cols = outer_increment.shape
    _, _, rows, cols = courant.shape
    flat_rows = levels * rows
    fine = wide_cols // cols
    lanes = 128
    observed = (obs_column.shape[0] // lanes, lanes)
    span = levels + 4
    assert 4 * levels * GROUP == cols and levels >= REACH and rows % TILE == 0 and ends[1] > 1
    f32, bf16 = jnp.float32, jnp.bfloat16
    outer_shape = (levels * outer_rows, wide_cols)
    vmem = pl.BlockSpec(memory_space=pltpu.VMEM)
    hbm = pl.BlockSpec(memory_space=pl.ANY)
    held = pl.pallas_call(
        functools.partial(kernel, ends),
        out_shape=(
            pltpu.VMEM((levels, rows, cols), f32),
            pltpu.VMEM((levels, rows, cols), f32),
            pltpu.VMEM(outer_shape, bf16),
        ),
        in_specs=[hbm] * 5,
        out_specs=(vmem,) * 3,
        scratch_shapes=[
            pltpu.VMEM(courant.shape, bf16),
            pltpu.VMEM(observed, jnp.int32),
            pltpu.VMEM(observed, jnp.int32),
            pltpu.VMEM(observed, f32),
            pltpu.VMEM((levels * outer_rows, cols), f32),
            pltpu.VMEM((levels, 4, rows, cols), f32),
            pltpu.VMEM((2, REACH - 1, 4, rows, cols), f32),
            pltpu.VMEM((2, rows, cols), f32),
            pltpu.VMEM((2, levels, 4, TILE, cols), f32),
            pltpu.VMEM((2, 2, 2 * TILE, cols), f32),
            pltpu.VMEM((2, 2, 2 * TILE, cols), f32),
            pltpu.VMEM((2, REACH - 1, 4, TILE, cols), f32),
            pltpu.VMEM((rows, cols), f32),
            pltpu.VMEM((3, 3, rows, cols), f32),
            pltpu.VMEM((3, 2, 3, TILE, cols), f32),
            pltpu.VMEM((span, 2, rows, cols), f32),
            pltpu.VMEM((2, span - 2, 2, TILE, cols), f32),
            pltpu.VMEM((2, rows, cols), f32),
            pltpu.VMEM((2, 2, rows, cols), f32),
            pltpu.VMEM((2, 3, 2, TILE, cols), f32),
            pltpu.VMEM((2048, 1, cols), f32),
            pltpu.SemaphoreType.DMA((5,)),
            pltpu.SemaphoreType.DMA,
            pltpu.SemaphoreType.DMA((2,)),
        ],
        compiler_params=pltpu.CompilerParams(collective_id=0, has_side_effects=True),
    )(
        outer_increment.reshape(outer_shape),
        courant,
        obs_column.reshape(observed),
        obs_level.reshape(observed),
        obs_value.reshape(observed),
    )
    state, adjoint, following = pl.pallas_call(
        finish,
        out_shape=(
            jax.ShapeDtypeStruct((levels, rows, cols), f32),
            jax.ShapeDtypeStruct((levels, rows, cols), f32),
            jax.ShapeDtypeStruct(outer_shape, bf16),
        ),
        in_specs=[vmem] * 3,
        out_specs=(hbm,) * 3,
        scratch_shapes=[
            pltpu.VMEM((fine, levels * outer_rows, cols), f32),
            pltpu.VMEM(outer_shape, bf16),
            pltpu.SemaphoreType.DMA((2 + levels,)),
        ],
    )(*[pltpu.with_memory_space_constraint(x, pltpu.VMEM) for x in held])
    return state, adjoint, following.reshape(outer_increment.shape)


def solution(mesh):
    ends = tuple(mesh.shape[a] for a in ("lat", "lon", "lev"))
    block = P("lev", "lat", "lon")
    observed = P(("lat", "lon"))
    return jax.shard_map(
        functools.partial(shards, ends),
        mesh=mesh,
        in_specs=(block, P(None, "lev", "lat", "lon"), observed, observed, observed),
        out_specs=(block, block, block),
        check_vma=False,
    )
```

```python
import functools

import jax
import jax.numpy as jnp
from jax import lax
from jax.experimental import pallas as pl
from jax.experimental.pallas import tpu as pltpu
from jax.sharding import PartitionSpec as P

MESH = pl.DeviceIdType.MESH
REACH = 4
GROUP = 2 * REACH
TILE = 8


def bf16_parts(x, count):
    parts = []
    for _ in range(count):
        part = x.astype(jnp.bfloat16).astype(jnp.float32)
        parts.append(part)
        x = x - part
    return parts


def forward(v, c, minus, plus):
    sizes = [jnp.abs(n) for n in c]
    result = (1.0 - sizes[0] - sizes[1] - sizes[2]) * v
    for k in range(3):
        result = result + sizes[k] * jnp.where(c[k] > 0.0, minus[k], plus[k])
    return result


def shares(p, c):
    low, up = [], []
    for n in c:
        moved = jnp.abs(n) * p
        low.append(jnp.where(n > 0.0, moved, 0.0))
        up.append(jnp.where(n > 0.0, 0.0, moved))
    return low, up


def centre_of(c):
    return 1.0 - jnp.abs(c[0]) - jnp.abs(c[1]) - jnp.abs(c[2])


def kernel(
    ends, outer_hbm, courant_hbm, col_hbm, lvl_hbm, val_hbm,
    state_v, adj_v, outer,
    courant, col, lvl, val, sums,
    own, face_in, last_in, side_in, edge_out, edge_in, halo,
    strip, strip_full, strip_half,
    seen, seen_in, seen_strip, seen_full, seen_half, units,
    in_sem, send_sem, recv_sem, ready,
):
    n_lat, n_lon, n_lev = ends
    levels, rows, cols = state_v.shape
    flat_rows = levels * rows
    wide_cols = outer.shape[1]
    fine = wide_cols // cols
    near = REACH - 1
    span = seen.shape[0]
    beyond = (span - levels) // 2

    me_lat, me_lon, me_lev = (lax.axis_index(a) for a in ("lat", "lon", "lev"))
    links = (
        ("lev", me_lev + 1, me_lev < n_lev - 1),
        ("lev", me_lev - 1, me_lev > 0),
        ("lat", me_lat + 1, me_lat < n_lat - 1),
        ("lat", me_lat - 1, me_lat > 0),
        ("lon", lax.rem(me_lon + 1, n_lon), None),
        ("lon", lax.rem(me_lon + n_lon - 1, n_lon), None),
    )
    turns = (0, 1) if n_lon > 2 else (0,)
    bands = ((rows - TILE, TILE), (0, TILE))

    def both(flags):
        return functools.reduce(jnp.logical_and, flags) if flags else None

    def guarded(exists, action):
        if exists is None:
            action()
        else:
            pl.when(exists)(action)

    def stage_of(which):
        if 0 in which:
            return 3
        if 1 in which:
            return 1 if len(which) == 3 else 0
        return 2 if 2 in which else 0

    class Message:
        def __init__(self, which, source, landing, sem):
            self.needs = tuple(w for w in which if w < 4)
            self.stage = stage_of(which)
            self.target = {links[w][0]: links[w][1] for w in which}
            self.exists = both([links[w][2] for w in self.needs])
            self.arrives = both([links[w ^ 1][2] for w in self.needs])
            self.source, self.landing, self.sem = source, landing, sem

        def start(self):
            def begin():
                pltpu.make_async_remote_copy(
                    src_ref=self.source, dst_ref=self.landing, send_sem=send_sem, recv_sem=recv_sem.at[self.sem],
                    device_id=self.target, device_id_type=MESH,
                ).start()

            guarded(self.exists, begin)

        def lines(self):
            total = 1
            for n in self.landing.shape:
                total = total * n
            return total // cols

    partners, first, second = [], [], []
    for a in (2, 1, 0):
        for t in (0, 1, None):
            for u in turns + (None,):
                which = [a - 1] if a else []
                which = which + ([2 + t] if t is not None else []) + ([4 + u] if u is not None else [])
                if not which:
                    continue
                partners.append(which)
                b = 0 if u is None else u + 1
                if t is None:
                    first.append(Message(which, strip, strip_full.at[a, b], 0))
                else:
                    first.append(Message(which, strip.at[pl.ds(*bands[t])], strip_half.at[a, t, b], 0))
                if u is None:
                    if a and t is None:
                        begin = levels - near if a == 1 else 0
                        furthest = levels - REACH if a == 1 else near
                        first.append(Message(which, own.at[pl.ds(begin, near)], face_in.at[a - 1], 0))
                        first.append(Message(which, own.at[furthest, 0], last_in.at[a - 1], 0))
                    elif a:
                        first.append(Message(which, edge_out.at[a - 1, t], edge_in.at[a - 1, t], 0))
                    else:
                        first.append(Message(which, own.at[:, :, pl.ds(*bands[t])], side_in.at[t], 0))
                if not a:
                    if t is None:
                        second.append(Message(which, seen_strip, seen_full.at[u], 1))
                    else:
                        second.append(Message(which, seen_strip.at[:, pl.ds(*bands[t])], seen_half.at[t, b], 1))
                    if u is None:
                        kept = pl.ds(1, span - 2)
                        second.append(Message(which, seen.at[kept, :, pl.ds(*bands[t])], seen_in.at[t], 1))
    first.sort(key=lambda m: m.lines() - 64 * len(m.target))

    def count(chosen):
        return sum(
            1 if flags is None else flags.astype(jnp.int32)
            for flags in (both([links[w][2] for w in which if w < 4]) for which in chosen)
        )

    def signal(sem, chosen):
        for which in chosen:
            target = {links[w][0]: links[w][1] for w in which}
            guarded(
                both([links[w][2] for w in which if w < 4]),
                lambda target=target: pl.semaphore_signal(sem, inc=1, device_id=target, device_id_type=MESH),
            )

    barrier = pltpu.get_barrier_semaphore()
    near_by = [which for which in partners if len(which) < 3 or not {0, 1} & set(which)]
    lower = [which for which in near_by if 1 in which]
    upper = [which for which in near_by if 0 in which]
    level = [which for which in near_by if which not in lower + upper]
    north = [which for which in level if 2 in which]
    south = [which for which in level if 3 in which]
    around = [which for which in level if which not in north + south]
    signal(barrier, upper + north + around)

    loads = [
        pltpu.make_async_copy(src, dst, in_sem.at[i])
        for i, (src, dst) in enumerate(
            ((outer_hbm, outer), (courant_hbm, courant), (col_hbm, col), (lvl_hbm, lvl), (val_hbm, val))
        )
    ]
    for load in loads:
        load.start()

    def settle(messages, flip, sem, known=()):
        if len(known) < 4:
            for has in (True, False):
                flag = links[len(known)][2]
                pl.when(flag if has else jnp.logical_not(flag))(
                    lambda has=has: settle(messages, flip, sem, known + (has,))
                )
            return
        total = sum(m.lines() for m in messages if all(known[w ^ flip] for w in m.needs))
        view = units.at[pl.ds(0, total)]
        pltpu.make_async_copy(view, view, sem).wait()

    def clear(ref):
        ref[...] = jnp.zeros(ref.shape, jnp.float32)

    for m in first + second:
        if m.arrives is not None:
            pl.when(jnp.logical_not(m.arrives))(lambda m=m: clear(m.landing))
    clear(halo)

    lane = lax.broadcasted_iota(jnp.int32, (rows, cols), 1)
    group = lane // GROUP
    pool = (
        lax.broadcasted_iota(jnp.int32, (wide_cols, cols), 0) // fine
        == lax.broadcasted_iota(jnp.int32, (wide_cols, cols), 1)
    ).astype(jnp.float32).astype(jnp.bfloat16)

    loads[1].wait()
    for k in range(3):
        own[:, k + 1] = courant[k].astype(jnp.float32)
    loads[0].wait()
    sums[...] = jnp.dot(outer[...], pool, preferred_element_type=jnp.float32)
    coarse = sums[pl.ds(0, flat_rows, stride=fine), :]
    for k in range(1, fine):
        coarse = coarse + sums[pl.ds(k, flat_rows, stride=fine), :]
    own[:, 0] = (coarse * (1.0 / (fine * fine))).reshape(levels, rows, cols)

    ends_only = jnp.zeros((rows, cols), jnp.float32)
    for f in (1, 2, 3, 0):
        for l in range(levels):
            place = f * levels + l
            ends_only = jnp.where(group == place, pltpu.roll(own[l, f], (REACH + GROUP * place) % cols, axis=1), ends_only)
    strip[...] = ends_only

    entries = [(0, i, j) for i in range(1, REACH) for j in range(1, REACH + 1 - i)]
    entries = entries + [(f, i, j) for f in (1, 2, 3) for i in range(1, near) for j in range(1, near + 1 - i)]
    for s in range(2):
        for t in range(2):
            for n, (f, i, j) in enumerate(entries):
                l = levels - i if s == 0 else i - 1
                r = rows - j if t == 0 else j - 1
                edge_out[s, t, n : n + 1, :] = own[l, f, r : r + 1, :]

    pl.semaphore_wait(barrier, count(lower + south + around))
    signal(ready.at[0], around)
    signal(ready.at[2], lower)
    signal(ready.at[1], south)
    for m in first:
        if m.stage == 0:
            m.start()

    for load in loads[2:]:
        load.wait()
    where_row = (lvl[...] - me_lev * levels + beyond) * rows + col[...] // cols
    where_col = col[...] % cols
    parts = bf16_parts(val[...], 2)
    pieces, width = col.shape
    row_id = lax.broadcasted_iota(jnp.int32, (span * rows, width), 0)
    col_id = lax.broadcasted_iota(jnp.int32, (cols, width), 0)
    hits = [[] for _ in range(3)]
    tables = []
    for k in range(pieces):
        match = where_row[k : k + 1] == row_id
        hits[0].append(jnp.where(match, 1.0, 0.0).astype(jnp.bfloat16))
        for i, part in enumerate(parts):
            hits[i + 1].append(jnp.where(match, part[k : k + 1], 0.0).astype(jnp.bfloat16))
        tables.append(jnp.where(where_col[k : k + 1] == col_id, 1.0, 0.0).astype(jnp.bfloat16))
    left_side = jnp.concatenate([jnp.concatenate(h, axis=1) for h in hits], axis=0)
    totals = lax.dot_general(
        left_side, jnp.concatenate(tables, axis=1), (((1,), (1,)), ((), ())),
        preferred_element_type=jnp.float32,
    )
    wide_rows = span * rows
    counted = totals[:wide_rows].reshape(span, rows, cols)
    summed = (totals[wide_rows : 2 * wide_rows] + totals[2 * wide_rows :]).reshape(span, rows, cols)
    seen[:, 0] = counted
    seen[:, 1] = summed
    for i, values in enumerate((counted, summed)):
        ends_only = jnp.zeros((rows, cols), jnp.float32)
        for g in range(span):
            place = g + REACH - beyond
            ends_only = jnp.where(group == place, pltpu.roll(values[g], (REACH + GROUP * place) % cols, axis=1), ends_only)
        seen_strip[i] = ends_only
    for m in second:
        if m.stage == 0:
            m.start()
    for stage, chosen, exists in ((1, around, None), (2, north, links[2][2]), (3, upper, links[0][2])):
        guarded(exists, lambda stage=stage, chosen=chosen: pl.semaphore_wait(ready.at[stage - 1], count(chosen)))
        for m in first + second:
            if m.stage == stage:
                m.start()

    settle(first, 1, recv_sem.at[0])

    tall = rows + TILE
    half = lax.broadcasted_iota(jnp.int32, (TILE, cols), 0) < TILE // 2
    lanes = lax.broadcasted_iota(jnp.int32, (tall, cols), 1)
    slot = lanes % GROUP
    left_half = slot < REACH
    blank = jnp.zeros((TILE, cols), jnp.float32)

    def joined(full, before, after):
        return jnp.concatenate([full, jnp.where(half, after, before)], axis=0)

    for s in range(2):
        for t in range(2):
            for n, (f, i, j) in enumerate(entries):
                r = TILE - j if t == 0 else j - 1
                halo[s, i - 1, f, r : r + 1, :] = edge_in[s, t, n : n + 1, :]

    def cell(l, f):
        if 0 <= l < levels:
            return joined(own[l, f], side_in[0, l, f], side_in[1, l, f])
        s, i = (0, -l) if l < 0 else (1, l - levels + 1)
        if i == REACH:
            return jnp.concatenate([last_in[s], blank], axis=0)
        full = face_in[s, near - i, f] if s == 0 else face_in[s, i - 1, f]
        return jnp.concatenate([full, halo[s, i - 1, f]], axis=0)

    def down(x):
        return pltpu.roll(x, 1, axis=0)

    def up_row(x):
        return pltpu.roll(x, tall - 1, axis=0)

    def right(x, by=1):
        return pltpu.roll(x, by, axis=1)

    def left(x, by=1):
        return pltpu.roll(x, cols - by, axis=1)

    before_b, after_b = 1, (2 if n_lon > 2 else 1)

    def strip_block(a, b):
        full = strip[...] if a == 0 and b == 0 else strip_full[a, b]
        return joined(full, strip_half[a, 0, b], strip_half[a, 1, b])

    def placed(blocks, f):
        turned = [right(blocks[a], (GROUP * levels * (n - f)) % cols) if n != f else blocks[a] for n, a in enumerate((1, 0, 2))]
        width = GROUP * levels
        return jnp.where(lanes < width, turned[0], jnp.where(lanes < 2 * width, turned[1], turned[2]))

    mine = [strip_block(a, 0) for a in range(3)]
    sides = []
    sides.append([jnp.where(left_half, strip_block(a, before_b), mine[a]) for a in range(3)])
    sides.append([jnp.where(left_half, mine[a], strip_block(a, after_b)) for a in range(3)])
    side_c, side_v = [], []
    for blocks in sides:
        c = [placed(blocks, k + 1) for k in range(3)]
        v = placed(blocks, 0)
        for _ in range(2):
            v = forward(v, c, [right(v, GROUP), down(v), right(v)], [left(v, GROUP), up_row(v), left(v)])
        side_c.append(c)
        side_v.append(v)

    def inserted(z, l):
        return right(z, (cols - REACH - GROUP * (l + REACH)) % cols)

    speeds = {l: [cell(l, k + 1) for k in range(3)] for l in range(-near, levels + near)}
    v = {l: cell(l, 0) for l in range(-REACH, levels + REACH)}
    for reach in (near, near - 1):
        v = {
            l: forward(v[l], speeds[l], [v[l - 1], down(v[l]), right(v[l])], [v[l + 1], up_row(v[l]), left(v[l])])
            for l in range(-reach, levels + reach)
        }
    fix = jnp.where(left_half, side_v[1], side_v[0])
    rim = (lanes < 2) | (lanes >= cols - 2)
    v = {l: jnp.where(rim, inserted(fix, l), v[l]) for l in v}
    for l in range(levels):
        state_v[l] = v[l][:rows]

    settle(second, 1, recv_sem.at[1])

    def seen_cell(l, i):
        g = l + beyond
        if 0 < g < span - 1:
            return joined(seen[g, i], seen_in[0, g - 1, i], seen_in[1, g - 1, i])
        return jnp.concatenate([seen[g, i], blank], axis=0)

    def seen_block(b, i):
        full = seen_strip[i] if b == 0 else seen_full[b - 1, i]
        return joined(full, seen_half[0, b, i], seen_half[1, b, i])

    side_q = []
    for side in range(2):
        known = []
        for i in range(2):
            if side == 0:
                known.append(jnp.where(left_half, seen_block(before_b, i), seen_block(0, i)))
            else:
                known.append(jnp.where(left_half, seen_block(0, i), seen_block(after_b, i)))
        p = known[0] * side_v[side] - known[1]
        c = side_c[side]
        low, up = shares(p, c)
        q = centre_of(c) * p + left(low[0], GROUP) + right(up[0], GROUP)
        q = q + up_row(low[1]) + down(up[1]) + left(low[2]) + right(up[2])
        low, up = shares(q, c)
        side_q.append((q, right(up[2]) if side == 0 else left(low[2])))
    fix = jnp.where(left_half, side_q[1][0], side_q[0][0])
    crossing = jnp.where(left_half, side_q[1][1], side_q[0][1])

    p = {l: seen_cell(l, 0) * v[l] - seen_cell(l, 1) for l in v}
    low, up = {}, {}
    for l in p:
        low[l], up[l] = shares(p[l], speeds[l])
    rim = (lanes < 1) | (lanes >= cols - 1)
    q = {}
    for l in range(-1, levels + 1):
        total = centre_of(speeds[l]) * p[l] + low[l + 1][0] + up[l - 1][0]
        total = total + up_row(low[l][1]) + down(up[l][1]) + left(low[l][2]) + right(up[l][2])
        q[l] = jnp.where(rim, inserted(fix, l), total)
    for l in q:
        low[l], up[l] = shares(q[l], speeds[l])
    for l in range(levels):
        total = centre_of(speeds[l]) * q[l] + low[l + 1][0] + up[l - 1][0]
        total = total + up_row(low[l][1]) + down(up[l][1])
        total = total + jnp.where(rim, inserted(crossing, l), 0.0)
        total = total + jnp.where(lanes >= cols - 1, 0.0, left(low[l][2])) + jnp.where(lanes < 1, 0.0, right(up[l][2]))
        adj_v[l] = total[:rows]

    settle(first + second, 0, send_sem)


def finish(state_v, adj_v, outer, state_hbm, adj_hbm, next_hbm, wide, nxt, out_sem):
    levels, rows, cols = state_v.shape
    flat_rows = levels * rows
    wide_cols = outer.shape[1]
    fine = wide_cols // cols
    outer_rows = outer.shape[0] // levels
    stores = [
        pltpu.make_async_copy(state_v, state_hbm, out_sem.at[0]),
        pltpu.make_async_copy(adj_v, adj_hbm, out_sem.at[1]),
    ]
    for store in stores:
        store.start()
    field = adj_v[...]

    table = (
        lax.broadcasted_iota(jnp.int32, (cols, wide_cols), 0)
        == lax.broadcasted_iota(jnp.int32, (cols, wide_cols), 1) // fine
    ).astype(jnp.float32).astype(jnp.bfloat16)
    halves = bf16_parts(field.reshape(flat_rows, cols), 2)
    spread = jnp.dot(
        jnp.concatenate([h.astype(jnp.bfloat16) for h in halves], axis=1),
        jnp.concatenate([table, table], axis=0),
        preferred_element_type=jnp.float32,
    )
    for k in range(fine):
        for c in range(fine):
            wide[c, pl.ds(k, flat_rows, stride=fine), :] = spread[:, c * cols : (c + 1) * cols]
    for level in range(levels):
        span = pl.ds(level * outer_rows, outer_rows)
        for c in range(fine):
            lanes = pl.ds(c * cols, cols)
            nxt[span, lanes] = (outer[span, lanes].astype(jnp.float32) - wide[c, span, :]).astype(jnp.bfloat16)
        store = pltpu.make_async_copy(nxt.at[span], next_hbm.at[span], out_sem.at[2 + level])
        store.start()
        stores.append(store)
    for store in stores:
        store.wait()


def shards(ends, outer_increment, courant, obs_column, obs_level, obs_value):
    levels, outer_rows, wide_cols = outer_increment.shape
    _, _, rows, cols = courant.shape
    flat_rows = levels * rows
    fine = wide_cols // cols
    lanes = 128
    observed = (obs_column.shape[0] // lanes, lanes)
    span = levels + 4
    assert 4 * levels * GROUP == cols and levels >= REACH and rows % TILE == 0 and ends[1] > 1
    f32, bf16 = jnp.float32, jnp.bfloat16
    outer_shape = (levels * outer_rows, wide_cols)
    vmem = pl.BlockSpec(memory_space=pltpu.VMEM)
    hbm = pl.BlockSpec(memory_space=pl.ANY)
    held = pl.pallas_call(
        functools.partial(kernel, ends),
        out_shape=(
            pltpu.VMEM((levels, rows, cols), f32),
            pltpu.VMEM((levels, rows, cols), f32),
            pltpu.VMEM(outer_shape, bf16),
        ),
        in_specs=[hbm] * 5,
        out_specs=(vmem,) * 3,
        scratch_shapes=[
            pltpu.VMEM(courant.shape, bf16),
            pltpu.VMEM(observed, jnp.int32),
            pltpu.VMEM(observed, jnp.int32),
            pltpu.VMEM(observed, f32),
            pltpu.VMEM((levels * outer_rows, cols), f32),
            pltpu.VMEM((levels, 4, rows, cols), f32),
            pltpu.VMEM((2, REACH - 1, 4, rows, cols), f32),
            pltpu.VMEM((2, rows, cols), f32),
            pltpu.VMEM((2, levels, 4, TILE, cols), f32),
            pltpu.VMEM((2, 2, 2 * TILE, cols), f32),
            pltpu.VMEM((2, 2, 2 * TILE, cols), f32),
            pltpu.VMEM((2, REACH - 1, 4, TILE, cols), f32),
            pltpu.VMEM((rows, cols), f32),
            pltpu.VMEM((3, 3, rows, cols), f32),
            pltpu.VMEM((3, 2, 3, TILE, cols), f32),
            pltpu.VMEM((span, 2, rows, cols), f32),
            pltpu.VMEM((2, span - 2, 2, TILE, cols), f32),
            pltpu.VMEM((2, rows, cols), f32),
            pltpu.VMEM((2, 2, rows, cols), f32),
            pltpu.VMEM((2, 3, 2, TILE, cols), f32),
            pltpu.VMEM((2048, 1, cols), f32),
            pltpu.SemaphoreType.DMA((5,)),
            pltpu.SemaphoreType.DMA,
            pltpu.SemaphoreType.DMA((2,)),
            pltpu.SemaphoreType.REGULAR((3,)),
        ],
        compiler_params=pltpu.CompilerParams(collective_id=0, has_side_effects=True),
    )(
        outer_increment.reshape(outer_shape),
        courant,
        obs_column.reshape(observed),
        obs_level.reshape(observed),
        obs_value.reshape(observed),
    )
    state, adjoint, following = pl.pallas_call(
        finish,
        out_shape=(
            jax.ShapeDtypeStruct((levels, rows, cols), f32),
            jax.ShapeDtypeStruct((levels, rows, cols), f32),
            jax.ShapeDtypeStruct(outer_shape, bf16),
        ),
        in_specs=[vmem] * 3,
        out_specs=(hbm,) * 3,
        scratch_shapes=[
            pltpu.VMEM((fine, levels * outer_rows, cols), f32),
            pltpu.VMEM(outer_shape, bf16),
            pltpu.SemaphoreType.DMA((2 + levels,)),
        ],
    )(*[pltpu.with_memory_space_constraint(x, pltpu.VMEM) for x in held])
    return state, adjoint, following.reshape(outer_increment.shape)


def solution(mesh):
    ends = tuple(mesh.shape[a] for a in ("lat", "lon", "lev"))
    block = P("lev", "lat", "lon")
    observed = P(("lat", "lon"))
    return jax.shard_map(
        functools.partial(shards, ends),
        mesh=mesh,
        in_specs=(block, P(None, "lev", "lat", "lon"), observed, observed, observed),
        out_specs=(block, block, block),
        check_vma=False,
    )
```

```python
import functools

import jax
import jax.numpy as jnp
from jax import lax
from jax.experimental import pallas as pl
from jax.experimental.pallas import tpu as pltpu
from jax.sharding import PartitionSpec as P

MESH = pl.DeviceIdType.MESH
REACH = 4
GROUP = 2 * REACH
TILE = 8


def bf16_parts(x, count):
    parts = []
    for _ in range(count):
        part = x.astype(jnp.bfloat16).astype(jnp.float32)
        parts.append(part)
        x = x - part
    return parts


def forward(v, c, minus, plus):
    sizes = [jnp.abs(n) for n in c]
    result = (1.0 - sizes[0] - sizes[1] - sizes[2]) * v
    for k in range(3):
        result = result + sizes[k] * jnp.where(c[k] > 0.0, minus[k], plus[k])
    return result


def shares(p, c):
    low, up = [], []
    for n in c:
        moved = jnp.abs(n) * p
        low.append(jnp.where(n > 0.0, moved, 0.0))
        up.append(jnp.where(n > 0.0, 0.0, moved))
    return low, up


def centre_of(c):
    return 1.0 - jnp.abs(c[0]) - jnp.abs(c[1]) - jnp.abs(c[2])


def kernel(
    ends, outer_hbm, courant_hbm, col_hbm, lvl_hbm, val_hbm,
    state_v, adj_v, outer,
    courant, col, lvl, val, sums,
    own, face_in, deep_out, deep_in, side_in, edge_out, edge_in, halo,
    strip, strip_full, strip_half,
    seen, seen_in, seen_strip, seen_full, seen_half, units,
    in_sem, send_sem, recv_sem, ready,
):
    n_lat, n_lon, n_lev = ends
    levels, rows, cols = state_v.shape
    flat_rows = levels * rows
    wide_cols = outer.shape[1]
    fine = wide_cols // cols
    near = REACH - 1
    span = seen.shape[0]
    beyond = (span - levels) // 2

    me_lat, me_lon, me_lev = (lax.axis_index(a) for a in ("lat", "lon", "lev"))
    links = (
        ("lev", me_lev + 1, me_lev < n_lev - 1),
        ("lev", me_lev - 1, me_lev > 0),
        ("lat", me_lat + 1, me_lat < n_lat - 1),
        ("lat", me_lat - 1, me_lat > 0),
        ("lon", lax.rem(me_lon + 1, n_lon), None),
        ("lon", lax.rem(me_lon + n_lon - 1, n_lon), None),
    )
    turns = (0, 1) if n_lon > 2 else (0,)
    bands = ((rows - TILE, TILE), (0, TILE))

    def both(flags):
        return functools.reduce(jnp.logical_and, flags) if flags else None

    def guarded(exists, action):
        if exists is None:
            action()
        else:
            pl.when(exists)(action)

    def stage_of(which):
        if 0 in which:
            return 3 if len(which) == 1 else 4
        if 1 in which:
            return 1 if len(which) == 3 else 0
        return 2 if 2 in which else 0

    class Message:
        def __init__(self, which, source, landing, sem, stage=None):
            self.needs = tuple(w for w in which if w < 4)
            self.stage = stage_of(which) if stage is None else stage
            self.target = {links[w][0]: links[w][1] for w in which}
            self.exists = both([links[w][2] for w in self.needs])
            self.arrives = both([links[w ^ 1][2] for w in self.needs])
            self.source, self.landing, self.sem = source, landing, sem

        def start(self):
            def begin():
                pltpu.make_async_remote_copy(
                    src_ref=self.source, dst_ref=self.landing, send_sem=send_sem, recv_sem=recv_sem.at[self.sem],
                    device_id=self.target, device_id_type=MESH,
                ).start()

            guarded(self.exists, begin)

        def lines(self):
            total = 1
            for n in self.landing.shape:
                total = total * n
            return total // cols

    partners, first, second = [], [], []
    for a in (2, 1, 0):
        for t in (0, 1, None):
            for u in turns + (None,):
                which = [a - 1] if a else []
                which = which + ([2 + t] if t is not None else []) + ([4 + u] if u is not None else [])
                if not which:
                    continue
                partners.append(which)
                b = 0 if u is None else u + 1
                if t is None:
                    first.append(Message(which, strip, strip_full.at[a, b], 0))
                else:
                    first.append(Message(which, strip.at[pl.ds(*bands[t])], strip_half.at[a, t, b], 0))
                if u is None:
                    if a and t is None:
                        begin = levels - near + 1 if a == 1 else 0
                        first.append(Message(which, own.at[pl.ds(begin, near - 1)], face_in.at[a - 1], 0))
                        first.append(Message(which, deep_out.at[a - 1], deep_in.at[a - 1], 0, 1 if a == 2 else 4))
                    elif a:
                        first.append(Message(which, edge_out.at[a - 1, t], edge_in.at[a - 1, t], 0))
                    else:
                        first.append(Message(which, own.at[:, :, pl.ds(*bands[t])], side_in.at[t], 0))
                if not a:
                    if t is None:
                        second.append(Message(which, seen_strip, seen_full.at[u], 1))
                    else:
                        second.append(Message(which, seen_strip.at[:, pl.ds(*bands[t])], seen_half.at[t, b], 1))
                    if u is None:
                        kept = pl.ds(1, span - 2)
                        second.append(Message(which, seen.at[kept, :, pl.ds(*bands[t])], seen_in.at[t], 1))
    first.sort(key=lambda m: m.lines() - 64 * len(m.target))

    def count(chosen):
        return sum(
            1 if flags is None else flags.astype(jnp.int32)
            for flags in (both([links[w][2] for w in which if w < 4]) for which in chosen)
        )

    def signal(sem, chosen):
        for which in chosen:
            target = {links[w][0]: links[w][1] for w in which}
            guarded(
                both([links[w][2] for w in which if w < 4]),
                lambda target=target: pl.semaphore_signal(sem, inc=1, device_id=target, device_id_type=MESH),
            )

    barrier = pltpu.get_barrier_semaphore()
    near_by = [which for which in partners if len(which) < 3 or not {0, 1} & set(which)]
    lower = sorted([which for which in near_by if 1 in which], key=len)
    upper = sorted([which for which in near_by if 0 in which], key=len)
    level = [which for which in near_by if which not in lower + upper]
    north = [which for which in level if 2 in which]
    south = [which for which in level if 3 in which]
    around = [which for which in level if which not in north + south]
    signal(barrier, upper + north + around)

    loads = [
        pltpu.make_async_copy(src, dst, in_sem.at[i])
        for i, (src, dst) in enumerate(
            ((outer_hbm, outer), (courant_hbm, courant), (col_hbm, col), (lvl_hbm, lvl), (val_hbm, val))
        )
    ]
    for load in loads:
        load.start()

    def settle(messages, flip, sem, known=()):
        if len(known) < 4:
            for has in (True, False):
                flag = links[len(known)][2]
                pl.when(flag if has else jnp.logical_not(flag))(
                    lambda has=has: settle(messages, flip, sem, known + (has,))
                )
            return
        total = sum(m.lines() for m in messages if all(known[w ^ flip] for w in m.needs))
        view = units.at[pl.ds(0, total)]
        pltpu.make_async_copy(view, view, sem).wait()

    def clear(ref):
        ref[...] = jnp.zeros(ref.shape, jnp.float32)

    for m in first + second:
        if m.arrives is not None:
            pl.when(jnp.logical_not(m.arrives))(lambda m=m: clear(m.landing))
    clear(halo)

    lane = lax.broadcasted_iota(jnp.int32, (rows, cols), 1)
    group = lane // GROUP
    pool = (
        lax.broadcasted_iota(jnp.int32, (wide_cols, cols), 0) // fine
        == lax.broadcasted_iota(jnp.int32, (wide_cols, cols), 1)
    ).astype(jnp.float32).astype(jnp.bfloat16)

    loads[1].wait()
    for k in range(3):
        own[:, k + 1] = courant[k].astype(jnp.float32)
    loads[0].wait()
    sums[...] = jnp.dot(outer[...], pool, preferred_element_type=jnp.float32)
    coarse = sums[pl.ds(0, flat_rows, stride=fine), :]
    for k in range(1, fine):
        coarse = coarse + sums[pl.ds(k, flat_rows, stride=fine), :]
    own[:, 0] = (coarse * (1.0 / (fine * fine))).reshape(levels, rows, cols)

    ends_only = jnp.zeros((rows, cols), jnp.float32)
    for f in (1, 2, 3, 0):
        for l in range(levels):
            place = f * levels + l
            ends_only = jnp.where(group == place, pltpu.roll(own[l, f], (REACH + GROUP * place) % cols, axis=1), ends_only)
    strip[...] = ends_only

    entries = [(0, i, j) for i in range(1, REACH) for j in range(1, REACH + 1 - i)]
    entries = entries + [(f, i, j) for f in (1, 2, 3) for i in range(1, near) for j in range(1, near + 1 - i)]
    for s in range(2):
        for t in range(2):
            for n, (f, i, j) in enumerate(entries):
                l = levels - i if s == 0 else i - 1
                r = rows - j if t == 0 else j - 1
                edge_out[s, t, n : n + 1, :] = own[l, f, r : r + 1, :]

    pl.semaphore_wait(barrier, count(lower + south + around))
    signal(ready.at[0], around)
    signal(ready.at[2], lower[:1])
    signal(ready.at[3], lower[1:])
    signal(ready.at[1], south)
    for m in first:
        if m.stage == 0:
            m.start()

    row = lax.broadcasted_iota(jnp.int32, (rows, cols), 0)
    for s in range(2):
        l = levels - near if s == 0 else near - 1
        v = own[l, 0]
        c = [own[l, k + 1] for k in range(3)]
        above = jnp.where(row == 0, 0.0, pltpu.roll(v, 1, axis=0))
        below = jnp.where(row == rows - 1, 0.0, pltpu.roll(v, rows - 1, axis=0))
        deep_out[s, 0] = v
        deep_out[s, 1] = forward(
            v, c, [own[l - 1, 0], above, pltpu.roll(v, 1, axis=1)], [own[l + 1, 0], below, pltpu.roll(v, cols - 1, axis=1)]
        )
        deep_out[s, 2] = c[1]

    for load in loads[2:]:
        load.wait()
    where_row = (lvl[...] - me_lev * levels + beyond) * rows + col[...] // cols
    where_col = col[...] % cols
    parts = bf16_parts(val[...], 2)
    pieces, width = col.shape
    row_id = lax.broadcasted_iota(jnp.int32, (span * rows, width), 0)
    col_id = lax.broadcasted_iota(jnp.int32, (cols, width), 0)
    hits = [[] for _ in range(3)]
    tables = []
    for k in range(pieces):
        match = where_row[k : k + 1] == row_id
        hits[0].append(jnp.where(match, 1.0, 0.0).astype(jnp.bfloat16))
        for i, part in enumerate(parts):
            hits[i + 1].append(jnp.where(match, part[k : k + 1], 0.0).astype(jnp.bfloat16))
        tables.append(jnp.where(where_col[k : k + 1] == col_id, 1.0, 0.0).astype(jnp.bfloat16))
    left_side = jnp.concatenate([jnp.concatenate(h, axis=1) for h in hits], axis=0)
    totals = lax.dot_general(
        left_side, jnp.concatenate(tables, axis=1), (((1,), (1,)), ((), ())),
        preferred_element_type=jnp.float32,
    )
    wide_rows = span * rows
    counted = totals[:wide_rows].reshape(span, rows, cols)
    summed = (totals[wide_rows : 2 * wide_rows] + totals[2 * wide_rows :]).reshape(span, rows, cols)
    seen[:, 0] = counted
    seen[:, 1] = summed
    for i, values in enumerate((counted, summed)):
        ends_only = jnp.zeros((rows, cols), jnp.float32)
        for g in range(span):
            place = g + REACH - beyond
            ends_only = jnp.where(group == place, pltpu.roll(values[g], (REACH + GROUP * place) % cols, axis=1), ends_only)
        seen_strip[i] = ends_only
    for m in second:
        if m.stage == 0:
            m.start()
    for stage, chosen, exists in ((1, around, None), (2, north, links[2][2]), (3, upper[:1], links[0][2]), (4, upper[1:], links[0][2])):
        guarded(exists, lambda stage=stage, chosen=chosen: pl.semaphore_wait(ready.at[stage - 1], count(chosen)))
        for m in first + second:
            if m.stage == stage:
                m.start()

    settle(first, 1, recv_sem.at[0])

    tall = rows + TILE
    half = lax.broadcasted_iota(jnp.int32, (TILE, cols), 0) < TILE // 2
    lanes = lax.broadcasted_iota(jnp.int32, (tall, cols), 1)
    slot = lanes % GROUP
    left_half = slot < REACH
    blank = jnp.zeros((TILE, cols), jnp.float32)

    def joined(full, before, after):
        return jnp.concatenate([full, jnp.where(half, after, before)], axis=0)

    for s in range(2):
        for t in range(2):
            for n, (f, i, j) in enumerate(entries):
                r = TILE - j if t == 0 else j - 1
                halo[s, i - 1, f, r : r + 1, :] = edge_in[s, t, n : n + 1, :]

    def cell(l, f):
        if 0 <= l < levels:
            return joined(own[l, f], side_in[0, l, f], side_in[1, l, f])
        s, i = (0, -l) if l < 0 else (1, l - levels + 1)
        if i == near:
            return jnp.concatenate([deep_in[s, f], halo[s, i - 1, f]], axis=0)
        full = face_in[s, near - 1 - i, f] if s == 0 else face_in[s, i - 1, f]
        return jnp.concatenate([full, halo[s, i - 1, f]], axis=0)

    def down(x):
        return pltpu.roll(x, 1, axis=0)

    def up_row(x):
        return pltpu.roll(x, tall - 1, axis=0)

    def right(x, by=1):
        return pltpu.roll(x, by, axis=1)

    def left(x, by=1):
        return pltpu.roll(x, cols - by, axis=1)

    before_b, after_b = 1, (2 if n_lon > 2 else 1)

    def strip_block(a, b):
        full = strip[...] if a == 0 and b == 0 else strip_full[a, b]
        return joined(full, strip_half[a, 0, b], strip_half[a, 1, b])

    def placed(blocks, f):
        turned = [right(blocks[a], (GROUP * levels * (n - f)) % cols) if n != f else blocks[a] for n, a in enumerate((1, 0, 2))]
        width = GROUP * levels
        return jnp.where(lanes < width, turned[0], jnp.where(lanes < 2 * width, turned[1], turned[2]))

    mine = [strip_block(a, 0) for a in range(3)]
    sides = []
    sides.append([jnp.where(left_half, strip_block(a, before_b), mine[a]) for a in range(3)])
    sides.append([jnp.where(left_half, mine[a], strip_block(a, after_b)) for a in range(3)])
    side_c, side_v = [], []
    for blocks in sides:
        c = [placed(blocks, k + 1) for k in range(3)]
        v = placed(blocks, 0)
        for _ in range(2):
            v = forward(v, c, [right(v, GROUP), down(v), right(v)], [left(v, GROUP), up_row(v), left(v)])
        side_c.append(c)
        side_v.append(v)

    def inserted(z, l):
        return right(z, (cols - REACH - GROUP * (l + REACH)) % cols)

    speeds = {l: [cell(l, k + 1) for k in range(3)] for l in range(1 - near, levels + near - 1)}
    start = {l: cell(l, 0) for l in range(-near, levels + near)}

    def step(v, l):
        return forward(v[l], speeds[l], [v[l - 1], down(v[l]), right(v[l])], [v[l + 1], up_row(v[l]), left(v[l])])

    v = {l: step(start, l) for l in speeds}
    for s in range(2):
        l = -near if s == 0 else levels + near - 1
        c = deep_in[s, 2]
        above = jnp.where((row == 0) & (c > 0.0), down(start[l])[:rows], 0.0)
        below = jnp.where((row == rows - 1) & (c <= 0.0), up_row(start[l])[:rows], 0.0)
        v[l] = jnp.concatenate([deep_in[s, 1] + jnp.abs(c) * (above + below), blank], axis=0)
    v = {l: step(v, l) for l in speeds}
    fix = jnp.where(left_half, side_v[1], side_v[0])
    rim = (lanes < 2) | (lanes >= cols - 2)
    v = {l: jnp.where(rim, inserted(fix, l), v[l]) for l in v}
    for l in range(levels):
        state_v[l] = v[l][:rows]

    settle(second, 1, recv_sem.at[1])

    def seen_cell(l, i):
        g = l + beyond
        if 0 < g < span - 1:
            return joined(seen[g, i], seen_in[0, g - 1, i], seen_in[1, g - 1, i])
        return jnp.concatenate([seen[g, i], blank], axis=0)

    def seen_block(b, i):
        full = seen_strip[i] if b == 0 else seen_full[b - 1, i]
        return joined(full, seen_half[0, b, i], seen_half[1, b, i])

    side_q = []
    for side in range(2):
        known = []
        for i in range(2):
            if side == 0:
                known.append(jnp.where(left_half, seen_block(before_b, i), seen_block(0, i)))
            else:
                known.append(jnp.where(left_half, seen_block(0, i), seen_block(after_b, i)))
        p = known[0] * side_v[side] - known[1]
        c = side_c[side]
        low, up = shares(p, c)
        q = centre_of(c) * p + left(low[0], GROUP) + right(up[0], GROUP)
        q = q + up_row(low[1]) + down(up[1]) + left(low[2]) + right(up[2])
        low, up = shares(q, c)
        side_q.append((q, right(up[2]) if side == 0 else left(low[2])))
    fix = jnp.where(left_half, side_q[1][0], side_q[0][0])
    crossing = jnp.where(left_half, side_q[1][1], side_q[0][1])

    p = {l: seen_cell(l, 0) * v[l] - seen_cell(l, 1) for l in v}
    low, up = {}, {}
    for l in p:
        low[l], up[l] = shares(p[l], speeds[l])
    rim = (lanes < 1) | (lanes >= cols - 1)
    q = {}
    for l in range(-1, levels + 1):
        total = centre_of(speeds[l]) * p[l] + low[l + 1][0] + up[l - 1][0]
        total = total + up_row(low[l][1]) + down(up[l][1]) + left(low[l][2]) + right(up[l][2])
        q[l] = jnp.where(rim, inserted(fix, l), total)
    for l in q:
        low[l], up[l] = shares(q[l], speeds[l])
    for l in range(levels):
        total = centre_of(speeds[l]) * q[l] + low[l + 1][0] + up[l - 1][0]
        total = total + up_row(low[l][1]) + down(up[l][1])
        total = total + jnp.where(rim, inserted(crossing, l), 0.0)
        total = total + jnp.where(lanes >= cols - 1, 0.0, left(low[l][2])) + jnp.where(lanes < 1, 0.0, right(up[l][2]))
        adj_v[l] = total[:rows]

    settle(first + second, 0, send_sem)


def finish(state_v, adj_v, outer, state_hbm, adj_hbm, next_hbm, wide, nxt, out_sem):
    levels, rows, cols = state_v.shape
    flat_rows = levels * rows
    wide_cols = outer.shape[1]
    fine = wide_cols // cols
    outer_rows = outer.shape[0] // levels
    stores = [
        pltpu.make_async_copy(state_v, state_hbm, out_sem.at[0]),
        pltpu.make_async_copy(adj_v, adj_hbm, out_sem.at[1]),
    ]
    for store in stores:
        store.start()
    field = adj_v[...]

    table = (
        lax.broadcasted_iota(jnp.int32, (cols, wide_cols), 0)
        == lax.broadcasted_iota(jnp.int32, (cols, wide_cols), 1) // fine
    ).astype(jnp.float32).astype(jnp.bfloat16)
    halves = bf16_parts(field.reshape(flat_rows, cols), 2)
    spread = jnp.dot(
        jnp.concatenate([h.astype(jnp.bfloat16) for h in halves], axis=1),
        jnp.concatenate([table, table], axis=0),
        preferred_element_type=jnp.float32,
    )
    for k in range(fine):
        for c in range(fine):
            wide[c, pl.ds(k, flat_rows, stride=fine), :] = spread[:, c * cols : (c + 1) * cols]
    for level in range(levels):
        span = pl.ds(level * outer_rows, outer_rows)
        for c in range(fine):
            lanes = pl.ds(c * cols, cols)
            nxt[span, lanes] = (outer[span, lanes].astype(jnp.float32) - wide[c, span, :]).astype(jnp.bfloat16)
        store = pltpu.make_async_copy(nxt.at[span], next_hbm.at[span], out_sem.at[2 + level])
        store.start()
        stores.append(store)
    for store in stores:
        store.wait()


def shards(ends, outer_increment, courant, obs_column, obs_level, obs_value):
    levels, outer_rows, wide_cols = outer_increment.shape
    _, _, rows, cols = courant.shape
    flat_rows = levels * rows
    fine = wide_cols // cols
    lanes = 128
    observed = (obs_column.shape[0] // lanes, lanes)
    span = levels + 4
    assert 4 * levels * GROUP == cols and levels >= REACH and rows % TILE == 0 and ends[1] > 1
    f32, bf16 = jnp.float32, jnp.bfloat16
    outer_shape = (levels * outer_rows, wide_cols)
    vmem = pl.BlockSpec(memory_space=pltpu.VMEM)
    hbm = pl.BlockSpec(memory_space=pl.ANY)
    held = pl.pallas_call(
        functools.partial(kernel, ends),
        out_shape=(
            pltpu.VMEM((levels, rows, cols), f32),
            pltpu.VMEM((levels, rows, cols), f32),
            pltpu.VMEM(outer_shape, bf16),
        ),
        in_specs=[hbm] * 5,
        out_specs=(vmem,) * 3,
        scratch_shapes=[
            pltpu.VMEM(courant.shape, bf16),
            pltpu.VMEM(observed, jnp.int32),
            pltpu.VMEM(observed, jnp.int32),
            pltpu.VMEM(observed, f32),
            pltpu.VMEM((levels * outer_rows, cols), f32),
            pltpu.VMEM((levels, 4, rows, cols), f32),
            pltpu.VMEM((2, REACH - 2, 4, rows, cols), f32),
            pltpu.VMEM((2, 3, rows, cols), f32),
            pltpu.VMEM((2, 3, rows, cols), f32),
            pltpu.VMEM((2, levels, 4, TILE, cols), f32),
            pltpu.VMEM((2, 2, 2 * TILE, cols), f32),
            pltpu.VMEM((2, 2, 2 * TILE, cols), f32),
            pltpu.VMEM((2, REACH - 1, 4, TILE, cols), f32),
            pltpu.VMEM((rows, cols), f32),
            pltpu.VMEM((3, 3, rows, cols), f32),
            pltpu.VMEM((3, 2, 3, TILE, cols), f32),
            pltpu.VMEM((span, 2, rows, cols), f32),
            pltpu.VMEM((2, span - 2, 2, TILE, cols), f32),
            pltpu.VMEM((2, rows, cols), f32),
            pltpu.VMEM((2, 2, rows, cols), f32),
            pltpu.VMEM((2, 3, 2, TILE, cols), f32),
            pltpu.VMEM((2048, 1, cols), f32),
            pltpu.SemaphoreType.DMA((5,)),
            pltpu.SemaphoreType.DMA,
            pltpu.SemaphoreType.DMA((2,)),
            pltpu.SemaphoreType.REGULAR((4,)),
        ],
        compiler_params=pltpu.CompilerParams(collective_id=0, has_side_effects=True),
    )(
        outer_increment.reshape(outer_shape),
        courant,
        obs_column.reshape(observed),
        obs_level.reshape(observed),
        obs_value.reshape(observed),
    )
    state, adjoint, following = pl.pallas_call(
        finish,
        out_shape=(
            jax.ShapeDtypeStruct((levels, rows, cols), f32),
            jax.ShapeDtypeStruct((levels, rows, cols), f32),
            jax.ShapeDtypeStruct(outer_shape, bf16),
        ),
        in_specs=[vmem] * 3,
        out_specs=(hbm,) * 3,
        scratch_shapes=[
            pltpu.VMEM((fine, levels * outer_rows, cols), f32),
            pltpu.VMEM(outer_shape, bf16),
            pltpu.SemaphoreType.DMA((2 + levels,)),
        ],
    )(*[pltpu.with_memory_space_constraint(x, pltpu.VMEM) for x in held])
    return state, adjoint, following.reshape(outer_increment.shape)


def solution(mesh):
    ends = tuple(mesh.shape[a] for a in ("lat", "lon", "lev"))
    block = P("lev", "lat", "lon")
    observed = P(("lat", "lon"))
    return jax.shard_map(
        functools.partial(shards, ends),
        mesh=mesh,
        in_specs=(block, P(None, "lev", "lat", "lon"), observed, observed, observed),
        out_specs=(block, block, block),
        check_vma=False,
    )
```

```python
import functools

import jax
import jax.numpy as jnp
from jax import lax
from jax.experimental import pallas as pl
from jax.experimental.pallas import tpu as pltpu
from jax.sharding import PartitionSpec as P

MESH = pl.DeviceIdType.MESH
REACH = 4
GROUP = 2 * REACH
TILE = 8


def bf16_parts(x, count):
    parts = []
    for _ in range(count):
        part = x.astype(jnp.bfloat16).astype(jnp.float32)
        parts.append(part)
        x = x - part
    return parts


def forward(v, c, minus, plus):
    sizes = [jnp.abs(n) for n in c]
    result = (1.0 - sizes[0] - sizes[1] - sizes[2]) * v
    for k in range(3):
        result = result + sizes[k] * jnp.where(c[k] > 0.0, minus[k], plus[k])
    return result


def shares(p, c):
    low, up = [], []
    for n in c:
        moved = jnp.abs(n) * p
        low.append(jnp.where(n > 0.0, moved, 0.0))
        up.append(jnp.where(n > 0.0, 0.0, moved))
    return low, up


def centre_of(c):
    return 1.0 - jnp.abs(c[0]) - jnp.abs(c[1]) - jnp.abs(c[2])


def kernel(
    ends, outer_hbm, courant_hbm, col_hbm, lvl_hbm, val_hbm,
    state_v, adj_v, outer,
    courant, col, lvl, val, sums,
    own, face_in, deep_out, deep_in, side_in, edge_out, edge_in, halo,
    strip, strip_full, strip_half,
    seen, seen_in, seen_strip, seen_full, seen_half, units,
    in_sem, send_sem, recv_sem, ready,
):
    n_lat, n_lon, n_lev = ends
    levels, rows, cols = state_v.shape
    flat_rows = levels * rows
    wide_cols = outer.shape[1]
    fine = wide_cols // cols
    near = REACH - 1
    span = seen.shape[0]
    beyond = (span - levels) // 2

    loads = [
        pltpu.make_async_copy(src, dst, in_sem.at[i])
        for i, (src, dst) in enumerate(
            ((outer_hbm, outer), (courant_hbm, courant), (col_hbm, col), (lvl_hbm, lvl), (val_hbm, val))
        )
    ]
    for load in loads:
        load.start()

    me_lat, me_lon, me_lev = (lax.axis_index(a) for a in ("lat", "lon", "lev"))
    links = (
        ("lev", me_lev + 1, me_lev < n_lev - 1),
        ("lev", me_lev - 1, me_lev > 0),
        ("lat", me_lat + 1, me_lat < n_lat - 1),
        ("lat", me_lat - 1, me_lat > 0),
        ("lon", lax.rem(me_lon + 1, n_lon), None),
        ("lon", lax.rem(me_lon + n_lon - 1, n_lon), None),
    )
    turns = (0, 1) if n_lon > 2 else (0,)
    bands = ((rows - TILE, TILE), (0, TILE))

    def both(flags):
        return functools.reduce(jnp.logical_and, flags) if flags else None

    def guarded(exists, action):
        if exists is None:
            action()
        else:
            pl.when(exists)(action)

    def flags_of(which):
        return [links[w][2] for w in which if w < 4]

    def lon_of(which):
        return [w for w in which if w > 3]

    def is_ahead(which):
        return me_lon < links[lon_of(which)[0]][1]

    def is_behind(which):
        return me_lon > links[lon_of(which)[0]][1]

    class Message:
        def __init__(self, which, source, landing, sem, later=False):
            self.which, self.later = which, later
            self.needs = tuple(w for w in which if w < 4)
            self.target = {links[w][0]: links[w][1] for w in which}
            self.arrives = both([links[w ^ 1][2] for w in self.needs])
            self.source, self.landing, self.sem = source, landing, sem

        def start(self, flag=None):
            def begin():
                pltpu.make_async_remote_copy(
                    src_ref=self.source, dst_ref=self.landing, send_sem=send_sem, recv_sem=recv_sem.at[self.sem],
                    device_id=self.target, device_id_type=MESH,
                ).start()

            guarded(both(flags_of(self.which) + ([] if flag is None else [flag])), begin)

        def lines(self):
            total = 1
            for n in self.landing.shape:
                total = total * n
            return total // cols

    partners, first, second, faces = [], [], [], []
    for a in (2, 1, 0):
        for t in (0, 1, None):
            for u in turns + (None,):
                which = [a - 1] if a else []
                which = which + ([2 + t] if t is not None else []) + ([4 + u] if u is not None else [])
                if not which:
                    continue
                partners.append(which)
                b = 0 if u is None else u + 1
                if t is None:
                    first.append(Message(which, strip, strip_full.at[a, b], 0))
                else:
                    first.append(Message(which, strip.at[pl.ds(*bands[t])], strip_half.at[a, t, b], 0))
                if u is None:
                    if a and t is None:
                        for i in range(1, near):
                            l, place = (levels - i, near - 1 - i) if a == 1 else (i - 1, i - 1)
                            faces.append(Message(which, own.at[l], face_in.at[a - 1, place], 2, i > 1))
                        faces.append(Message(which, deep_out.at[a - 1], deep_in.at[a - 1], 2, True))
                    elif a:
                        first.append(Message(which, edge_out.at[a - 1, t], edge_in.at[a - 1, t], 0))
                    else:
                        faces.append(Message(which, own.at[:, :, pl.ds(*bands[t])], side_in.at[t], 2))
                if not a:
                    if t is None:
                        second.append(Message(which, seen_strip, seen_full.at[u], 1))
                    else:
                        second.append(Message(which, seen_strip.at[:, pl.ds(*bands[t])], seen_half.at[t, b], 1))
                    if u is None:
                        kept = pl.ds(1, span - 2)
                        second.append(Message(which, seen.at[kept, :, pl.ds(*bands[t])], seen_in.at[t], 1))
    first.sort(key=lambda m: -len(m.target))

    def pick(test, side=None):
        return [(which, None if side is None else side(which)) for which in partners if test(which)]

    def count(chosen):
        total = 0
        for which, flag in chosen:
            exists = both(flags_of(which) + ([] if flag is None else [flag]))
            total = total + (1 if exists is None else exists.astype(jnp.int32))
        return total

    def signal(sem, chosen):
        for which, flag in chosen:
            target = {links[w][0]: links[w][1] for w in which}
            guarded(
                both(flags_of(which) + ([] if flag is None else [flag])),
                lambda target=target: pl.semaphore_signal(sem, inc=1, device_id=target, device_id_type=MESH),
            )

    def level_lon(which):
        return lon_of(which) and not {0, 1} & set(which)

    def corner(which):
        return len(which) == 3

    lower = pick(lambda w: 1 in w and not corner(w))
    upper = pick(lambda w: 0 in w and not corner(w))
    lower_face, upper_face = [[c for c in side if len(c[0]) == 1] for side in (lower, upper)]
    lower_rest, upper_rest = [[c for c in side if len(c[0]) > 1] for side in (lower, upper)]
    lower_south = pick(lambda w: corner(w) and 1 in w and 3 in w)
    upper_north = pick(lambda w: corner(w) and 0 in w and 2 in w)
    south, north = pick(lambda w: w == [3]), pick(lambda w: w == [2])
    behind, ahead = pick(level_lon, is_behind), pick(level_lon, is_ahead)

    barrier = pltpu.get_barrier_semaphore()
    signal(barrier, upper_north + upper_rest + upper_face + ahead + north)

    def settle(messages, flip, sem, known=()):
        if len(known) < 4:
            for has in (True, False):
                flag = links[len(known)][2]
                pl.when(flag if has else jnp.logical_not(flag))(
                    lambda has=has: settle(messages, flip, sem, known + (has,))
                )
            return
        total = sum(m.lines() for m in messages if all(known[w ^ flip] for w in m.needs))
        view = units.at[pl.ds(0, total)]
        pltpu.make_async_copy(view, view, sem).wait()

    def clear(ref):
        ref[...] = jnp.zeros(ref.shape, jnp.float32)

    for m in first + second + faces:
        if m.arrives is not None:
            pl.when(jnp.logical_not(m.arrives))(lambda m=m: clear(m.landing))
    clear(halo)

    lane = lax.broadcasted_iota(jnp.int32, (rows, cols), 1)
    group = lane // GROUP
    pool = (
        lax.broadcasted_iota(jnp.int32, (wide_cols, cols), 0) // fine
        == lax.broadcasted_iota(jnp.int32, (wide_cols, cols), 1)
    ).astype(jnp.float32).astype(jnp.bfloat16)

    loads[1].wait()
    for k in range(3):
        own[:, k + 1] = courant[k].astype(jnp.float32)
    loads[0].wait()
    sums[...] = jnp.dot(outer[...], pool, preferred_element_type=jnp.float32)
    coarse = sums[pl.ds(0, flat_rows, stride=fine), :]
    for k in range(1, fine):
        coarse = coarse + sums[pl.ds(k, flat_rows, stride=fine), :]
    own[:, 0] = (coarse * (1.0 / (fine * fine))).reshape(levels, rows, cols)

    ends_only = jnp.zeros((rows, cols), jnp.float32)
    for f in (1, 2, 3, 0):
        for l in range(levels):
            place = f * levels + l
            ends_only = jnp.where(group == place, pltpu.roll(own[l, f], (REACH + GROUP * place) % cols, axis=1), ends_only)
    strip[...] = ends_only

    entries = [(0, i, j) for i in range(1, REACH) for j in range(1, REACH + 1 - i)]
    entries = entries + [(f, i, j) for f in (1, 2, 3) for i in range(1, near) for j in range(1, near + 1 - i)]
    for s in range(2):
        for t in range(2):
            for n, (f, i, j) in enumerate(entries):
                l = levels - i if s == 0 else i - 1
                r = rows - j if t == 0 else j - 1
                edge_out[s, t, n : n + 1, :] = own[l, f, r : r + 1, :]

    def send(messages, test, side=None, later=False):
        for m in messages:
            if test(m.which) and m.later == later:
                m.start(None if side is None else side(m.which))

    def at_once(w):
        return (1 in w and not (corner(w) and 2 in w)) or w == [3]

    def to_north(w):
        return w == [2] or (corner(w) and 1 in w and 2 in w)

    expected = count(lower + lower_south + south + behind)
    pl.when(expected > 0)(lambda: pl.semaphore_wait(barrier, expected))
    signal(ready.at[3], lower_rest)
    signal(ready.at[0], behind)
    signal(ready.at[2], lower_face)
    signal(ready.at[1], south)
    signal(ready.at[4], [(w, is_behind(w)) for w, _ in lower_south])
    send(first, at_once)
    send(first, level_lon, is_behind)
    send(faces, at_once)

    row = lax.broadcasted_iota(jnp.int32, (rows, cols), 0)
    for s in range(2):
        l = levels - near if s == 0 else near - 1
        v = own[l, 0]
        c = [own[l, k + 1] for k in range(3)]
        above = jnp.where(row == 0, 0.0, pltpu.roll(v, 1, axis=0))
        below = jnp.where(row == rows - 1, 0.0, pltpu.roll(v, rows - 1, axis=0))
        deep_out[s, 0] = v
        deep_out[s, 1] = forward(
            v, c, [own[l - 1, 0], above, pltpu.roll(v, 1, axis=1)], [own[l + 1, 0], below, pltpu.roll(v, cols - 1, axis=1)]
        )
        deep_out[s, 2] = c[1]

    for load in loads[2:]:
        load.wait()
    where_row = (lvl[...] - me_lev * levels + beyond) * rows + col[...] // cols
    where_col = col[...] % cols
    parts = bf16_parts(val[...], 2)
    pieces, width = col.shape
    row_id = lax.broadcasted_iota(jnp.int32, (span * rows, width), 0)
    col_id = lax.broadcasted_iota(jnp.int32, (cols, width), 0)
    hits = [[] for _ in range(3)]
    tables = []
    for k in range(pieces):
        match = where_row[k : k + 1] == row_id
        hits[0].append(jnp.where(match, 1.0, 0.0).astype(jnp.bfloat16))
        for i, part in enumerate(parts):
            hits[i + 1].append(jnp.where(match, part[k : k + 1], 0.0).astype(jnp.bfloat16))
        tables.append(jnp.where(where_col[k : k + 1] == col_id, 1.0, 0.0).astype(jnp.bfloat16))
    left_side = jnp.concatenate([jnp.concatenate(h, axis=1) for h in hits], axis=0)
    totals = lax.dot_general(
        left_side, jnp.concatenate(tables, axis=1), (((1,), (1,)), ((), ())),
        preferred_element_type=jnp.float32,
    )
    wide_rows = span * rows
    counted = totals[:wide_rows].reshape(span, rows, cols)
    summed = (totals[wide_rows : 2 * wide_rows] + totals[2 * wide_rows :]).reshape(span, rows, cols)
    seen[:, 0] = counted
    seen[:, 1] = summed
    for i, values in enumerate((counted, summed)):
        ends_only = jnp.zeros((rows, cols), jnp.float32)
        for g in range(span):
            place = g + REACH - beyond
            ends_only = jnp.where(group == place, pltpu.roll(values[g], (REACH + GROUP * place) % cols, axis=1), ends_only)
        seen_strip[i] = ends_only
    send(second, at_once)
    send(second, level_lon, is_behind)

    def go_north():
        pl.semaphore_wait(ready.at[1], 1)
        send(first + faces + second, to_north)

    early = me_lon > 0
    pl.when(links[2][2] & early)(go_north)
    send(faces, at_once, later=True)
    pl.when(links[2][2] & jnp.logical_not(early))(go_north)

    @pl.when(me_lon < n_lon - 1)
    def _():
        pl.semaphore_wait(ready.at[0], count(ahead))
        send(first + second, level_lon, is_ahead)

    @pl.when(links[0][2])
    def _():
        pl.semaphore_wait(ready.at[2], 1)
        send(faces, lambda w: 0 in w)
        pl.semaphore_wait(ready.at[3], count(upper_rest))
        send(first, lambda w: 0 in w and not (corner(w) and 2 in w))
        send(first, lambda w: corner(w) and 0 in w and 2 in w, is_behind)
        send(faces, lambda w: 0 in w, later=True)

    @pl.when(links[0][2] & links[2][2] & (me_lon < n_lon - 1))
    def _():
        pl.semaphore_wait(ready.at[4], count([(w, is_ahead(w)) for w, _ in upper_north]))
        send(first, lambda w: corner(w) and 0 in w and 2 in w, is_ahead)

    settle(first, 1, recv_sem.at[0])
    settle(second, 1, recv_sem.at[1])

    tall = rows + TILE
    half = lax.broadcasted_iota(jnp.int32, (TILE, cols), 0) < TILE // 2
    lanes = lax.broadcasted_iota(jnp.int32, (tall, cols), 1)
    slot = lanes % GROUP
    left_half = slot < REACH
    blank = jnp.zeros((TILE, cols), jnp.float32)

    def joined(full, before, after):
        return jnp.concatenate([full, jnp.where(half, after, before)], axis=0)

    for s in range(2):
        for t in range(2):
            for n, (f, i, j) in enumerate(entries):
                r = TILE - j if t == 0 else j - 1
                halo[s, i - 1, f, r : r + 1, :] = edge_in[s, t, n : n + 1, :]

    def cell(l, f):
        if 0 <= l < levels:
            return joined(own[l, f], side_in[0, l, f], side_in[1, l, f])
        s, i = (0, -l) if l < 0 else (1, l - levels + 1)
        if i == near:
            return jnp.concatenate([deep_in[s, f], halo[s, i - 1, f]], axis=0)
        full = face_in[s, near - 1 - i, f] if s == 0 else face_in[s, i - 1, f]
        return jnp.concatenate([full, halo[s, i - 1, f]], axis=0)

    def down(x):
        return pltpu.roll(x, 1, axis=0)

    def up_row(x):
        return pltpu.roll(x, tall - 1, axis=0)

    def right(x, by=1):
        return pltpu.roll(x, by, axis=1)

    def left(x, by=1):
        return pltpu.roll(x, cols - by, axis=1)

    before_b, after_b = 1, (2 if n_lon > 2 else 1)

    def strip_block(a, b):
        full = strip[...] if a == 0 and b == 0 else strip_full[a, b]
        return joined(full, strip_half[a, 0, b], strip_half[a, 1, b])

    def placed(blocks, f):
        turned = [right(blocks[a], (GROUP * levels * (n - f)) % cols) if n != f else blocks[a] for n, a in enumerate((1, 0, 2))]
        width = GROUP * levels
        return jnp.where(lanes < width, turned[0], jnp.where(lanes < 2 * width, turned[1], turned[2]))

    mine = [strip_block(a, 0) for a in range(3)]
    sides = []
    sides.append([jnp.where(left_half, strip_block(a, before_b), mine[a]) for a in range(3)])
    sides.append([jnp.where(left_half, mine[a], strip_block(a, after_b)) for a in range(3)])
    side_c, side_v = [], []
    for blocks in sides:
        c = [placed(blocks, k + 1) for k in range(3)]
        v = placed(blocks, 0)
        for _ in range(2):
            v = forward(v, c, [right(v, GROUP), down(v), right(v)], [left(v, GROUP), up_row(v), left(v)])
        side_c.append(c)
        side_v.append(v)

    def inserted(z, l):
        return right(z, (cols - REACH - GROUP * (l + REACH)) % cols)

    def seen_block(b, i):
        full = seen_strip[i] if b == 0 else seen_full[b - 1, i]
        return joined(full, seen_half[0, b, i], seen_half[1, b, i])

    side_q = []
    for side in range(2):
        known = []
        for i in range(2):
            if side == 0:
                known.append(jnp.where(left_half, seen_block(before_b, i), seen_block(0, i)))
            else:
                known.append(jnp.where(left_half, seen_block(0, i), seen_block(after_b, i)))
        p = known[0] * side_v[side] - known[1]
        c = side_c[side]
        low, up = shares(p, c)
        q = centre_of(c) * p + left(low[0], GROUP) + right(up[0], GROUP)
        q = q + up_row(low[1]) + down(up[1]) + left(low[2]) + right(up[2])
        low, up = shares(q, c)
        side_q.append((q, right(up[2]) if side == 0 else left(low[2])))
    fix = jnp.where(left_half, side_q[1][0], side_q[0][0])
    crossing = jnp.where(left_half, side_q[1][1], side_q[0][1])

    fix_v = jnp.where(left_half, side_v[1], side_v[0])
    fix_v = {l: inserted(fix_v, l) for l in range(2 - near - 1, levels + near - 1)}
    fix_q = {l: inserted(fix, l) for l in range(-1, levels + 1)}
    crossing = {l: inserted(crossing, l) for l in range(levels)}

    settle(faces, 1, recv_sem.at[2])

    speeds = {l: [cell(l, k + 1) for k in range(3)] for l in range(1 - near, levels + near - 1)}
    start = {l: cell(l, 0) for l in range(-near, levels + near)}

    def step(v, l):
        return forward(v[l], speeds[l], [v[l - 1], down(v[l]), right(v[l])], [v[l + 1], up_row(v[l]), left(v[l])])

    v = {l: step(start, l) for l in speeds}
    for s in range(2):
        l = -near if s == 0 else levels + near - 1
        c = deep_in[s, 2]
        above = jnp.where((row == 0) & (c > 0.0), down(start[l])[:rows], 0.0)
        below = jnp.where((row == rows - 1) & (c <= 0.0), up_row(start[l])[:rows], 0.0)
        v[l] = jnp.concatenate([deep_in[s, 1] + jnp.abs(c) * (above + below), blank], axis=0)
    v = {l: step(v, l) for l in speeds}
    rim = (lanes < 2) | (lanes >= cols - 2)
    v = {l: jnp.where(rim, fix_v[l], v[l]) for l in v}
    for l in range(levels):
        state_v[l] = v[l][:rows]

    def seen_cell(l, i):
        g = l + beyond
        if 0 < g < span - 1:
            return joined(seen[g, i], seen_in[0, g - 1, i], seen_in[1, g - 1, i])
        return jnp.concatenate([seen[g, i], blank], axis=0)

    p = {l: seen_cell(l, 0) * v[l] - seen_cell(l, 1) for l in v}
    low, up = {}, {}
    for l in p:
        low[l], up[l] = shares(p[l], speeds[l])
    rim = (lanes < 1) | (lanes >= cols - 1)
    q = {}
    for l in range(-1, levels + 1):
        total = centre_of(speeds[l]) * p[l] + low[l + 1][0] + up[l - 1][0]
        total = total + up_row(low[l][1]) + down(up[l][1]) + left(low[l][2]) + right(up[l][2])
        q[l] = jnp.where(rim, fix_q[l], total)
    for l in q:
        low[l], up[l] = shares(q[l], speeds[l])
    for l in range(levels):
        total = centre_of(speeds[l]) * q[l] + low[l + 1][0] + up[l - 1][0]
        total = total + up_row(low[l][1]) + down(up[l][1])
        total = total + jnp.where(rim, crossing[l], 0.0)
        total = total + jnp.where(lanes >= cols - 1, 0.0, left(low[l][2])) + jnp.where(lanes < 1, 0.0, right(up[l][2]))
        adj_v[l] = total[:rows]

    settle(first + second + faces, 0, send_sem)


def finish(state_v, adj_v, outer, state_hbm, adj_hbm, next_hbm, wide, nxt, out_sem):
    levels, rows, cols = state_v.shape
    flat_rows = levels * rows
    wide_cols = outer.shape[1]
    fine = wide_cols // cols
    outer_rows = outer.shape[0] // levels
    stores = [
        pltpu.make_async_copy(state_v, state_hbm, out_sem.at[0]),
        pltpu.make_async_copy(adj_v, adj_hbm, out_sem.at[1]),
    ]
    for store in stores:
        store.start()
    field = adj_v[...]

    table = (
        lax.broadcasted_iota(jnp.int32, (cols, wide_cols), 0)
        == lax.broadcasted_iota(jnp.int32, (cols, wide_cols), 1) // fine
    ).astype(jnp.float32).astype(jnp.bfloat16)
    halves = bf16_parts(field.reshape(flat_rows, cols), 2)
    spread = jnp.dot(
        jnp.concatenate([h.astype(jnp.bfloat16) for h in halves], axis=1),
        jnp.concatenate([table, table], axis=0),
        preferred_element_type=jnp.float32,
    )
    for k in range(fine):
        for c in range(fine):
            wide[c, pl.ds(k, flat_rows, stride=fine), :] = spread[:, c * cols : (c + 1) * cols]
    for level in range(levels):
        span = pl.ds(level * outer_rows, outer_rows)
        for c in range(fine):
            lanes = pl.ds(c * cols, cols)
            nxt[span, lanes] = (outer[span, lanes].astype(jnp.float32) - wide[c, span, :]).astype(jnp.bfloat16)
        store = pltpu.make_async_copy(nxt.at[span], next_hbm.at[span], out_sem.at[2 + level])
        store.start()
        stores.append(store)
    for store in stores:
        store.wait()


def shards(ends, outer_increment, courant, obs_column, obs_level, obs_value):
    levels, outer_rows, wide_cols = outer_increment.shape
    _, _, rows, cols = courant.shape
    flat_rows = levels * rows
    fine = wide_cols // cols
    lanes = 128
    observed = (obs_column.shape[0] // lanes, lanes)
    span = levels + 4
    assert 4 * levels * GROUP == cols and levels >= REACH and rows % TILE == 0 and ends[1] > 1
    f32, bf16 = jnp.float32, jnp.bfloat16
    outer_shape = (levels * outer_rows, wide_cols)
    vmem = pl.BlockSpec(memory_space=pltpu.VMEM)
    hbm = pl.BlockSpec(memory_space=pl.ANY)
    held = pl.pallas_call(
        functools.partial(kernel, ends),
        out_shape=(
            pltpu.VMEM((levels, rows, cols), f32),
            pltpu.VMEM((levels, rows, cols), f32),
            pltpu.VMEM(outer_shape, bf16),
        ),
        in_specs=[hbm] * 5,
        out_specs=(vmem,) * 3,
        scratch_shapes=[
            pltpu.VMEM(courant.shape, bf16),
            pltpu.VMEM(observed, jnp.int32),
            pltpu.VMEM(observed, jnp.int32),
            pltpu.VMEM(observed, f32),
            pltpu.VMEM((levels * outer_rows, cols), f32),
            pltpu.VMEM((levels, 4, rows, cols), f32),
            pltpu.VMEM((2, REACH - 2, 4, rows, cols), f32),
            pltpu.VMEM((2, 3, rows, cols), f32),
            pltpu.VMEM((2, 3, rows, cols), f32),
            pltpu.VMEM((2, levels, 4, TILE, cols), f32),
            pltpu.VMEM((2, 2, 2 * TILE, cols), f32),
            pltpu.VMEM((2, 2, 2 * TILE, cols), f32),
            pltpu.VMEM((2, REACH - 1, 4, TILE, cols), f32),
            pltpu.VMEM((rows, cols), f32),
            pltpu.VMEM((3, 3, rows, cols), f32),
            pltpu.VMEM((3, 2, 3, TILE, cols), f32),
            pltpu.VMEM((span, 2, rows, cols), f32),
            pltpu.VMEM((2, span - 2, 2, TILE, cols), f32),
            pltpu.VMEM((2, rows, cols), f32),
            pltpu.VMEM((2, 2, rows, cols), f32),
            pltpu.VMEM((2, 3, 2, TILE, cols), f32),
            pltpu.VMEM((2048, 1, cols), f32),
            pltpu.SemaphoreType.DMA((5,)),
            pltpu.SemaphoreType.DMA,
            pltpu.SemaphoreType.DMA((3,)),
            pltpu.SemaphoreType.REGULAR((5,)),
        ],
        compiler_params=pltpu.CompilerParams(collective_id=0, has_side_effects=True),
    )(
        outer_increment.reshape(outer_shape),
        courant,
        obs_column.reshape(observed),
        obs_level.reshape(observed),
        obs_value.reshape(observed),
    )
    state, adjoint, following = pl.pallas_call(
        finish,
        out_shape=(
            jax.ShapeDtypeStruct((levels, rows, cols), f32),
            jax.ShapeDtypeStruct((levels, rows, cols), f32),
            jax.ShapeDtypeStruct(outer_shape, bf16),
        ),
        in_specs=[vmem] * 3,
        out_specs=(hbm,) * 3,
        scratch_shapes=[
            pltpu.VMEM((fine, levels * outer_rows, cols), f32),
            pltpu.VMEM(outer_shape, bf16),
            pltpu.SemaphoreType.DMA((2 + levels,)),
        ],
    )(*[pltpu.with_memory_space_constraint(x, pltpu.VMEM) for x in held])
    return state, adjoint, following.reshape(outer_increment.shape)


def solution(mesh):
    ends = tuple(mesh.shape[a] for a in ("lat", "lon", "lev"))
    block = P("lev", "lat", "lon")
    observed = P(("lat", "lon"))
    return jax.shard_map(
        functools.partial(shards, ends),
        mesh=mesh,
        in_specs=(block, P(None, "lev", "lat", "lon"), observed, observed, observed),
        out_specs=(block, block, block),
        check_vma=False,
    )
```

```python
import functools

import jax
import jax.numpy as jnp
from jax import lax
from jax.experimental import pallas as pl
from jax.experimental.pallas import tpu as pltpu
from jax.sharding import PartitionSpec as P

MESH = pl.DeviceIdType.MESH
REACH = 4
GROUP = 2 * REACH
TILE = 8


def bf16_parts(x, count):
    parts = []
    for _ in range(count):
        part = x.astype(jnp.bfloat16).astype(jnp.float32)
        parts.append(part)
        x = x - part
    return parts


def forward(v, c, minus, plus):
    sizes = [jnp.abs(n) for n in c]
    result = (1.0 - sizes[0] - sizes[1] - sizes[2]) * v
    for k in range(3):
        result = result + sizes[k] * jnp.where(c[k] > 0.0, minus[k], plus[k])
    return result


def shares(p, c):
    low, up = [], []
    for n in c:
        moved = jnp.abs(n) * p
        low.append(jnp.where(n > 0.0, moved, 0.0))
        up.append(jnp.where(n > 0.0, 0.0, moved))
    return low, up


def centre_of(c):
    return 1.0 - jnp.abs(c[0]) - jnp.abs(c[1]) - jnp.abs(c[2])


def kernel(
    ends, outer_hbm, courant_hbm, col_hbm, lvl_hbm, val_hbm,
    state_v, adj_v, outer,
    courant, col, lvl, val, sums,
    own, face_in, deep_out, deep_in, side_in, edge_out, edge_in, halo,
    strip, strip_full, strip_half,
    seen, seen_in, seen_strip, seen_full, seen_half, units,
    in_sem, send_sem, recv_sem, ready,
):
    n_lat, n_lon, n_lev = ends
    levels, rows, cols = state_v.shape
    flat_rows = levels * rows
    wide_cols = outer.shape[1]
    fine = wide_cols // cols
    near = REACH - 1
    span = seen.shape[0]
    beyond = (span - levels) // 2

    loads = [
        pltpu.make_async_copy(src, dst, in_sem.at[i])
        for i, (src, dst) in enumerate(
            ((outer_hbm, outer), (courant_hbm, courant), (col_hbm, col), (lvl_hbm, lvl), (val_hbm, val))
        )
    ]
    for load in loads:
        load.start()

    me_lat, me_lon, me_lev = (lax.axis_index(a) for a in ("lat", "lon", "lev"))
    links = (
        ("lev", me_lev + 1, me_lev < n_lev - 1),
        ("lev", me_lev - 1, me_lev > 0),
        ("lat", me_lat + 1, me_lat < n_lat - 1),
        ("lat", me_lat - 1, me_lat > 0),
        ("lon", lax.rem(me_lon + 1, n_lon), None),
        ("lon", lax.rem(me_lon + n_lon - 1, n_lon), None),
    )
    turns = (0, 1) if n_lon > 2 else (0,)
    bands = ((rows - TILE, TILE), (0, TILE))

    def both(flags):
        return functools.reduce(jnp.logical_and, flags) if flags else None

    def guarded(exists, action):
        if exists is None:
            action()
        else:
            pl.when(exists)(action)

    def flags_of(which):
        return [links[w][2] for w in which if w < 4]

    def lon_of(which):
        return [w for w in which if w > 3]

    def is_ahead(which):
        return me_lon < links[lon_of(which)[0]][1]

    def is_behind(which):
        return me_lon > links[lon_of(which)[0]][1]

    class Message:
        def __init__(self, which, source, landing, sem, later=0):
            self.which, self.later = which, later
            self.needs = tuple(w for w in which if w < 4)
            self.target = {links[w][0]: links[w][1] for w in which}
            self.arrives = both([links[w ^ 1][2] for w in self.needs])
            self.source, self.landing, self.sem = source, landing, sem

        def start(self, flag=None):
            def begin():
                pltpu.make_async_remote_copy(
                    src_ref=self.source, dst_ref=self.landing, send_sem=send_sem, recv_sem=recv_sem.at[self.sem],
                    device_id=self.target, device_id_type=MESH,
                ).start()

            guarded(both(flags_of(self.which) + ([] if flag is None else [flag])), begin)

        def lines(self):
            total = 1
            for n in self.landing.shape:
                total = total * n
            return total // cols

    partners, first, second, faces = [], [], [], []
    for a in (2, 1, 0):
        for t in (0, 1, None):
            for u in turns + (None,):
                which = [a - 1] if a else []
                which = which + ([2 + t] if t is not None else []) + ([4 + u] if u is not None else [])
                if not which:
                    continue
                partners.append(which)
                b = 0 if u is None else u + 1
                if t is None:
                    first.append(Message(which, strip, strip_full.at[a, b], 0))
                else:
                    first.append(Message(which, strip.at[pl.ds(*bands[t])], strip_half.at[a, t, b], 0))
                if u is None:
                    if a and t is None:
                        faces.append(Message(which, own.at[levels - 1 if a == 1 else 0], face_in.at[a - 1], 2))
                        faces.append(Message(which, deep_out.at[a - 1], deep_in.at[a - 1], 2, 2))
                    elif a:
                        first.append(Message(which, edge_out.at[a - 1, t], edge_in.at[a - 1, t], 0))
                    else:
                        faces.append(Message(which, own.at[:, :, pl.ds(*bands[t])], side_in.at[t], 2))
                if not a:
                    if t is None:
                        second.append(Message(which, seen_strip, seen_full.at[u], 1))
                    else:
                        second.append(Message(which, seen_strip.at[:, pl.ds(*bands[t])], seen_half.at[t, b], 1))
                    if u is None:
                        kept = pl.ds(1, span - 2)
                        second.append(Message(which, seen.at[kept, :, pl.ds(*bands[t])], seen_in.at[t], 1))
    first.sort(key=lambda m: -len(m.target))

    def pick(test, side=None):
        return [(which, None if side is None else side(which)) for which in partners if test(which)]

    def count(chosen):
        total = 0
        for which, flag in chosen:
            exists = both(flags_of(which) + ([] if flag is None else [flag]))
            total = total + (1 if exists is None else exists.astype(jnp.int32))
        return total

    def signal(sem, chosen):
        for which, flag in chosen:
            target = {links[w][0]: links[w][1] for w in which}
            guarded(
                both(flags_of(which) + ([] if flag is None else [flag])),
                lambda target=target: pl.semaphore_signal(sem, inc=1, device_id=target, device_id_type=MESH),
            )

    def level_lon(which):
        return lon_of(which) and not {0, 1} & set(which)

    def corner(which):
        return len(which) == 3

    lower = pick(lambda w: 1 in w and not corner(w))
    upper = pick(lambda w: 0 in w and not corner(w))
    lower_face, upper_face = [[c for c in side if len(c[0]) == 1] for side in (lower, upper)]
    lower_rest, upper_rest = [[c for c in side if len(c[0]) > 1] for side in (lower, upper)]
    lower_south = pick(lambda w: corner(w) and 1 in w and 3 in w)
    upper_north = pick(lambda w: corner(w) and 0 in w and 2 in w)
    south, north = pick(lambda w: w == [3]), pick(lambda w: w == [2])
    behind, ahead = pick(level_lon, is_behind), pick(level_lon, is_ahead)

    barrier = pltpu.get_barrier_semaphore()
    signal(barrier, upper_north + upper_rest + upper_face + ahead + north)

    def settle(messages, flip, sem, known=()):
        if len(known) < 4:
            for has in (True, False):
                flag = links[len(known)][2]
                pl.when(flag if has else jnp.logical_not(flag))(
                    lambda has=has: settle(messages, flip, sem, known + (has,))
                )
            return
        total = sum(m.lines() for m in messages if all(known[w ^ flip] for w in m.needs))
        view = units.at[pl.ds(0, total)]
        pltpu.make_async_copy(view, view, sem).wait()

    def clear(ref):
        ref[...] = jnp.zeros(ref.shape, jnp.float32)

    for m in first + second + faces:
        if m.arrives is not None:
            pl.when(jnp.logical_not(m.arrives))(lambda m=m: clear(m.landing))
    clear(halo)

    lane = lax.broadcasted_iota(jnp.int32, (rows, cols), 1)
    group = lane // GROUP
    pool = (
        lax.broadcasted_iota(jnp.int32, (wide_cols, cols), 0) // fine
        == lax.broadcasted_iota(jnp.int32, (wide_cols, cols), 1)
    ).astype(jnp.float32).astype(jnp.bfloat16)

    loads[1].wait()
    for k in range(3):
        own[:, k + 1] = courant[k].astype(jnp.float32)
    loads[0].wait()
    sums[...] = jnp.dot(outer[...], pool, preferred_element_type=jnp.float32)
    coarse = sums[pl.ds(0, flat_rows, stride=fine), :]
    for k in range(1, fine):
        coarse = coarse + sums[pl.ds(k, flat_rows, stride=fine), :]
    own[:, 0] = (coarse * (1.0 / (fine * fine))).reshape(levels, rows, cols)

    ends_only = jnp.zeros((rows, cols), jnp.float32)
    for f in (1, 2, 3, 0):
        for l in range(levels):
            place = f * levels + l
            ends_only = jnp.where(group == place, pltpu.roll(own[l, f], (REACH + GROUP * place) % cols, axis=1), ends_only)
    strip[...] = ends_only

    entries = [(0, i, j) for i in range(1, REACH) for j in range(1, REACH + 1 - i)]
    entries = entries + [(f, i, j) for f in (1, 2, 3) for i in range(1, near) for j in range(1, near + 1 - i)]
    for s in range(2):
        for t in range(2):
            for n, (f, i, j) in enumerate(entries):
                l = levels - i if s == 0 else i - 1
                r = rows - j if t == 0 else j - 1
                edge_out[s, t, n : n + 1, :] = own[l, f, r : r + 1, :]

    def send(messages, test, side=None, later=0):
        for m in messages:
            if test(m.which) and m.later == later:
                m.start(None if side is None else side(m.which))

    def at_once(w):
        return (1 in w and not (corner(w) and 2 in w)) or w == [3]

    def to_north(w):
        return w == [2] or (corner(w) and 1 in w and 2 in w)

    expected = count(lower + lower_south + south + behind)
    pl.when(expected > 0)(lambda: pl.semaphore_wait(barrier, expected))
    signal(ready.at[4], [(w, is_behind(w)) for w, _ in lower_south])
    signal(ready.at[3], lower_rest)
    signal(ready.at[0], behind)
    signal(ready.at[2], lower_face)
    signal(ready.at[1], south)
    send(first, at_once)
    send(first, level_lon, is_behind)
    send(faces, at_once)

    row = lax.broadcasted_iota(jnp.int32, (rows, cols), 0)
    high = rows // TILE
    zero = jnp.zeros((rows, cols), jnp.float32)

    def inner(v, c, before, after):
        above = jnp.where(row == 0, 0.0, pltpu.roll(v, 1, axis=0))
        below = jnp.where(row == rows - 1, 0.0, pltpu.roll(v, rows - 1, axis=0))
        return forward(v, c, [before, above, pltpu.roll(v, 1, axis=1)], [after, below, pltpu.roll(v, cols - 1, axis=1)])

    def rim_rows(second_level, third_level):
        kept = [(second_level, 2, r) for r in (0, 1, rows - 2, rows - 1)]
        return kept + [(second_level, 3, r) for r in (0, rows - 1)] + [(third_level, 2, r) for r in (0, rows - 1)]

    pairs = ((levels - 2, levels - 3), (1, 2))
    once = {
        l: inner(own[l, 0], [own[l, k + 1] for k in range(3)], own[l - 1, 0], own[l + 1, 0])
        for l in sorted(set(pairs[0] + pairs[1]))
    }
    for s, (l, far) in enumerate(pairs):
        c = [own[l, k + 1] for k in range(3)]
        twice = inner(once[l], c, zero if s else once[far], once[far] if s else zero)
        for n, plane in enumerate((own[l, 0], once[l], twice, c[0])):
            deep_out[s, n * high : (n + 1) * high] = plane.reshape(high, TILE, cols)
        for n, (at, f, r) in enumerate(rim_rows(l, far)):
            deep_out[s, 4 * high, n : n + 1, :] = own[at, f, r : r + 1, :]

    for load in loads[2:]:
        load.wait()
    where_row = (lvl[...] - me_lev * levels + beyond) * rows + col[...] // cols
    where_col = col[...] % cols
    parts = bf16_parts(val[...], 2)
    pieces, width = col.shape
    row_id = lax.broadcasted_iota(jnp.int32, (span * rows, width), 0)
    col_id = lax.broadcasted_iota(jnp.int32, (cols, width), 0)
    hits = [[] for _ in range(3)]
    tables = []
    for k in range(pieces):
        match = where_row[k : k + 1] == row_id
        hits[0].append(jnp.where(match, 1.0, 0.0).astype(jnp.bfloat16))
        for i, part in enumerate(parts):
            hits[i + 1].append(jnp.where(match, part[k : k + 1], 0.0).astype(jnp.bfloat16))
        tables.append(jnp.where(where_col[k : k + 1] == col_id, 1.0, 0.0).astype(jnp.bfloat16))
    left_side = jnp.concatenate([jnp.concatenate(h, axis=1) for h in hits], axis=0)
    totals = lax.dot_general(
        left_side, jnp.concatenate(tables, axis=1), (((1,), (1,)), ((), ())),
        preferred_element_type=jnp.float32,
    )
    wide_rows = span * rows
    counted = totals[:wide_rows].reshape(span, rows, cols)
    summed = (totals[wide_rows : 2 * wide_rows] + totals[2 * wide_rows :]).reshape(span, rows, cols)
    seen[:, 0] = counted
    seen[:, 1] = summed
    for i, values in enumerate((counted, summed)):
        ends_only = jnp.zeros((rows, cols), jnp.float32)
        for g in range(span):
            place = g + REACH - beyond
            ends_only = jnp.where(group == place, pltpu.roll(values[g], (REACH + GROUP * place) % cols, axis=1), ends_only)
        seen_strip[i] = ends_only
    send(second, at_once)
    send(second, level_lon, is_behind)

    def go_north():
        pl.semaphore_wait(ready.at[1], 1)
        send(first + faces + second, to_north)

    early = me_lon > 0
    pl.when(links[2][2] & early)(go_north)
    send(faces, at_once, later=2)
    pl.when(links[2][2] & jnp.logical_not(early))(go_north)

    @pl.when(me_lon < n_lon - 1)
    def _():
        pl.semaphore_wait(ready.at[0], count(ahead))
        send(first + second, level_lon, is_ahead)

    @pl.when(links[0][2])
    def _():
        pl.semaphore_wait(ready.at[2], 1)
        send(faces, lambda w: 0 in w)
        pl.semaphore_wait(ready.at[3], count(upper_rest))
        send(first, lambda w: 0 in w and not (corner(w) and 2 in w))
        send(first, lambda w: corner(w) and 0 in w and 2 in w, is_behind)

    @pl.when(links[0][2] & links[2][2] & (me_lon < n_lon - 1))
    def _():
        pl.semaphore_wait(ready.at[4], count([(w, is_ahead(w)) for w, _ in upper_north]))
        send(first, lambda w: corner(w) and 0 in w and 2 in w, is_ahead)

    pl.when(links[0][2])(lambda: send(faces, lambda w: 0 in w, later=2))

    settle(first, 1, recv_sem.at[0])

    tall = rows + TILE
    half = lax.broadcasted_iota(jnp.int32, (TILE, cols), 0) < TILE // 2
    lanes = lax.broadcasted_iota(jnp.int32, (tall, cols), 1)
    slot = lanes % GROUP
    left_half = slot < REACH
    blank = jnp.zeros((TILE, cols), jnp.float32)

    def joined(full, before, after):
        return jnp.concatenate([full, jnp.where(half, after, before)], axis=0)

    for s in range(2):
        for t in range(2):
            for n, (f, i, j) in enumerate(entries):
                r = TILE - j if t == 0 else j - 1
                halo[s, i - 1, f, r : r + 1, :] = edge_in[s, t, n : n + 1, :]

    def cell(l, f):
        if 0 <= l < levels:
            return joined(own[l, f], side_in[0, l, f], side_in[1, l, f])
        s, i = (0, -l) if l < 0 else (1, l - levels + 1)
        return jnp.concatenate([face_in[s, f], halo[s, i - 1, f]], axis=0)

    def down(x):
        return pltpu.roll(x, 1, axis=0)

    def up_row(x):
        return pltpu.roll(x, tall - 1, axis=0)

    def right(x, by=1):
        return pltpu.roll(x, by, axis=1)

    def left(x, by=1):
        return pltpu.roll(x, cols - by, axis=1)

    before_b, after_b = 1, (2 if n_lon > 2 else 1)

    def strip_block(a, b):
        full = strip[...] if a == 0 and b == 0 else strip_full[a, b]
        return joined(full, strip_half[a, 0, b], strip_half[a, 1, b])

    def placed(blocks, f):
        turned = [right(blocks[a], (GROUP * levels * (n - f)) % cols) if n != f else blocks[a] for n, a in enumerate((1, 0, 2))]
        width = GROUP * levels
        return jnp.where(lanes < width, turned[0], jnp.where(lanes < 2 * width, turned[1], turned[2]))

    mine = [strip_block(a, 0) for a in range(3)]
    sides = []
    sides.append([jnp.where(left_half, strip_block(a, before_b), mine[a]) for a in range(3)])
    sides.append([jnp.where(left_half, mine[a], strip_block(a, after_b)) for a in range(3)])
    side_c, side_v = [], []
    for blocks in sides:
        c = [placed(blocks, k + 1) for k in range(3)]
        v = placed(blocks, 0)
        for _ in range(2):
            v = forward(v, c, [right(v, GROUP), down(v), right(v)], [left(v, GROUP), up_row(v), left(v)])
        side_c.append(c)
        side_v.append(v)

    def inserted(z, l):
        return right(z, (cols - REACH - GROUP * (l + REACH)) % cols)

    def seen_block(b, i):
        full = seen_strip[i] if b == 0 else seen_full[b - 1, i]
        return joined(full, seen_half[0, b, i], seen_half[1, b, i])

    settle(second, 1, recv_sem.at[1])
    side_q = []
    for side in range(2):
        known = []
        for i in range(2):
            if side == 0:
                known.append(jnp.where(left_half, seen_block(before_b, i), seen_block(0, i)))
            else:
                known.append(jnp.where(left_half, seen_block(0, i), seen_block(after_b, i)))
        p = known[0] * side_v[side] - known[1]
        c = side_c[side]
        low, up = shares(p, c)
        q = centre_of(c) * p + left(low[0], GROUP) + right(up[0], GROUP)
        q = q + up_row(low[1]) + down(up[1]) + left(low[2]) + right(up[2])
        low, up = shares(q, c)
        side_q.append((q, right(up[2]) if side == 0 else left(low[2])))
    fix = jnp.where(left_half, side_q[1][0], side_q[0][0])
    crossing = jnp.where(left_half, side_q[1][1], side_q[0][1])

    fix_v = jnp.where(left_half, side_v[1], side_v[0])
    fix_v = {l: inserted(fix_v, l) for l in range(2 - near - 1, levels + near - 1)}
    fix_q = {l: inserted(fix, l) for l in range(-1, levels + 1)}
    crossing = {l: inserted(crossing, l) for l in range(levels)}

    settle(faces, 1, recv_sem.at[2])

    speeds = {l: [cell(l, k + 1) for k in range(3)] for l in range(-1, levels + 1)}
    start = {l: cell(l, 0) for l in range(-1, levels + 1)}
    beside = ((-2, -1, -3), (levels + 1, levels, levels + 2))

    def deep(s, n):
        return deep_in[s, n * high : (n + 1) * high].reshape(rows, cols)

    def kept_rows(s, places):
        plane = zero
        for n, r in places:
            plane = jnp.where(row == r, deep_in[s, 4 * high, n : n + 1, :], plane)
        return plane

    def across(c, x):
        above = jnp.where((row == 0) & (c > 0.0), down(x)[:rows], 0.0)
        below = jnp.where((row == rows - 1) & (c <= 0.0), up_row(x)[:rows], 0.0)
        return jnp.abs(c) * (above + below)

    def step(v, l):
        return forward(v[l], speeds[l], [v[l - 1], down(v[l]), right(v[l])], [v[l + 1], up_row(v[l]), left(v[l])])

    outside = []
    for s, (l, _, far) in enumerate(beside):
        c = [
            deep(s, 3),
            kept_rows(s, ((0, 0), (1, 1), (2, rows - 2), (3, rows - 1))),
            kept_rows(s, ((4, 0), (5, rows - 1))),
        ]
        start[l] = jnp.concatenate([deep(s, 0), halo[s, 1, 0]], axis=0)
        start[far] = jnp.concatenate([zero, halo[s, 2, 0]], axis=0)
        speeds[l] = [jnp.concatenate([c[k], halo[s, 1, k + 1]], axis=0) for k in range(3)]
        gained = across(c[1], start[l])
        further = across(kept_rows(s, ((6, 0), (7, rows - 1))), start[far])
        outside.append((c, gained, further))
    v = {l: step(start, l) for l in range(-1, levels + 1)}
    for s, (l, _, _) in enumerate(beside):
        v[l] = jnp.concatenate([deep(s, 1) + outside[s][1], step(start, l)[rows:]], axis=0)
    second_v = {l: step(v, l) for l in range(-1, levels + 1)}
    for s, (l, by, _) in enumerate(beside):
        c, gained, further = outside[s]
        sizes = [jnp.abs(n) for n in c]
        inward, outward = v[by][:rows], further
        crossed = jnp.concatenate([gained, v[l][rows:]], axis=0)
        total = deep(s, 2) + (1.0 - sizes[0] - sizes[1] - sizes[2]) * gained
        total = total + sizes[0] * jnp.where(c[0] > 0.0, inward if s else outward, outward if s else inward)
        total = total + sizes[1] * jnp.where(c[1] > 0.0, down(crossed)[:rows], up_row(crossed)[:rows])
        total = total + sizes[2] * jnp.where(
            c[2] > 0.0, pltpu.roll(gained, 1, axis=1), pltpu.roll(gained, cols - 1, axis=1)
        )
        second_v[l] = jnp.concatenate([total, blank], axis=0)
        speeds[l] = [jnp.concatenate([c[0], blank], axis=0)]
    v = second_v
    rim = (lanes < 2) | (lanes >= cols - 2)
    v = {l: jnp.where(rim, fix_v[l], v[l]) for l in v}
    for l in range(levels):
        state_v[l] = v[l][:rows]

    def seen_cell(l, i):
        g = l + beyond
        if 0 < g < span - 1:
            return joined(seen[g, i], seen_in[0, g - 1, i], seen_in[1, g - 1, i])
        return jnp.concatenate([seen[g, i], blank], axis=0)

    p = {l: seen_cell(l, 0) * v[l] - seen_cell(l, 1) for l in v}
    low, up = {}, {}
    for l in p:
        low[l], up[l] = shares(p[l], speeds[l])
    rim = (lanes < 1) | (lanes >= cols - 1)
    q = {}
    for l in range(-1, levels + 1):
        total = centre_of(speeds[l]) * p[l] + low[l + 1][0] + up[l - 1][0]
        total = total + up_row(low[l][1]) + down(up[l][1]) + left(low[l][2]) + right(up[l][2])
        q[l] = jnp.where(rim, fix_q[l], total)
    for l in q:
        low[l], up[l] = shares(q[l], speeds[l])
    for l in range(levels):
        total = centre_of(speeds[l]) * q[l] + low[l + 1][0] + up[l - 1][0]
        total = total + up_row(low[l][1]) + down(up[l][1])
        total = total + jnp.where(rim, crossing[l], 0.0)
        total = total + jnp.where(lanes >= cols - 1, 0.0, left(low[l][2])) + jnp.where(lanes < 1, 0.0, right(up[l][2]))
        adj_v[l] = total[:rows]

    settle(first + second + faces, 0, send_sem)


def finish(state_v, adj_v, outer, state_hbm, adj_hbm, next_hbm, wide, nxt, out_sem):
    levels, rows, cols = state_v.shape
    flat_rows = levels * rows
    wide_cols = outer.shape[1]
    fine = wide_cols // cols
    outer_rows = outer.shape[0] // levels
    stores = [
        pltpu.make_async_copy(state_v, state_hbm, out_sem.at[0]),
        pltpu.make_async_copy(adj_v, adj_hbm, out_sem.at[1]),
    ]
    for store in stores:
        store.start()
    field = adj_v[...]

    table = (
        lax.broadcasted_iota(jnp.int32, (cols, wide_cols), 0)
        == lax.broadcasted_iota(jnp.int32, (cols, wide_cols), 1) // fine
    ).astype(jnp.float32).astype(jnp.bfloat16)
    halves = bf16_parts(field.reshape(flat_rows, cols), 2)
    spread = jnp.dot(
        jnp.concatenate([h.astype(jnp.bfloat16) for h in halves], axis=1),
        jnp.concatenate([table, table], axis=0),
        preferred_element_type=jnp.float32,
    )
    for k in range(fine):
        for c in range(fine):
            wide[c, pl.ds(k, flat_rows, stride=fine), :] = spread[:, c * cols : (c + 1) * cols]
    for level in range(levels):
        span = pl.ds(level * outer_rows, outer_rows)
        for c in range(fine):
            lanes = pl.ds(c * cols, cols)
            nxt[span, lanes] = (outer[span, lanes].astype(jnp.float32) - wide[c, span, :]).astype(jnp.bfloat16)
        store = pltpu.make_async_copy(nxt.at[span], next_hbm.at[span], out_sem.at[2 + level])
        store.start()
        stores.append(store)
    for store in stores:
        store.wait()


def shards(ends, outer_increment, courant, obs_column, obs_level, obs_value):
    levels, outer_rows, wide_cols = outer_increment.shape
    _, _, rows, cols = courant.shape
    flat_rows = levels * rows
    fine = wide_cols // cols
    lanes = 128
    observed = (obs_column.shape[0] // lanes, lanes)
    span = levels + 4
    assert 4 * levels * GROUP == cols and levels >= REACH and rows % TILE == 0 and ends[1] > 1
    f32, bf16 = jnp.float32, jnp.bfloat16
    outer_shape = (levels * outer_rows, wide_cols)
    vmem = pl.BlockSpec(memory_space=pltpu.VMEM)
    hbm = pl.BlockSpec(memory_space=pl.ANY)
    held = pl.pallas_call(
        functools.partial(kernel, ends),
        out_shape=(
            pltpu.VMEM((levels, rows, cols), f32),
            pltpu.VMEM((levels, rows, cols), f32),
            pltpu.VMEM(outer_shape, bf16),
        ),
        in_specs=[hbm] * 5,
        out_specs=(vmem,) * 3,
        scratch_shapes=[
            pltpu.VMEM(courant.shape, bf16),
            pltpu.VMEM(observed, jnp.int32),
            pltpu.VMEM(observed, jnp.int32),
            pltpu.VMEM(observed, f32),
            pltpu.VMEM((levels * outer_rows, cols), f32),
            pltpu.VMEM((levels, 4, rows, cols), f32),
            pltpu.VMEM((2, 4, rows, cols), f32),
            pltpu.VMEM((2, 4 * rows // TILE + 1, TILE, cols), f32),
            pltpu.VMEM((2, 4 * rows // TILE + 1, TILE, cols), f32),
            pltpu.VMEM((2, levels, 4, TILE, cols), f32),
            pltpu.VMEM((2, 2, 2 * TILE, cols), f32),
            pltpu.VMEM((2, 2, 2 * TILE, cols), f32),
            pltpu.VMEM((2, REACH - 1, 4, TILE, cols), f32),
            pltpu.VMEM((rows, cols), f32),
            pltpu.VMEM((3, 3, rows, cols), f32),
            pltpu.VMEM((3, 2, 3, TILE, cols), f32),
            pltpu.VMEM((span, 2, rows, cols), f32),
            pltpu.VMEM((2, span - 2, 2, TILE, cols), f32),
            pltpu.VMEM((2, rows, cols), f32),
            pltpu.VMEM((2, 2, rows, cols), f32),
            pltpu.VMEM((2, 3, 2, TILE, cols), f32),
            pltpu.VMEM((2048, 1, cols), f32),
            pltpu.SemaphoreType.DMA((5,)),
            pltpu.SemaphoreType.DMA,
            pltpu.SemaphoreType.DMA((3,)),
            pltpu.SemaphoreType.REGULAR((5,)),
        ],
        compiler_params=pltpu.CompilerParams(collective_id=0, has_side_effects=True),
    )(
        outer_increment.reshape(outer_shape),
        courant,
        obs_column.reshape(observed),
        obs_level.reshape(observed),
        obs_value.reshape(observed),
    )
    state, adjoint, following = pl.pallas_call(
        finish,
        out_shape=(
            jax.ShapeDtypeStruct((levels, rows, cols), f32),
            jax.ShapeDtypeStruct((levels, rows, cols), f32),
            jax.ShapeDtypeStruct(outer_shape, bf16),
        ),
        in_specs=[vmem] * 3,
        out_specs=(hbm,) * 3,
        scratch_shapes=[
            pltpu.VMEM((fine, levels * outer_rows, cols), f32),
            pltpu.VMEM(outer_shape, bf16),
            pltpu.SemaphoreType.DMA((2 + levels,)),
        ],
    )(*[pltpu.with_memory_space_constraint(x, pltpu.VMEM) for x in held])
    return state, adjoint, following.reshape(outer_increment.shape)


def solution(mesh):
    ends = tuple(mesh.shape[a] for a in ("lat", "lon", "lev"))
    block = P("lev", "lat", "lon")
    observed = P(("lat", "lon"))
    return jax.shard_map(
        functools.partial(shards, ends),
        mesh=mesh,
        in_specs=(block, P(None, "lev", "lat", "lon"), observed, observed, observed),
        out_specs=(block, block, block),
        check_vma=False,
    )
```

```python
import functools

import jax
import jax.numpy as jnp
from jax import lax
from jax.experimental import pallas as pl
from jax.experimental.pallas import tpu as pltpu
from jax.sharding import PartitionSpec as P

MESH = pl.DeviceIdType.MESH
REACH = 4
GROUP = 2 * REACH
TILE = 8


def bf16_parts(x, count):
    parts = []
    for _ in range(count):
        part = x.astype(jnp.bfloat16).astype(jnp.float32)
        parts.append(part)
        x = x - part
    return parts


def forward(v, c, minus, plus):
    sizes = [jnp.abs(n) for n in c]
    result = (1.0 - sizes[0] - sizes[1] - sizes[2]) * v
    for k in range(3):
        result = result + sizes[k] * jnp.where(c[k] > 0.0, minus[k], plus[k])
    return result


def shares(p, c):
    low, up = [], []
    for n in c:
        moved = jnp.abs(n) * p
        low.append(jnp.where(n > 0.0, moved, 0.0))
        up.append(jnp.where(n > 0.0, 0.0, moved))
    return low, up


def centre_of(c):
    return 1.0 - jnp.abs(c[0]) - jnp.abs(c[1]) - jnp.abs(c[2])


def kernel(
    ends, outer_hbm, courant_hbm, col_hbm, lvl_hbm, val_hbm,
    state_v, adj_v, outer,
    courant, col, lvl, val, sums,
    own, face_in, deep_out, deep_in, side_in, edge_out, edge_in, halo,
    strip, strip_full, strip_half,
    seen, seen_in, seen_strip, seen_full, seen_half, units,
    in_sem, send_sem, recv_sem, ready,
):
    n_lat, n_lon, n_lev = ends
    levels, rows, cols = state_v.shape
    flat_rows = levels * rows
    wide_cols = outer.shape[1]
    fine = wide_cols // cols
    near = REACH - 1
    span = seen.shape[0]
    beyond = (span - levels) // 2

    loads = [
        pltpu.make_async_copy(src, dst, in_sem.at[min(i, 2)])
        for i, (src, dst) in enumerate(
            ((outer_hbm, outer), (courant_hbm, courant), (col_hbm, col), (lvl_hbm, lvl), (val_hbm, val))
        )
    ]
    for load in loads:
        load.start()

    me_lat, me_lon, me_lev = (lax.axis_index(a) for a in ("lat", "lon", "lev"))
    links = (
        ("lev", me_lev + 1, me_lev < n_lev - 1),
        ("lev", me_lev - 1, me_lev > 0),
        ("lat", me_lat + 1, me_lat < n_lat - 1),
        ("lat", me_lat - 1, me_lat > 0),
        ("lon", lax.rem(me_lon + 1, n_lon), None),
        ("lon", lax.rem(me_lon + n_lon - 1, n_lon), None),
    )
    turns = (0, 1) if n_lon > 2 else (0,)
    bands = ((rows - TILE, TILE), (0, TILE))

    def both(flags):
        return functools.reduce(jnp.logical_and, flags) if flags else None

    def guarded(exists, action):
        if exists is None:
            action()
        else:
            pl.when(exists)(action)

    def flags_of(which):
        return [links[w][2] for w in which if w < 4]

    def lon_of(which):
        return [w for w in which if w > 3]

    def is_ahead(which):
        return me_lon < links[lon_of(which)[0]][1]

    def is_behind(which):
        return me_lon > links[lon_of(which)[0]][1]

    class Message:
        def __init__(self, which, source, landing, sem, later=0):
            self.which, self.later = which, later
            self.needs = tuple(w for w in which if w < 4)
            self.target = {links[w][0]: links[w][1] for w in which}
            self.arrives = both([links[w ^ 1][2] for w in self.needs])
            self.source, self.landing, self.sem = source, landing, sem

        def start(self, flag=None):
            def begin():
                pltpu.make_async_remote_copy(
                    src_ref=self.source, dst_ref=self.landing, send_sem=send_sem, recv_sem=recv_sem.at[self.sem],
                    device_id=self.target, device_id_type=MESH,
                ).start()

            guarded(both(flags_of(self.which) + ([] if flag is None else [flag])), begin)

        def lines(self):
            total = 1
            for n in self.landing.shape:
                total = total * n
            return total // cols

    partners, first, second, faces = [], [], [], []
    for a in (2, 1, 0):
        for t in (0, 1, None):
            for u in turns + (None,):
                which = [a - 1] if a else []
                which = which + ([2 + t] if t is not None else []) + ([4 + u] if u is not None else [])
                if not which:
                    continue
                partners.append(which)
                b = 0 if u is None else u + 1
                if t is None:
                    first.append(Message(which, strip, strip_full.at[a, b], 0))
                else:
                    first.append(Message(which, strip.at[pl.ds(*bands[t])], strip_half.at[a, t, b], 0))
                if u is None:
                    if a and t is None:
                        faces.append(Message(which, own.at[levels - 1 if a == 1 else 0], face_in.at[a - 1], 2))
                        faces.append(Message(which, deep_out.at[a - 1], deep_in.at[a - 1], 2, 2))
                    elif a:
                        first.append(Message(which, edge_out.at[a - 1, t], edge_in.at[a - 1, t], 0))
                    else:
                        faces.append(Message(which, own.at[:, :, pl.ds(*bands[t])], side_in.at[t], 2))
                if not a:
                    if t is None:
                        second.append(Message(which, seen_strip, seen_full.at[u], 1))
                    else:
                        second.append(Message(which, seen_strip.at[:, pl.ds(*bands[t])], seen_half.at[t, b], 1))
                    if u is None:
                        kept = pl.ds(1, span - 2)
                        second.append(Message(which, seen.at[kept, :, pl.ds(*bands[t])], seen_in.at[t], 1))
    first.sort(key=lambda m: -len(m.target))

    def pick(test, side=None):
        return [(which, None if side is None else side(which)) for which in partners if test(which)]

    def count(chosen):
        total = 0
        for which, flag in chosen:
            exists = both(flags_of(which) + ([] if flag is None else [flag]))
            total = total + (1 if exists is None else exists.astype(jnp.int32))
        return total

    def signal(sem, chosen):
        for which, flag in chosen:
            target = {links[w][0]: links[w][1] for w in which}
            guarded(
                both(flags_of(which) + ([] if flag is None else [flag])),
                lambda target=target: pl.semaphore_signal(sem, inc=1, device_id=target, device_id_type=MESH),
            )

    def level_lon(which):
        return lon_of(which) and not {0, 1} & set(which)

    def corner(which):
        return len(which) == 3

    lower = pick(lambda w: 1 in w and not corner(w))
    upper = pick(lambda w: 0 in w and not corner(w))
    lower_face, upper_face = [[c for c in side if len(c[0]) == 1] for side in (lower, upper)]
    lower_rest, upper_rest = [[c for c in side if len(c[0]) > 1] for side in (lower, upper)]
    lower_south = pick(lambda w: corner(w) and 1 in w and 3 in w)
    upper_north = pick(lambda w: corner(w) and 0 in w and 2 in w)
    lower_north = pick(lambda w: corner(w) and 1 in w and 2 in w, is_behind)
    upper_south = pick(lambda w: corner(w) and 0 in w and 3 in w, is_ahead)
    south, north = pick(lambda w: w == [3]), pick(lambda w: w == [2])
    behind, ahead = pick(level_lon, is_behind), pick(level_lon, is_ahead)

    barrier = pltpu.get_barrier_semaphore()
    signal(barrier, upper_north + upper_south + upper_rest + upper_face + ahead + north)

    def settle(messages, flip, sem, known=()):
        if len(known) < 4:
            for has in (True, False):
                flag = links[len(known)][2]
                pl.when(flag if has else jnp.logical_not(flag))(
                    lambda has=has: settle(messages, flip, sem, known + (has,))
                )
            return
        total = sum(m.lines() for m in messages if all(known[w ^ flip] for w in m.needs))
        view = units.at[pl.ds(0, total)]
        pltpu.make_async_copy(view, view, sem).wait()

    def clear(ref):
        ref[...] = jnp.zeros(ref.shape, jnp.float32)

    for m in first + second + faces:
        if m.arrives is not None:
            pl.when(jnp.logical_not(m.arrives))(lambda m=m: clear(m.landing))
    clear(halo)

    lane = lax.broadcasted_iota(jnp.int32, (rows, cols), 1)
    group = lane // GROUP
    pool = (
        lax.broadcasted_iota(jnp.int32, (wide_cols, cols), 0) // fine
        == lax.broadcasted_iota(jnp.int32, (wide_cols, cols), 1)
    ).astype(jnp.float32).astype(jnp.bfloat16)

    loads[1].wait()
    for k in range(3):
        own[:, k + 1] = courant[k].astype(jnp.float32)
    loads[0].wait()
    sums[...] = jnp.dot(outer[...], pool, preferred_element_type=jnp.float32)
    coarse = sums[pl.ds(0, flat_rows, stride=fine), :]
    for k in range(1, fine):
        coarse = coarse + sums[pl.ds(k, flat_rows, stride=fine), :]
    own[:, 0] = (coarse * (1.0 / (fine * fine))).reshape(levels, rows, cols)

    ends_only = jnp.zeros((rows, cols), jnp.float32)
    for f in (1, 2, 3, 0):
        for l in range(levels):
            place = f * levels + l
            ends_only = jnp.where(group == place, pltpu.roll(own[l, f], (REACH + GROUP * place) % cols, axis=1), ends_only)
    strip[...] = ends_only

    entries = [(0, i, j) for i in range(1, REACH) for j in range(1, REACH + 1 - i)]
    entries = entries + [(f, i, j) for f in (1, 2, 3) for i in range(1, near) for j in range(1, near + 1 - i)]
    for s in range(2):
        for t in range(2):
            for n, (f, i, j) in enumerate(entries):
                l = levels - i if s == 0 else i - 1
                r = rows - j if t == 0 else j - 1
                edge_out[s, t, n : n + 1, :] = own[l, f, r : r + 1, :]

    def send(messages, test, side=None, later=0):
        for m in messages:
            if test(m.which) and m.later == later:
                m.start(None if side is None else side(m.which))

    def at_once(w):
        return (1 in w and not (corner(w) and 2 in w)) or w == [3]

    def north_corner(w):
        return corner(w) and 1 in w and 2 in w

    expected = count(lower + lower_south + lower_north + south + behind)
    pl.when(expected > 0)(lambda: pl.semaphore_wait(barrier, expected))
    signal(ready.at[4], [(w, is_behind(w)) for w, _ in lower_south])
    signal(ready.at[3], lower_rest)
    signal(ready.at[0], behind)
    signal(ready.at[2], lower_face)
    signal(ready.at[1], south)
    send(first, north_corner, is_behind)
    send(first, at_once)
    send(first, level_lon, is_behind)
    send(faces, at_once)

    row = lax.broadcasted_iota(jnp.int32, (rows, cols), 0)
    high = rows // TILE
    zero = jnp.zeros((rows, cols), jnp.float32)

    def inner(v, c, before, after):
        above = jnp.where(row == 0, 0.0, pltpu.roll(v, 1, axis=0))
        below = jnp.where(row == rows - 1, 0.0, pltpu.roll(v, rows - 1, axis=0))
        return forward(v, c, [before, above, pltpu.roll(v, 1, axis=1)], [after, below, pltpu.roll(v, cols - 1, axis=1)])

    def rim_rows(second_level, third_level):
        kept = [(second_level, 2, r) for r in (0, 1, rows - 2, rows - 1)]
        return kept + [(second_level, 3, r) for r in (0, rows - 1)] + [(third_level, 2, r) for r in (0, rows - 1)]

    pairs = ((levels - 2, levels - 3), (1, 2))
    once = {
        l: inner(own[l, 0], [own[l, k + 1] for k in range(3)], own[l - 1, 0], own[l + 1, 0])
        for l in sorted(set(pairs[0] + pairs[1]))
    }
    for s, (l, far) in enumerate(pairs):
        c = [own[l, k + 1] for k in range(3)]
        twice = inner(once[l], c, zero if s else once[far], once[far] if s else zero)
        for n, plane in enumerate((own[l, 0], once[l], twice, c[0])):
            deep_out[s, n * high : (n + 1) * high] = plane.reshape(high, TILE, cols)
        for n, (at, f, r) in enumerate(rim_rows(l, far)):
            deep_out[s, 4 * high, n : n + 1, :] = own[at, f, r : r + 1, :]

    view = units.at[pl.ds(0, 3 * col.shape[0])]
    pltpu.make_async_copy(view, view, in_sem.at[2]).wait()
    where_row = (lvl[...] - me_lev * levels + beyond) * rows + col[...] // cols
    where_col = col[...] % cols
    parts = bf16_parts(val[...], 2)
    pieces, width = col.shape
    row_id = lax.broadcasted_iota(jnp.int32, (span * rows, width), 0)
    col_id = lax.broadcasted_iota(jnp.int32, (cols, width), 0)
    hits = [[] for _ in range(3)]
    tables = []
    for k in range(pieces):
        match = where_row[k : k + 1] == row_id
        hits[0].append(jnp.where(match, 1.0, 0.0).astype(jnp.bfloat16))
        for i, part in enumerate(parts):
            hits[i + 1].append(jnp.where(match, part[k : k + 1], 0.0).astype(jnp.bfloat16))
        tables.append(jnp.where(where_col[k : k + 1] == col_id, 1.0, 0.0).astype(jnp.bfloat16))
    left_side = jnp.concatenate([jnp.concatenate(h, axis=1) for h in hits], axis=0)
    totals = lax.dot_general(
        left_side, jnp.concatenate(tables, axis=1), (((1,), (1,)), ((), ())),
        preferred_element_type=jnp.float32,
    )
    wide_rows = span * rows
    counted = totals[:wide_rows].reshape(span, rows, cols)
    summed = (totals[wide_rows : 2 * wide_rows] + totals[2 * wide_rows :]).reshape(span, rows, cols)
    seen[:, 0] = counted
    seen[:, 1] = summed
    for i, values in enumerate((counted, summed)):
        ends_only = jnp.zeros((rows, cols), jnp.float32)
        for g in range(span):
            place = g + REACH - beyond
            ends_only = jnp.where(group == place, pltpu.roll(values[g], (REACH + GROUP * place) % cols, axis=1), ends_only)
        seen_strip[i] = ends_only
    send(second, at_once)
    send(second, level_lon, is_behind)

    send(faces, at_once, later=2)

    @pl.when(links[2][2])
    def _():
        pl.semaphore_wait(ready.at[1], 1)
        send(first, north_corner, is_ahead)
        send(first + faces + second, lambda w: w == [2])

    @pl.when(me_lon < n_lon - 1)
    def _():
        pl.semaphore_wait(ready.at[0], count(ahead))
        send(first + second, level_lon, is_ahead)

    @pl.when(links[0][2])
    def _():
        pl.semaphore_wait(ready.at[2], 1)
        send(faces, lambda w: 0 in w)
        pl.semaphore_wait(ready.at[3], count(upper_rest))
        send(first, lambda w: 0 in w and not (corner(w) and 2 in w))
        send(first, lambda w: corner(w) and 0 in w and 2 in w, is_behind)

    @pl.when(links[0][2] & links[2][2] & (me_lon < n_lon - 1))
    def _():
        pl.semaphore_wait(ready.at[4], count([(w, is_ahead(w)) for w, _ in upper_north]))
        send(first, lambda w: corner(w) and 0 in w and 2 in w, is_ahead)

    pl.when(links[0][2])(lambda: send(faces, lambda w: 0 in w, later=2))

    settle(first, 1, recv_sem.at[0])

    tall = rows + TILE
    half = lax.broadcasted_iota(jnp.int32, (TILE, cols), 0) < TILE // 2
    lanes = lax.broadcasted_iota(jnp.int32, (tall, cols), 1)
    slot = lanes % GROUP
    left_half = slot < REACH
    blank = jnp.zeros((TILE, cols), jnp.float32)

    def joined(full, before, after):
        return jnp.concatenate([full, jnp.where(half, after, before)], axis=0)

    for s in range(2):
        for t in range(2):
            for n, (f, i, j) in enumerate(entries):
                r = TILE - j if t == 0 else j - 1
                halo[s, i - 1, f, r : r + 1, :] = edge_in[s, t, n : n + 1, :]

    def cell(l, f):
        if 0 <= l < levels:
            return joined(own[l, f], side_in[0, l, f], side_in[1, l, f])
        s, i = (0, -l) if l < 0 else (1, l - levels + 1)
        return jnp.concatenate([face_in[s, f], halo[s, i - 1, f]], axis=0)

    def down(x):
        return pltpu.roll(x, 1, axis=0)

    def up_row(x):
        return pltpu.roll(x, tall - 1, axis=0)

    def right(x, by=1):
        return pltpu.roll(x, by, axis=1)

    def left(x, by=1):
        return pltpu.roll(x, cols - by, axis=1)

    before_b, after_b = 1, (2 if n_lon > 2 else 1)

    def strip_block(a, b):
        full = strip[...] if a == 0 and b == 0 else strip_full[a, b]
        return joined(full, strip_half[a, 0, b], strip_half[a, 1, b])

    def placed(blocks, f):
        turned = [right(blocks[a], (GROUP * levels * (n - f)) % cols) if n != f else blocks[a] for n, a in enumerate((1, 0, 2))]
        width = GROUP * levels
        return jnp.where(lanes < width, turned[0], jnp.where(lanes < 2 * width, turned[1], turned[2]))

    mine = [strip_block(a, 0) for a in range(3)]
    sides = []
    sides.append([jnp.where(left_half, strip_block(a, before_b), mine[a]) for a in range(3)])
    sides.append([jnp.where(left_half, mine[a], strip_block(a, after_b)) for a in range(3)])
    side_c, side_v = [], []
    for blocks in sides:
        c = [placed(blocks, k + 1) for k in range(3)]
        v = placed(blocks, 0)
        for _ in range(2):
            v = forward(v, c, [right(v, GROUP), down(v), right(v)], [left(v, GROUP), up_row(v), left(v)])
        side_c.append(c)
        side_v.append(v)

    def inserted(z, l):
        return right(z, (cols - REACH - GROUP * (l + REACH)) % cols)

    def seen_block(b, i):
        full = seen_strip[i] if b == 0 else seen_full[b - 1, i]
        return joined(full, seen_half[0, b, i], seen_half[1, b, i])

    settle(second, 1, recv_sem.at[1])
    settle(faces, 1, recv_sem.at[2])
    side_q = []
    for side in range(2):
        known = []
        for i in range(2):
            if side == 0:
                known.append(jnp.where(left_half, seen_block(before_b, i), seen_block(0, i)))
            else:
                known.append(jnp.where(left_half, seen_block(0, i), seen_block(after_b, i)))
        p = known[0] * side_v[side] - known[1]
        c = side_c[side]
        low, up = shares(p, c)
        q = centre_of(c) * p + left(low[0], GROUP) + right(up[0], GROUP)
        q = q + up_row(low[1]) + down(up[1]) + left(low[2]) + right(up[2])
        low, up = shares(q, c)
        side_q.append((q, right(up[2]) if side == 0 else left(low[2])))
    fix = jnp.where(left_half, side_q[1][0], side_q[0][0])
    crossing = jnp.where(left_half, side_q[1][1], side_q[0][1])

    fix_v = jnp.where(left_half, side_v[1], side_v[0])
    fix_v = {l: inserted(fix_v, l) for l in range(2 - near - 1, levels + near - 1)}
    fix_q = {l: inserted(fix, l) for l in range(-1, levels + 1)}
    crossing = {l: inserted(crossing, l) for l in range(levels)}

    speeds = {l: [cell(l, k + 1) for k in range(3)] for l in range(-1, levels + 1)}
    start = {l: cell(l, 0) for l in range(-1, levels + 1)}
    beside = ((-2, -1, -3), (levels + 1, levels, levels + 2))

    def deep(s, n):
        return deep_in[s, n * high : (n + 1) * high].reshape(rows, cols)

    def kept_rows(s, places):
        plane = zero
        for n, r in places:
            plane = jnp.where(row == r, deep_in[s, 4 * high, n : n + 1, :], plane)
        return plane

    def across(c, x):
        above = jnp.where((row == 0) & (c > 0.0), down(x)[:rows], 0.0)
        below = jnp.where((row == rows - 1) & (c <= 0.0), up_row(x)[:rows], 0.0)
        return jnp.abs(c) * (above + below)

    def step(v, l):
        return forward(v[l], speeds[l], [v[l - 1], down(v[l]), right(v[l])], [v[l + 1], up_row(v[l]), left(v[l])])

    outside = []
    for s, (l, _, far) in enumerate(beside):
        c = [
            deep(s, 3),
            kept_rows(s, ((0, 0), (1, 1), (2, rows - 2), (3, rows - 1))),
            kept_rows(s, ((4, 0), (5, rows - 1))),
        ]
        start[l] = jnp.concatenate([deep(s, 0), halo[s, 1, 0]], axis=0)
        start[far] = jnp.concatenate([zero, halo[s, 2, 0]], axis=0)
        speeds[l] = [jnp.concatenate([c[k], halo[s, 1, k + 1]], axis=0) for k in range(3)]
        gained = across(c[1], start[l])
        further = across(kept_rows(s, ((6, 0), (7, rows - 1))), start[far])
        outside.append((c, gained, further))
    v = {l: step(start, l) for l in range(-1, levels + 1)}
    for s, (l, _, _) in enumerate(beside):
        v[l] = jnp.concatenate([deep(s, 1) + outside[s][1], step(start, l)[rows:]], axis=0)
    second_v = {l: step(v, l) for l in range(-1, levels + 1)}
    for s, (l, by, _) in enumerate(beside):
        c, gained, further = outside[s]
        sizes = [jnp.abs(n) for n in c]
        inward, outward = v[by][:rows], further
        crossed = jnp.concatenate([gained, v[l][rows:]], axis=0)
        total = deep(s, 2) + (1.0 - sizes[0] - sizes[1] - sizes[2]) * gained
        total = total + sizes[0] * jnp.where(c[0] > 0.0, inward if s else outward, outward if s else inward)
        total = total + sizes[1] * jnp.where(c[1] > 0.0, down(crossed)[:rows], up_row(crossed)[:rows])
        total = total + sizes[2] * jnp.where(
            c[2] > 0.0, pltpu.roll(gained, 1, axis=1), pltpu.roll(gained, cols - 1, axis=1)
        )
        second_v[l] = jnp.concatenate([total, blank], axis=0)
        speeds[l] = [jnp.concatenate([c[0], blank], axis=0)]
    v = second_v
    rim = (lanes < 2) | (lanes >= cols - 2)
    v = {l: jnp.where(rim, fix_v[l], v[l]) for l in v}
    for l in range(levels):
        state_v[l] = v[l][:rows]

    def seen_cell(l, i):
        g = l + beyond
        if 0 < g < span - 1:
            return joined(seen[g, i], seen_in[0, g - 1, i], seen_in[1, g - 1, i])
        return jnp.concatenate([seen[g, i], blank], axis=0)

    p = {l: seen_cell(l, 0) * v[l] - seen_cell(l, 1) for l in v}
    low, up = {}, {}
    for l in p:
        low[l], up[l] = shares(p[l], speeds[l])
    rim = (lanes < 1) | (lanes >= cols - 1)
    q = {}
    for l in range(-1, levels + 1):
        total = centre_of(speeds[l]) * p[l] + low[l + 1][0] + up[l - 1][0]
        total = total + up_row(low[l][1]) + down(up[l][1]) + left(low[l][2]) + right(up[l][2])
        q[l] = jnp.where(rim, fix_q[l], total)
    for l in q:
        low[l], up[l] = shares(q[l], speeds[l])
    for l in range(levels):
        total = centre_of(speeds[l]) * q[l] + low[l + 1][0] + up[l - 1][0]
        total = total + up_row(low[l][1]) + down(up[l][1])
        total = total + jnp.where(rim, crossing[l], 0.0)
        total = total + jnp.where(lanes >= cols - 1, 0.0, left(low[l][2])) + jnp.where(lanes < 1, 0.0, right(up[l][2]))
        adj_v[l] = total[:rows]

    settle(first + second + faces, 0, send_sem)


def finish(state_v, adj_v, outer, state_hbm, adj_hbm, next_hbm, wide, nxt, out_sem):
    levels, rows, cols = state_v.shape
    flat_rows = levels * rows
    wide_cols = outer.shape[1]
    fine = wide_cols // cols
    outer_rows = outer.shape[0] // levels
    stores = [
        pltpu.make_async_copy(state_v, state_hbm, out_sem.at[0]),
        pltpu.make_async_copy(adj_v, adj_hbm, out_sem.at[1]),
    ]
    for store in stores:
        store.start()
    field = adj_v[...]

    table = (
        lax.broadcasted_iota(jnp.int32, (cols, wide_cols), 0)
        == lax.broadcasted_iota(jnp.int32, (cols, wide_cols), 1) // fine
    ).astype(jnp.float32).astype(jnp.bfloat16)
    halves = bf16_parts(field.reshape(flat_rows, cols), 2)
    spread = jnp.dot(
        jnp.concatenate([h.astype(jnp.bfloat16) for h in halves], axis=1),
        jnp.concatenate([table, table], axis=0),
        preferred_element_type=jnp.float32,
    )
    for k in range(fine):
        for c in range(fine):
            wide[c, pl.ds(k, flat_rows, stride=fine), :] = spread[:, c * cols : (c + 1) * cols]
    for level in range(levels):
        span = pl.ds(level * outer_rows, outer_rows)
        for c in range(fine):
            lanes = pl.ds(c * cols, cols)
            nxt[span, lanes] = (outer[span, lanes].astype(jnp.float32) - wide[c, span, :]).astype(jnp.bfloat16)
        store = pltpu.make_async_copy(nxt.at[span], next_hbm.at[span], out_sem.at[2 + level])
        store.start()
        stores.append(store)
    for store in stores:
        store.wait()


def shards(ends, outer_increment, courant, obs_column, obs_level, obs_value):
    levels, outer_rows, wide_cols = outer_increment.shape
    _, _, rows, cols = courant.shape
    flat_rows = levels * rows
    fine = wide_cols // cols
    lanes = 128
    observed = (obs_column.shape[0] // lanes, lanes)
    span = levels + 4
    assert 4 * levels * GROUP == cols and levels >= REACH and rows % TILE == 0 and ends[1] > 1
    f32, bf16 = jnp.float32, jnp.bfloat16
    outer_shape = (levels * outer_rows, wide_cols)
    vmem = pl.BlockSpec(memory_space=pltpu.VMEM)
    hbm = pl.BlockSpec(memory_space=pl.ANY)
    held = pl.pallas_call(
        functools.partial(kernel, ends),
        out_shape=(
            pltpu.VMEM((levels, rows, cols), f32),
            pltpu.VMEM((levels, rows, cols), f32),
            pltpu.VMEM(outer_shape, bf16),
        ),
        in_specs=[hbm] * 5,
        out_specs=(vmem,) * 3,
        scratch_shapes=[
            pltpu.VMEM(courant.shape, bf16),
            pltpu.VMEM(observed, jnp.int32),
            pltpu.VMEM(observed, jnp.int32),
            pltpu.VMEM(observed, f32),
            pltpu.VMEM((levels * outer_rows, cols), f32),
            pltpu.VMEM((levels, 4, rows, cols), f32),
            pltpu.VMEM((2, 4, rows, cols), f32),
            pltpu.VMEM((2, 4 * rows // TILE + 1, TILE, cols), f32),
            pltpu.VMEM((2, 4 * rows // TILE + 1, TILE, cols), f32),
            pltpu.VMEM((2, levels, 4, TILE, cols), f32),
            pltpu.VMEM((2, 2, 2 * TILE, cols), f32),
            pltpu.VMEM((2, 2, 2 * TILE, cols), f32),
            pltpu.VMEM((2, REACH - 1, 4, TILE, cols), f32),
            pltpu.VMEM((rows, cols), f32),
            pltpu.VMEM((3, 3, rows, cols), f32),
            pltpu.VMEM((3, 2, 3, TILE, cols), f32),
            pltpu.VMEM((span, 2, rows, cols), f32),
            pltpu.VMEM((2, span - 2, 2, TILE, cols), f32),
            pltpu.VMEM((2, rows, cols), f32),
            pltpu.VMEM((2, 2, rows, cols), f32),
            pltpu.VMEM((2, 3, 2, TILE, cols), f32),
            pltpu.VMEM((2048, 1, cols), f32),
            pltpu.SemaphoreType.DMA((3,)),
            pltpu.SemaphoreType.DMA,
            pltpu.SemaphoreType.DMA((3,)),
            pltpu.SemaphoreType.REGULAR((5,)),
        ],
        compiler_params=pltpu.CompilerParams(collective_id=0, has_side_effects=True),
    )(
        outer_increment.reshape(outer_shape),
        courant,
        obs_column.reshape(observed),
        obs_level.reshape(observed),
        obs_value.reshape(observed),
    )
    state, adjoint, following = pl.pallas_call(
        finish,
        out_shape=(
            jax.ShapeDtypeStruct((levels, rows, cols), f32),
            jax.ShapeDtypeStruct((levels, rows, cols), f32),
            jax.ShapeDtypeStruct(outer_shape, bf16),
        ),
        in_specs=[vmem] * 3,
        out_specs=(hbm,) * 3,
        scratch_shapes=[
            pltpu.VMEM((fine, levels * outer_rows, cols), f32),
            pltpu.VMEM(outer_shape, bf16),
            pltpu.SemaphoreType.DMA((2 + levels,)),
        ],
    )(*[pltpu.with_memory_space_constraint(x, pltpu.VMEM) for x in held])
    return state, adjoint, following.reshape(outer_increment.shape)


def solution(mesh):
    ends = tuple(mesh.shape[a] for a in ("lat", "lon", "lev"))
    block = P("lev", "lat", "lon")
    observed = P(("lat", "lon"))
    return jax.shard_map(
        functools.partial(shards, ends),
        mesh=mesh,
        in_specs=(block, P(None, "lev", "lat", "lon"), observed, observed, observed),
        out_specs=(block, block, block),
        check_vma=False,
    )
```

```python
import functools

import jax
import jax.numpy as jnp
from jax import lax
from jax.experimental import pallas as pl
from jax.experimental.pallas import tpu as pltpu
from jax.sharding import PartitionSpec as P

MESH = pl.DeviceIdType.MESH
REACH = 4
GROUP = 2 * REACH
TILE = 8


def bf16_parts(x, count):
    parts = []
    for _ in range(count):
        part = x.astype(jnp.bfloat16).astype(jnp.float32)
        parts.append(part)
        x = x - part
    return parts


def forward(v, c, minus, plus):
    sizes = [jnp.abs(n) for n in c]
    result = (1.0 - sizes[0] - sizes[1] - sizes[2]) * v
    for k in range(3):
        result = result + sizes[k] * jnp.where(c[k] > 0.0, minus[k], plus[k])
    return result


def again(v, c, minus, plus):
    result = centre_of(c) * v
    for k in range(3):
        low = jnp.maximum(c[k], 0.0)
        result = result + low * minus[k] + (low - c[k]) * plus[k]
    return result


def shares(p, c):
    low, up = [], []
    for n in c:
        low.append(jnp.maximum(n, 0.0) * p)
        up.append(low[-1] - n * p)
    return low, up


def centre_of(c):
    return 1.0 - jnp.abs(c[0]) - jnp.abs(c[1]) - jnp.abs(c[2])


def kernel(
    ends, outer_hbm, courant_hbm, col_hbm, lvl_hbm, val_hbm,
    state_v, adj_v, outer,
    courant, col, lvl, val, sums,
    own, face_in, deep_out, deep_in, side_in, edge_out, edge_in, halo,
    strip, strip_full, strip_half,
    seen, seen_in, seen_strip, seen_full, seen_half, units,
    in_sem, send_sem, recv_sem, ready,
):
    n_lat, n_lon, n_lev = ends
    levels, rows, cols = state_v.shape
    flat_rows = levels * rows
    wide_cols = outer.shape[1]
    fine = wide_cols // cols
    near = REACH - 1
    span = seen.shape[0]
    beyond = (span - levels) // 2

    loads = [
        pltpu.make_async_copy(src, dst, in_sem.at[min(i, 2)])
        for i, (src, dst) in enumerate(
            ((outer_hbm, outer), (courant_hbm, courant), (col_hbm, col), (lvl_hbm, lvl), (val_hbm, val))
        )
    ]
    for load in loads:
        load.start()

    me_lat, me_lon, me_lev = (lax.axis_index(a) for a in ("lat", "lon", "lev"))
    links = (
        ("lev", me_lev + 1, me_lev < n_lev - 1),
        ("lev", me_lev - 1, me_lev > 0),
        ("lat", me_lat + 1, me_lat < n_lat - 1),
        ("lat", me_lat - 1, me_lat > 0),
        ("lon", lax.rem(me_lon + 1, n_lon), None),
        ("lon", lax.rem(me_lon + n_lon - 1, n_lon), None),
    )
    turns = (0, 1) if n_lon > 2 else (0,)
    bands = ((rows - TILE, TILE), (0, TILE))

    def both(flags):
        return functools.reduce(jnp.logical_and, flags) if flags else None

    def guarded(exists, action):
        if exists is None:
            action()
        else:
            pl.when(exists)(action)

    def flags_of(which):
        return [links[w][2] for w in which if w < 4]

    def lon_of(which):
        return [w for w in which if w > 3]

    def is_ahead(which):
        return me_lon < links[lon_of(which)[0]][1]

    def is_behind(which):
        return me_lon > links[lon_of(which)[0]][1]

    class Message:
        def __init__(self, which, source, landing, sem, later=0):
            self.which, self.later = which, later
            self.needs = tuple(w for w in which if w < 4)
            self.target = {links[w][0]: links[w][1] for w in which}
            self.arrives = both([links[w ^ 1][2] for w in self.needs])
            self.source, self.landing, self.sem = source, landing, sem

        def start(self, flag=None):
            def begin():
                pltpu.make_async_remote_copy(
                    src_ref=self.source, dst_ref=self.landing, send_sem=send_sem, recv_sem=recv_sem.at[self.sem],
                    device_id=self.target, device_id_type=MESH,
                ).start()

            guarded(both(flags_of(self.which) + ([] if flag is None else [flag])), begin)

        def lines(self):
            total = 1
            for n in self.landing.shape:
                total = total * n
            return total // cols

    partners, first, second, faces = [], [], [], []
    for a in (2, 1, 0):
        for t in (0, 1, None):
            for u in turns + (None,):
                which = [a - 1] if a else []
                which = which + ([2 + t] if t is not None else []) + ([4 + u] if u is not None else [])
                if not which:
                    continue
                partners.append(which)
                b = 0 if u is None else u + 1
                if t is None:
                    first.append(Message(which, strip, strip_full.at[a, b], 0))
                else:
                    first.append(Message(which, strip.at[pl.ds(*bands[t])], strip_half.at[a, t, b], 0))
                if u is None:
                    if a and t is None:
                        faces.append(Message(which, own.at[levels - 1 if a == 1 else 0], face_in.at[a - 1], 1))
                        faces.append(Message(which, deep_out.at[a - 1], deep_in.at[a - 1], 1, 2))
                    elif a:
                        first.append(Message(which, edge_out.at[a - 1, t], edge_in.at[a - 1, t], 0))
                    else:
                        first.append(Message(which, own.at[:, :, pl.ds(*bands[t])], side_in.at[t], 0))
                if not a:
                    if t is None:
                        second.append(Message(which, seen_strip, seen_full.at[u], 1))
                    else:
                        second.append(Message(which, seen_strip.at[:, pl.ds(*bands[t])], seen_half.at[t, b], 1))
                    if u is None:
                        kept = pl.ds(1, span - 2)
                        second.append(Message(which, seen.at[kept, :, pl.ds(*bands[t])], seen_in.at[t], 1))
    first.sort(key=lambda m: m.lines() - 1024 * len(m.target))

    def pick(test, side=None):
        return [(which, None if side is None else side(which)) for which in partners if test(which)]

    def count(chosen):
        total = 0
        for which, flag in chosen:
            exists = both(flags_of(which) + ([] if flag is None else [flag]))
            total = total + (1 if exists is None else exists.astype(jnp.int32))
        return total

    def signal(sem, chosen):
        for which, flag in chosen:
            target = {links[w][0]: links[w][1] for w in which}
            guarded(
                both(flags_of(which) + ([] if flag is None else [flag])),
                lambda target=target: pl.semaphore_signal(sem, inc=1, device_id=target, device_id_type=MESH),
            )

    def level_lon(which):
        return lon_of(which) and not {0, 1} & set(which)

    def corner(which):
        return len(which) == 3

    lower = pick(lambda w: 1 in w and not corner(w))
    upper = pick(lambda w: 0 in w and not corner(w))
    lower_face, upper_face = [[c for c in side if len(c[0]) == 1] for side in (lower, upper)]
    lower_rest, upper_rest = [[c for c in side if len(c[0]) > 1] for side in (lower, upper)]
    lower_south = pick(lambda w: corner(w) and 1 in w and 3 in w)
    upper_north = pick(lambda w: corner(w) and 0 in w and 2 in w)
    lower_north = pick(lambda w: corner(w) and 1 in w and 2 in w, is_behind)
    upper_south = pick(lambda w: corner(w) and 0 in w and 3 in w, is_ahead)
    south, north = pick(lambda w: w == [3]), pick(lambda w: w == [2])
    behind, ahead = pick(level_lon, is_behind), pick(level_lon, is_ahead)

    barrier = pltpu.get_barrier_semaphore()
    signal(barrier, upper_rest[::-1] + upper_north + upper_face + ahead + upper_south + north)

    def settle(messages, flip, sem, known=()):
        if len(known) < 4:
            for has in (True, False):
                flag = links[len(known)][2]
                pl.when(flag if has else jnp.logical_not(flag))(
                    lambda has=has: settle(messages, flip, sem, known + (has,))
                )
            return
        total = sum(m.lines() for m in messages if all(known[w ^ flip] for w in m.needs))
        view = units.at[pl.ds(0, total)]
        pltpu.make_async_copy(view, view, sem).wait()

    def clear(ref):
        ref[...] = jnp.zeros(ref.shape, jnp.float32)

    for m in first + second + faces:
        if m.arrives is not None:
            pl.when(jnp.logical_not(m.arrives))(lambda m=m: clear(m.landing))
    clear(halo)

    lane = lax.broadcasted_iota(jnp.int32, (rows, cols), 1)
    group = lane // GROUP
    pool = (
        lax.broadcasted_iota(jnp.int32, (wide_cols, cols), 0) // fine
        == lax.broadcasted_iota(jnp.int32, (wide_cols, cols), 1)
    ).astype(jnp.float32).astype(jnp.bfloat16)

    loads[1].wait()
    for k in range(3):
        own[:, k + 1] = courant[k].astype(jnp.float32)
    loads[0].wait()
    sums[...] = jnp.dot(outer[...], pool, preferred_element_type=jnp.float32)
    coarse = sums[pl.ds(0, flat_rows, stride=fine), :]
    for k in range(1, fine):
        coarse = coarse + sums[pl.ds(k, flat_rows, stride=fine), :]
    own[:, 0] = (coarse * (1.0 / (fine * fine))).reshape(levels, rows, cols)

    ends_only = jnp.zeros((rows, cols), jnp.float32)
    for f in (1, 2, 3, 0):
        for l in range(levels):
            place = f * levels + l
            ends_only = jnp.where(group == place, pltpu.roll(own[l, f], (REACH + GROUP * place) % cols, axis=1), ends_only)
    strip[...] = ends_only

    entries = [(0, i, j) for i in range(1, REACH) for j in range(1, REACH + 1 - i)]
    entries = entries + [(f, i, j) for f in (1, 2, 3) for i in range(1, near) for j in range(1, near + 1 - i)]
    for s in range(2):
        for t in range(2):
            for n, (f, i, j) in enumerate(entries):
                l = levels - i if s == 0 else i - 1
                r = rows - j if t == 0 else j - 1
                edge_out[s, t, n : n + 1, :] = own[l, f, r : r + 1, :]

    def send(messages, test, side=None, later=0):
        for m in messages:
            if test(m.which) and m.later == later:
                m.start(None if side is None else side(m.which))

    def at_once(w):
        return (1 in w and not (corner(w) and 2 in w)) or w == [3]

    def north_corner(w):
        return corner(w) and 1 in w and 2 in w

    expected = count(lower + lower_south + lower_north + south + behind)
    pl.when(expected > 0)(lambda: pl.semaphore_wait(barrier, expected))
    signal(ready.at[4], [(w, is_behind(w)) for w, _ in lower_south])
    signal(ready.at[3], lower_rest)
    signal(ready.at[0], behind)
    signal(ready.at[2], lower_face)
    signal(ready.at[1], south)
    send(first, north_corner, is_behind)
    send(first, at_once)
    send(first, level_lon, is_behind)
    send(faces, at_once)

    row = lax.broadcasted_iota(jnp.int32, (rows, cols), 0)
    high = rows // TILE
    zero = jnp.zeros((rows, cols), jnp.float32)

    def inner(v, c, before, after):
        above = jnp.where(row == 0, 0.0, pltpu.roll(v, 1, axis=0))
        below = jnp.where(row == rows - 1, 0.0, pltpu.roll(v, rows - 1, axis=0))
        return forward(v, c, [before, above, pltpu.roll(v, 1, axis=1)], [after, below, pltpu.roll(v, cols - 1, axis=1)])

    def rim_rows(second_level, third_level):
        kept = [(second_level, 2, r) for r in (0, 1, rows - 2, rows - 1)]
        return kept + [(second_level, 3, r) for r in (0, rows - 1)] + [(third_level, 2, r) for r in (0, rows - 1)]

    pairs = ((levels - 2, levels - 3), (1, 2))
    once = {
        l: inner(own[l, 0], [own[l, k + 1] for k in range(3)], own[l - 1, 0], own[l + 1, 0])
        for l in sorted(set(pairs[0] + pairs[1]))
    }
    for s, (l, far) in enumerate(pairs):
        c = [own[l, k + 1] for k in range(3)]
        twice = inner(once[l], c, zero if s else once[far], once[far] if s else zero)
        for n, plane in enumerate((own[l, 0], once[l], twice, c[0])):
            deep_out[s, n * high : (n + 1) * high] = plane.reshape(high, TILE, cols)
        for n, (at, f, r) in enumerate(rim_rows(l, far)):
            deep_out[s, 4 * high, n : n + 1, :] = own[at, f, r : r + 1, :]

    view = units.at[pl.ds(0, 3 * col.shape[0])]
    pltpu.make_async_copy(view, view, in_sem.at[2]).wait()
    where_row = (lvl[...] - me_lev * levels + beyond) * rows + col[...] // cols
    where_col = col[...] % cols
    parts = bf16_parts(val[...], 2)
    pieces, width = col.shape
    row_id = lax.broadcasted_iota(jnp.int32, (span * rows, width), 0)
    col_id = lax.broadcasted_iota(jnp.int32, (cols, width), 0)
    hits = [[] for _ in range(3)]
    tables = []
    for k in range(pieces):
        match = where_row[k : k + 1] == row_id
        hits[0].append(jnp.where(match, 1.0, 0.0).astype(jnp.bfloat16))
        for i, part in enumerate(parts):
            hits[i + 1].append(jnp.where(match, part[k : k + 1], 0.0).astype(jnp.bfloat16))
        tables.append(jnp.where(where_col[k : k + 1] == col_id, 1.0, 0.0).astype(jnp.bfloat16))
    left_side = jnp.concatenate([jnp.concatenate(h, axis=1) for h in hits], axis=0)
    totals = lax.dot_general(
        left_side, jnp.concatenate(tables, axis=1), (((1,), (1,)), ((), ())),
        preferred_element_type=jnp.float32,
    )
    wide_rows = span * rows
    counted = totals[:wide_rows].reshape(span, rows, cols)
    summed = (totals[wide_rows : 2 * wide_rows] + totals[2 * wide_rows :]).reshape(span, rows, cols)
    seen[:, 0] = counted
    seen[:, 1] = summed
    for i, values in enumerate((counted, summed)):
        ends_only = jnp.zeros((rows, cols), jnp.float32)
        for g in range(span):
            place = g + REACH - beyond
            ends_only = jnp.where(group == place, pltpu.roll(values[g], (REACH + GROUP * place) % cols, axis=1), ends_only)
        seen_strip[i] = ends_only
    send(second, at_once)
    send(second, level_lon, is_behind)

    send(faces, at_once, later=2)

    @pl.when(links[2][2])
    def _():
        pl.semaphore_wait(ready.at[1], 1)
        send(first, north_corner, is_ahead)
        send(first + second, lambda w: w == [2])

    @pl.when(me_lon < n_lon - 1)
    def _():
        pl.semaphore_wait(ready.at[0], count(ahead))
        send(first + second, level_lon, is_ahead)

    @pl.when(links[0][2])
    def _():
        pl.semaphore_wait(ready.at[2], 1)
        send(faces, lambda w: 0 in w)
        pl.semaphore_wait(ready.at[3], count(upper_rest))
        send(first, lambda w: 0 in w and not (corner(w) and 2 in w))
        send(first, lambda w: corner(w) and 0 in w and 2 in w, is_behind)

    @pl.when(links[0][2] & links[2][2] & (me_lon < n_lon - 1))
    def _():
        pl.semaphore_wait(ready.at[4], count([(w, is_ahead(w)) for w, _ in upper_north]))
        send(first, lambda w: corner(w) and 0 in w and 2 in w, is_ahead)

    pl.when(links[0][2])(lambda: send(faces, lambda w: 0 in w, later=2))

    settle(first, 1, recv_sem.at[0])

    tall = rows + TILE
    half = lax.broadcasted_iota(jnp.int32, (TILE, cols), 0) < TILE // 2
    lanes = lax.broadcasted_iota(jnp.int32, (tall, cols), 1)
    slot = lanes % GROUP
    left_half = slot < REACH
    blank = jnp.zeros((TILE, cols), jnp.float32)

    def joined(full, before, after):
        return jnp.concatenate([full, jnp.where(half, after, before)], axis=0)

    for s in range(2):
        for t in range(2):
            for n, (f, i, j) in enumerate(entries):
                r = TILE - j if t == 0 else j - 1
                halo[s, i - 1, f, r : r + 1, :] = edge_in[s, t, n : n + 1, :]

    def cell(l, f):
        if 0 <= l < levels:
            return joined(own[l, f], side_in[0, l, f], side_in[1, l, f])
        s, i = (0, -l) if l < 0 else (1, l - levels + 1)
        return jnp.concatenate([face_in[s, f], halo[s, i - 1, f]], axis=0)

    def down(x):
        return pltpu.roll(x, 1, axis=0)

    def up_row(x):
        return pltpu.roll(x, tall - 1, axis=0)

    def right(x, by=1):
        return pltpu.roll(x, by, axis=1)

    def left(x, by=1):
        return pltpu.roll(x, cols - by, axis=1)

    before_b, after_b = 1, (2 if n_lon > 2 else 1)

    def strip_block(a, b):
        full = strip[...] if a == 0 and b == 0 else strip_full[a, b]
        return joined(full, strip_half[a, 0, b], strip_half[a, 1, b])

    def placed(blocks, f):
        turned = [right(blocks[a], (GROUP * levels * (n - f)) % cols) if n != f else blocks[a] for n, a in enumerate((1, 0, 2))]
        width = GROUP * levels
        return jnp.where(lanes < width, turned[0], jnp.where(lanes < 2 * width, turned[1], turned[2]))

    mine = [strip_block(a, 0) for a in range(3)]
    sides = []
    sides.append([jnp.where(left_half, strip_block(a, before_b), mine[a]) for a in range(3)])
    sides.append([jnp.where(left_half, mine[a], strip_block(a, after_b)) for a in range(3)])
    side_c, side_v = [], []
    for blocks in sides:
        c = [placed(blocks, k + 1) for k in range(3)]
        v = placed(blocks, 0)
        for _ in range(2):
            v = forward(v, c, [right(v, GROUP), down(v), right(v)], [left(v, GROUP), up_row(v), left(v)])
        side_c.append(c)
        side_v.append(v)

    def inserted(z, l):
        return right(z, (cols - REACH - GROUP * (l + REACH)) % cols)

    def seen_block(b, i):
        full = seen_strip[i] if b == 0 else seen_full[b - 1, i]
        return joined(full, seen_half[0, b, i], seen_half[1, b, i])

    speeds = {l: [cell(l, k + 1) for k in range(3)] for l in range(levels)}
    start = {l: cell(l, 0) for l in range(levels)}

    def lev_term(v, l):
        n = speeds[l][0]
        return jnp.abs(n) * jnp.where(n > 0.0, v[l - 1], v[l + 1])

    def within(v, l):
        result = centre_of(speeds[l]) * v[l]
        for n, minus, plus in zip(speeds[l][1:], (down(v[l]), right(v[l])), (up_row(v[l]), left(v[l]))):
            result = result + jnp.abs(n) * jnp.where(n > 0.0, minus, plus)
        return result

    begun = {l: within(start, l) for l in range(levels)}
    begun = {l: begun[l] + lev_term(start, l) if 0 < l < levels - 1 else begun[l] for l in begun}

    settle(second + faces, 1, recv_sem.at[1])
    side_q = []
    for side in range(2):
        known = []
        for i in range(2):
            if side == 0:
                known.append(jnp.where(left_half, seen_block(before_b, i), seen_block(0, i)))
            else:
                known.append(jnp.where(left_half, seen_block(0, i), seen_block(after_b, i)))
        p = known[0] * side_v[side] - known[1]
        c = side_c[side]
        low, up = shares(p, c)
        q = centre_of(c) * p + left(low[0], GROUP) + right(up[0], GROUP)
        q = q + up_row(low[1]) + down(up[1]) + left(low[2]) + right(up[2])
        low, up = shares(q, c)
        side_q.append((q, right(up[2]) if side == 0 else left(low[2])))
    fix = jnp.where(left_half, side_q[1][0], side_q[0][0])
    crossing = jnp.where(left_half, side_q[1][1], side_q[0][1])

    fix_v = jnp.where(left_half, side_v[1], side_v[0])
    fix_v = {l: inserted(fix_v, l) for l in range(2 - near - 1, levels + near - 1)}
    fix_q = {l: inserted(fix, l) for l in range(-1, levels + 1)}
    crossing = {l: inserted(crossing, l) for l in range(levels)}

    for l in (-1, levels):
        speeds[l] = [cell(l, k + 1) for k in range(3)]
        start[l] = cell(l, 0)
    beside = ((-2, -1, -3), (levels + 1, levels, levels + 2))

    def deep(s, n):
        return deep_in[s, n * high : (n + 1) * high].reshape(rows, cols)

    def kept_rows(s, places):
        plane = zero
        for n, r in places:
            plane = jnp.where(row == r, deep_in[s, 4 * high, n : n + 1, :], plane)
        return plane

    def across(c, x):
        above = jnp.where((row == 0) & (c > 0.0), down(x)[:rows], 0.0)
        below = jnp.where((row == rows - 1) & (c <= 0.0), up_row(x)[:rows], 0.0)
        return jnp.abs(c) * (above + below)

    def step(v, l, rule=forward):
        return rule(v[l], speeds[l], [v[l - 1], down(v[l]), right(v[l])], [v[l + 1], up_row(v[l]), left(v[l])])

    outside = []
    for s, (l, _, far) in enumerate(beside):
        c = [
            deep(s, 3),
            kept_rows(s, ((0, 0), (1, 1), (2, rows - 2), (3, rows - 1))),
            kept_rows(s, ((4, 0), (5, rows - 1))),
        ]
        start[l] = jnp.concatenate([deep(s, 0), halo[s, 1, 0]], axis=0)
        start[far] = jnp.concatenate([zero, halo[s, 2, 0]], axis=0)
        speeds[l] = [jnp.concatenate([c[k], halo[s, 1, k + 1]], axis=0) for k in range(3)]
        gained = across(c[1], start[l])
        further = across(kept_rows(s, ((6, 0), (7, rows - 1))), start[far])
        outside.append((c, gained, further))
    v = {l: step(start, l) for l in (-1, levels)}
    for l in range(levels):
        v[l] = begun[l] if 0 < l < levels - 1 else begun[l] + lev_term(start, l)
    for s, (l, _, _) in enumerate(beside):
        v[l] = jnp.concatenate([deep(s, 1) + outside[s][1], step(start, l)[rows:]], axis=0)
    second_v = {l: step(v, l, again) for l in range(-1, levels + 1)}
    for s, (l, by, _) in enumerate(beside):
        c, gained, further = outside[s]
        sizes = [jnp.abs(n) for n in c]
        inward, outward = v[by][:rows], further
        crossed = jnp.concatenate([gained, v[l][rows:]], axis=0)
        total = deep(s, 2) + (1.0 - sizes[0] - sizes[1] - sizes[2]) * gained
        total = total + sizes[0] * jnp.where(c[0] > 0.0, inward if s else outward, outward if s else inward)
        total = total + sizes[1] * jnp.where(c[1] > 0.0, down(crossed)[:rows], up_row(crossed)[:rows])
        total = total + sizes[2] * jnp.where(
            c[2] > 0.0, pltpu.roll(gained, 1, axis=1), pltpu.roll(gained, cols - 1, axis=1)
        )
        second_v[l] = jnp.concatenate([total, blank], axis=0)
        speeds[l] = [jnp.concatenate([c[0], blank], axis=0)]
    v = second_v
    rim = (lanes < 2) | (lanes >= cols - 2)
    v = {l: jnp.where(rim, fix_v[l], v[l]) for l in v}
    for l in range(levels):
        state_v[l] = v[l][:rows]

    def seen_cell(l, i):
        g = l + beyond
        if 0 < g < span - 1:
            return joined(seen[g, i], seen_in[0, g - 1, i], seen_in[1, g - 1, i])
        return jnp.concatenate([seen[g, i], blank], axis=0)

    p = {l: seen_cell(l, 0) * v[l] - seen_cell(l, 1) for l in v}
    low, up = {}, {}
    for l in p:
        low[l], up[l] = shares(p[l], speeds[l])
    rim = (lanes < 1) | (lanes >= cols - 1)
    q = {}
    for l in range(-1, levels + 1):
        total = centre_of(speeds[l]) * p[l] + low[l + 1][0] + up[l - 1][0]
        total = total + up_row(low[l][1]) + down(up[l][1]) + left(low[l][2]) + right(up[l][2])
        q[l] = jnp.where(rim, fix_q[l], total)
    for l in q:
        low[l], up[l] = shares(q[l], speeds[l])
    for l in range(levels):
        total = centre_of(speeds[l]) * q[l] + low[l + 1][0] + up[l - 1][0]
        total = total + up_row(low[l][1]) + down(up[l][1])
        total = total + jnp.where(rim, crossing[l], 0.0)
        total = total + jnp.where(lanes >= cols - 1, 0.0, left(low[l][2])) + jnp.where(lanes < 1, 0.0, right(up[l][2]))
        adj_v[l] = total[:rows]

    settle(first + second + faces, 0, send_sem)


def finish(state_v, adj_v, outer, state_hbm, adj_hbm, next_hbm, wide, nxt, out_sem):
    levels, rows, cols = state_v.shape
    flat_rows = levels * rows
    wide_cols = outer.shape[1]
    fine = wide_cols // cols
    outer_rows = outer.shape[0] // levels
    stores = [
        pltpu.make_async_copy(state_v, state_hbm, out_sem.at[0]),
        pltpu.make_async_copy(adj_v, adj_hbm, out_sem.at[1]),
    ]
    for store in stores:
        store.start()
    field = adj_v[...]

    table = (
        lax.broadcasted_iota(jnp.int32, (cols, wide_cols), 0)
        == lax.broadcasted_iota(jnp.int32, (cols, wide_cols), 1) // fine
    ).astype(jnp.float32).astype(jnp.bfloat16)
    halves = bf16_parts(field.reshape(flat_rows, cols), 2)
    spread = jnp.dot(
        jnp.concatenate([h.astype(jnp.bfloat16) for h in halves], axis=1),
        jnp.concatenate([table, table], axis=0),
        preferred_element_type=jnp.float32,
    )
    for k in range(fine):
        for c in range(fine):
            wide[c, pl.ds(k, flat_rows, stride=fine), :] = spread[:, c * cols : (c + 1) * cols]
    for level in range(levels):
        span = pl.ds(level * outer_rows, outer_rows)
        for c in range(fine):
            lanes = pl.ds(c * cols, cols)
            nxt[span, lanes] = (outer[span, lanes].astype(jnp.float32) - wide[c, span, :]).astype(jnp.bfloat16)
        store = pltpu.make_async_copy(nxt.at[span], next_hbm.at[span], out_sem.at[2 + level])
        store.start()
        stores.append(store)
    for store in stores:
        store.wait()


def shards(ends, outer_increment, courant, obs_column, obs_level, obs_value):
    levels, outer_rows, wide_cols = outer_increment.shape
    _, _, rows, cols = courant.shape
    flat_rows = levels * rows
    fine = wide_cols // cols
    lanes = 128
    observed = (obs_column.shape[0] // lanes, lanes)
    span = levels + 4
    assert 4 * levels * GROUP == cols and levels >= REACH and rows % TILE == 0 and ends[1] > 1
    f32, bf16 = jnp.float32, jnp.bfloat16
    outer_shape = (levels * outer_rows, wide_cols)
    vmem = pl.BlockSpec(memory_space=pltpu.VMEM)
    hbm = pl.BlockSpec(memory_space=pl.ANY)
    held = pl.pallas_call(
        functools.partial(kernel, ends),
        out_shape=(
            pltpu.VMEM((levels, rows, cols), f32),
            pltpu.VMEM((levels, rows, cols), f32),
            pltpu.VMEM(outer_shape, bf16),
        ),
        in_specs=[hbm] * 5,
        out_specs=(vmem,) * 3,
        scratch_shapes=[
            pltpu.VMEM(courant.shape, bf16),
            pltpu.VMEM(observed, jnp.int32),
            pltpu.VMEM(observed, jnp.int32),
            pltpu.VMEM(observed, f32),
            pltpu.VMEM((levels * outer_rows, cols), f32),
            pltpu.VMEM((levels, 4, rows, cols), f32),
            pltpu.VMEM((2, 4, rows, cols), f32),
            pltpu.VMEM((2, 4 * rows // TILE + 1, TILE, cols), f32),
            pltpu.VMEM((2, 4 * rows // TILE + 1, TILE, cols), f32),
            pltpu.VMEM((2, levels, 4, TILE, cols), f32),
            pltpu.VMEM((2, 2, 2 * TILE, cols), f32),
            pltpu.VMEM((2, 2, 2 * TILE, cols), f32),
            pltpu.VMEM((2, REACH - 1, 4, TILE, cols), f32),
            pltpu.VMEM((rows, cols), f32),
            pltpu.VMEM((3, 3, rows, cols), f32),
            pltpu.VMEM((3, 2, 3, TILE, cols), f32),
            pltpu.VMEM((span, 2, rows, cols), f32),
            pltpu.VMEM((2, span - 2, 2, TILE, cols), f32),
            pltpu.VMEM((2, rows, cols), f32),
            pltpu.VMEM((2, 2, rows, cols), f32),
            pltpu.VMEM((2, 3, 2, TILE, cols), f32),
            pltpu.VMEM((2048, 1, cols), f32),
            pltpu.SemaphoreType.DMA((3,)),
            pltpu.SemaphoreType.DMA,
            pltpu.SemaphoreType.DMA((2,)),
            pltpu.SemaphoreType.REGULAR((5,)),
        ],
        compiler_params=pltpu.CompilerParams(collective_id=0, has_side_effects=True),
    )(
        outer_increment.reshape(outer_shape),
        courant,
        obs_column.reshape(observed),
        obs_level.reshape(observed),
        obs_value.reshape(observed),
    )
    state, adjoint, following = pl.pallas_call(
        finish,
        out_shape=(
            jax.ShapeDtypeStruct((levels, rows, cols), f32),
            jax.ShapeDtypeStruct((levels, rows, cols), f32),
            jax.ShapeDtypeStruct(outer_shape, bf16),
        ),
        in_specs=[vmem] * 3,
        out_specs=(hbm,) * 3,
        scratch_shapes=[
            pltpu.VMEM((fine, levels * outer_rows, cols), f32),
            pltpu.VMEM(outer_shape, bf16),
            pltpu.SemaphoreType.DMA((2 + levels,)),
        ],
    )(*[pltpu.with_memory_space_constraint(x, pltpu.VMEM) for x in held])
    return state, adjoint, following.reshape(outer_increment.shape)


def solution(mesh):
    ends = tuple(mesh.shape[a] for a in ("lat", "lon", "lev"))
    block = P("lev", "lat", "lon")
    observed = P(("lat", "lon"))
    return jax.shard_map(
        functools.partial(shards, ends),
        mesh=mesh,
        in_specs=(block, P(None, "lev", "lat", "lon"), observed, observed, observed),
        out_specs=(block, block, block),
        check_vma=False,
    )
```

```python
import functools

import jax
import jax.numpy as jnp
from jax import lax
from jax.experimental import pallas as pl
from jax.experimental.pallas import tpu as pltpu
from jax.sharding import PartitionSpec as P

MESH = pl.DeviceIdType.MESH
REACH = 4
GROUP = 2 * REACH
TILE = 8


def bf16_parts(x, count):
    parts = []
    for _ in range(count):
        part = x.astype(jnp.bfloat16).astype(jnp.float32)
        parts.append(part)
        x = x - part
    return parts


def forward(v, c, minus, plus):
    sizes = [jnp.abs(n) for n in c]
    result = (1.0 - sizes[0] - sizes[1] - sizes[2]) * v
    for k in range(3):
        result = result + sizes[k] * jnp.where(c[k] > 0.0, minus[k], plus[k])
    return result


def again(v, c, minus, plus):
    result = centre_of(c) * v
    for k in range(3):
        low = jnp.maximum(c[k], 0.0)
        result = result + low * minus[k] + (low - c[k]) * plus[k]
    return result


def shares(p, c):
    low, up = [], []
    for n in c:
        low.append(jnp.maximum(n, 0.0) * p)
        up.append(low[-1] - n * p)
    return low, up


def centre_of(c):
    return 1.0 - jnp.abs(c[0]) - jnp.abs(c[1]) - jnp.abs(c[2])


def kernel(
    ends, outer_hbm, courant_hbm, col_hbm, lvl_hbm, val_hbm,
    state_v, adj_v, outer,
    courant, col, lvl, val, sums,
    own, face_in, deep_out, deep_in, side_in, edge_out, edge_in, halo,
    strip, strip_full, strip_half,
    seen, seen_in, seen_strip, seen_full, seen_half, units,
    in_sem, send_sem, recv_sem, ready,
):
    n_lat, n_lon, n_lev = ends
    levels, rows, cols = state_v.shape
    flat_rows = levels * rows
    wide_cols = outer.shape[1]
    fine = wide_cols // cols
    near = REACH - 1
    span = seen.shape[0]
    beyond = (span - levels) // 2

    loads = [
        pltpu.make_async_copy(src, dst, in_sem.at[min(i, 2)])
        for i, (src, dst) in enumerate(
            ((outer_hbm, outer), (courant_hbm, courant), (col_hbm, col), (lvl_hbm, lvl), (val_hbm, val))
        )
    ]
    for load in loads:
        load.start()

    me_lat, me_lon, me_lev = (lax.axis_index(a) for a in ("lat", "lon", "lev"))
    links = (
        ("lev", me_lev + 1, me_lev < n_lev - 1),
        ("lev", me_lev - 1, me_lev > 0),
        ("lat", me_lat + 1, me_lat < n_lat - 1),
        ("lat", me_lat - 1, me_lat > 0),
        ("lon", lax.rem(me_lon + 1, n_lon), None),
        ("lon", lax.rem(me_lon + n_lon - 1, n_lon), None),
    )
    turns = (0, 1) if n_lon > 2 else (0,)
    bands = ((rows - TILE, TILE), (0, TILE))

    def both(flags):
        return functools.reduce(jnp.logical_and, flags) if flags else None

    def guarded(exists, action):
        if exists is None:
            action()
        else:
            pl.when(exists)(action)

    def flags_of(which):
        return [links[w][2] for w in which if w < 4]

    def lon_of(which):
        return [w for w in which if w > 3]

    def is_ahead(which):
        return me_lon < links[lon_of(which)[0]][1]

    def is_behind(which):
        return me_lon > links[lon_of(which)[0]][1]

    class Message:
        def __init__(self, which, source, landing, sem, later=0):
            self.which, self.later = which, later
            self.needs = tuple(w for w in which if w < 4)
            self.target = {links[w][0]: links[w][1] for w in which}
            self.arrives = both([links[w ^ 1][2] for w in self.needs])
            self.source, self.landing, self.sem = source, landing, sem

        def start(self, flag=None):
            def begin():
                pltpu.make_async_remote_copy(
                    src_ref=self.source, dst_ref=self.landing, send_sem=send_sem, recv_sem=recv_sem.at[self.sem],
                    device_id=self.target, device_id_type=MESH,
                ).start()

            guarded(both(flags_of(self.which) + ([] if flag is None else [flag])), begin)

        def lines(self):
            total = 1
            for n in self.landing.shape:
                total = total * n
            return total // cols

    partners, first, second, faces = [], [], [], []
    for a in (2, 1, 0):
        for t in (0, 1, None):
            for u in turns + (None,):
                which = [a - 1] if a else []
                which = which + ([2 + t] if t is not None else []) + ([4 + u] if u is not None else [])
                if not which:
                    continue
                partners.append(which)
                b = 0 if u is None else u + 1
                if t is None:
                    first.append(Message(which, strip, strip_full.at[a, b], 0))
                else:
                    first.append(Message(which, strip.at[pl.ds(*bands[t])], strip_half.at[a, t, b], 0))
                if u is None:
                    if a and t is None:
                        faces.append(Message(which, own.at[levels - 1 if a == 1 else 0], face_in.at[a - 1], 1))
                        faces.append(Message(which, deep_out.at[a - 1], deep_in.at[a - 1], 1, 2))
                    elif a:
                        first.append(Message(which, edge_out.at[a - 1, t], edge_in.at[a - 1, t], 0))
                    else:
                        first.append(Message(which, own.at[:, :, pl.ds(*bands[t])], side_in.at[t], 0))
                if not a:
                    if t is None:
                        second.append(Message(which, seen_strip, seen_full.at[u], 1))
                    else:
                        second.append(Message(which, seen_strip.at[:, pl.ds(*bands[t])], seen_half.at[t, b], 1))
                    if u is None:
                        kept = pl.ds(1, span - 2)
                        second.append(Message(which, seen.at[kept, :, pl.ds(*bands[t])], seen_in.at[t], 1))
    first.sort(key=lambda m: m.lines() - 1024 * len(m.target))

    def pick(test, side=None):
        return [(which, None if side is None else side(which)) for which in partners if test(which)]

    def count(chosen):
        total = 0
        for which, flag in chosen:
            exists = both(flags_of(which) + ([] if flag is None else [flag]))
            total = total + (1 if exists is None else exists.astype(jnp.int32))
        return total

    def signal(sem, chosen):
        for which, flag in chosen:
            target = {links[w][0]: links[w][1] for w in which}
            guarded(
                both(flags_of(which) + ([] if flag is None else [flag])),
                lambda target=target: pl.semaphore_signal(sem, inc=1, device_id=target, device_id_type=MESH),
            )

    def level_lon(which):
        return lon_of(which) and not {0, 1} & set(which)

    def corner(which):
        return len(which) == 3

    lower = pick(lambda w: 1 in w and not corner(w))
    upper = pick(lambda w: 0 in w and not corner(w))
    lower_face, upper_face = [[c for c in side if len(c[0]) == 1] for side in (lower, upper)]
    lower_rest, upper_rest = [[c for c in side if len(c[0]) > 1] for side in (lower, upper)]
    lower_south = pick(lambda w: corner(w) and 1 in w and 3 in w)
    upper_north = pick(lambda w: corner(w) and 0 in w and 2 in w)
    lower_north = pick(lambda w: corner(w) and 1 in w and 2 in w, is_behind)
    upper_south = pick(lambda w: corner(w) and 0 in w and 3 in w, is_ahead)
    south, north = pick(lambda w: w == [3]), pick(lambda w: w == [2])
    behind, ahead = pick(level_lon, is_behind), pick(level_lon, is_ahead)

    barrier = pltpu.get_barrier_semaphore()
    signal(barrier, upper_rest[::-1] + upper_north + upper_face + ahead + upper_south + north)

    def settle(messages, flip, sem, known=()):
        if len(known) < 4:
            for has in (True, False):
                flag = links[len(known)][2]
                pl.when(flag if has else jnp.logical_not(flag))(
                    lambda has=has: settle(messages, flip, sem, known + (has,))
                )
            return
        total = sum(m.lines() for m in messages if all(known[w ^ flip] for w in m.needs))
        view = units.at[pl.ds(0, total)]
        pltpu.make_async_copy(view, view, sem).wait()

    def clear(ref):
        ref[...] = jnp.zeros(ref.shape, jnp.float32)

    for m in first + second + faces:
        if m.arrives is not None:
            pl.when(jnp.logical_not(m.arrives))(lambda m=m: clear(m.landing))
    clear(halo)

    lane = lax.broadcasted_iota(jnp.int32, (rows, cols), 1)
    group = lane // GROUP
    pool = (
        lax.broadcasted_iota(jnp.int32, (wide_cols, cols), 0) // fine
        == lax.broadcasted_iota(jnp.int32, (wide_cols, cols), 1)
    ).astype(jnp.float32).astype(jnp.bfloat16)

    loads[1].wait()
    for k in range(3):
        own[:, k + 1] = courant[k].astype(jnp.float32)
    loads[0].wait()
    sums[...] = jnp.dot(outer[...], pool, preferred_element_type=jnp.float32)
    coarse = sums[pl.ds(0, flat_rows, stride=fine), :]
    for k in range(1, fine):
        coarse = coarse + sums[pl.ds(k, flat_rows, stride=fine), :]
    own[:, 0] = (coarse * (1.0 / (fine * fine))).reshape(levels, rows, cols)

    ends_only = jnp.zeros((rows, cols), jnp.float32)
    for f in (1, 2, 3, 0):
        for l in range(levels):
            place = f * levels + l
            ends_only = jnp.where(group == place, pltpu.roll(own[l, f], (REACH + GROUP * place) % cols, axis=1), ends_only)
    strip[...] = ends_only

    entries = [(0, i, j) for i in range(1, REACH) for j in range(1, REACH + 1 - i)]
    entries = entries + [(f, i, j) for f in (1, 2, 3) for i in range(1, near) for j in range(1, near + 1 - i)]
    for s in range(2):
        for t in range(2):
            for n, (f, i, j) in enumerate(entries):
                l = levels - i if s == 0 else i - 1
                r = rows - j if t == 0 else j - 1
                edge_out[s, t, n : n + 1, :] = own[l, f, r : r + 1, :]

    def send(messages, test, side=None, later=0):
        for m in messages:
            if test(m.which) and m.later == later:
                m.start(None if side is None else side(m.which))

    def at_once(w):
        return (1 in w and not (corner(w) and 2 in w)) or w == [3]

    def north_corner(w):
        return corner(w) and 1 in w and 2 in w

    expected = count(lower + lower_south + lower_north + south + behind)
    pl.when(expected > 0)(lambda: pl.semaphore_wait(barrier, expected))
    signal(ready.at[4], [(w, is_behind(w)) for w, _ in lower_south])
    signal(ready.at[3], lower_rest)
    signal(ready.at[0], behind)
    signal(ready.at[2], lower_face)
    signal(ready.at[1], south)
    send(first, north_corner, is_behind)
    send(first, at_once)
    send(first, level_lon, is_behind)
    send(faces, at_once)

    row = lax.broadcasted_iota(jnp.int32, (rows, cols), 0)
    high = rows // TILE
    zero = jnp.zeros((rows, cols), jnp.float32)

    def inner(v, c, before, after):
        above = jnp.where(row == 0, 0.0, pltpu.roll(v, 1, axis=0))
        below = jnp.where(row == rows - 1, 0.0, pltpu.roll(v, rows - 1, axis=0))
        return forward(v, c, [before, above, pltpu.roll(v, 1, axis=1)], [after, below, pltpu.roll(v, cols - 1, axis=1)])

    def rim_rows(second_level, third_level):
        kept = [(second_level, 2, r) for r in (0, 1, rows - 2, rows - 1)]
        return kept + [(second_level, 3, r) for r in (0, rows - 1)] + [(third_level, 2, r) for r in (0, rows - 1)]

    view = units.at[pl.ds(0, 3 * col.shape[0])]
    pltpu.make_async_copy(view, view, in_sem.at[2]).wait()
    where_row = (lvl[...] - me_lev * levels + beyond) * rows + col[...] // cols
    where_col = col[...] % cols
    parts = bf16_parts(val[...], 2)
    pieces, width = col.shape
    row_id = lax.broadcasted_iota(jnp.int32, (span * rows, width), 0)
    col_id = lax.broadcasted_iota(jnp.int32, (cols, width), 0)
    hits = [[] for _ in range(3)]
    tables = []
    for k in range(pieces):
        match = where_row[k : k + 1] == row_id
        hits[0].append(jnp.where(match, 1.0, 0.0).astype(jnp.bfloat16))
        for i, part in enumerate(parts):
            hits[i + 1].append(jnp.where(match, part[k : k + 1], 0.0).astype(jnp.bfloat16))
        tables.append(jnp.where(where_col[k : k + 1] == col_id, 1.0, 0.0).astype(jnp.bfloat16))
    left_side = jnp.concatenate([jnp.concatenate(h, axis=1) for h in hits], axis=0)
    totals = lax.dot_general(
        left_side, jnp.concatenate(tables, axis=1), (((1,), (1,)), ((), ())),
        preferred_element_type=jnp.float32,
    )
    wide_rows = span * rows
    counted = totals[:wide_rows].reshape(span, rows, cols)
    summed = (totals[wide_rows : 2 * wide_rows] + totals[2 * wide_rows :]).reshape(span, rows, cols)
    seen[:, 0] = counted
    seen[:, 1] = summed
    for i, values in enumerate((counted, summed)):
        ends_only = jnp.zeros((rows, cols), jnp.float32)
        for g in range(span):
            place = g + REACH - beyond
            ends_only = jnp.where(group == place, pltpu.roll(values[g], (REACH + GROUP * place) % cols, axis=1), ends_only)
        seen_strip[i] = ends_only
    send(second, at_once)
    send(second, level_lon, is_behind)

    pairs = ((levels - 2, levels - 3), (1, 2))
    once = {
        l: inner(own[l, 0], [own[l, k + 1] for k in range(3)], own[l - 1, 0], own[l + 1, 0])
        for l in sorted(set(pairs[0] + pairs[1]))
    }
    for s, (l, far) in enumerate(pairs):
        c = [own[l, k + 1] for k in range(3)]
        twice = inner(once[l], c, zero if s else once[far], once[far] if s else zero)
        for n, plane in enumerate((own[l, 0], once[l], twice, c[0])):
            deep_out[s, n * high : (n + 1) * high] = plane.reshape(high, TILE, cols)
        for n, (at, f, r) in enumerate(rim_rows(l, far)):
            deep_out[s, 4 * high, n : n + 1, :] = own[at, f, r : r + 1, :]

    send(faces, at_once, later=2)

    @pl.when(links[2][2])
    def _():
        pl.semaphore_wait(ready.at[1], 1)
        send(first, north_corner, is_ahead)
        send(first + second, lambda w: w == [2])

    @pl.when(me_lon < n_lon - 1)
    def _():
        pl.semaphore_wait(ready.at[0], count(ahead))
        send(first + second, level_lon, is_ahead)

    @pl.when(links[0][2])
    def _():
        pl.semaphore_wait(ready.at[2], 1)
        send(faces, lambda w: 0 in w)
        pl.semaphore_wait(ready.at[3], count(upper_rest))
        send(first, lambda w: 0 in w and not (corner(w) and 2 in w))
        send(first, lambda w: corner(w) and 0 in w and 2 in w, is_behind)

    @pl.when(links[0][2] & links[2][2] & (me_lon < n_lon - 1))
    def _():
        pl.semaphore_wait(ready.at[4], count([(w, is_ahead(w)) for w, _ in upper_north]))
        send(first, lambda w: corner(w) and 0 in w and 2 in w, is_ahead)

    pl.when(links[0][2])(lambda: send(faces, lambda w: 0 in w, later=2))

    settle(first, 1, recv_sem.at[0])

    tall = rows + TILE
    half = lax.broadcasted_iota(jnp.int32, (TILE, cols), 0) < TILE // 2
    lanes = lax.broadcasted_iota(jnp.int32, (tall, cols), 1)
    slot = lanes % GROUP
    left_half = slot < REACH
    blank = jnp.zeros((TILE, cols), jnp.float32)

    def joined(full, before, after):
        return jnp.concatenate([full, jnp.where(half, after, before)], axis=0)

    for s in range(2):
        for t in range(2):
            for n, (f, i, j) in enumerate(entries):
                r = TILE - j if t == 0 else j - 1
                halo[s, i - 1, f, r : r + 1, :] = edge_in[s, t, n : n + 1, :]

    def cell(l, f):
        if 0 <= l < levels:
            return joined(own[l, f], side_in[0, l, f], side_in[1, l, f])
        s, i = (0, -l) if l < 0 else (1, l - levels + 1)
        return jnp.concatenate([face_in[s, f], halo[s, i - 1, f]], axis=0)

    def down(x):
        return pltpu.roll(x, 1, axis=0)

    def up_row(x):
        return pltpu.roll(x, tall - 1, axis=0)

    def right(x, by=1):
        return pltpu.roll(x, by, axis=1)

    def left(x, by=1):
        return pltpu.roll(x, cols - by, axis=1)

    before_b, after_b = 1, (2 if n_lon > 2 else 1)

    def strip_block(a, b):
        full = strip[...] if a == 0 and b == 0 else strip_full[a, b]
        return joined(full, strip_half[a, 0, b], strip_half[a, 1, b])

    def placed(blocks, f):
        turned = [right(blocks[a], (GROUP * levels * (n - f)) % cols) if n != f else blocks[a] for n, a in enumerate((1, 0, 2))]
        width = GROUP * levels
        return jnp.where(lanes < width, turned[0], jnp.where(lanes < 2 * width, turned[1], turned[2]))

    mine = [strip_block(a, 0) for a in range(3)]
    sides = []
    sides.append([jnp.where(left_half, strip_block(a, before_b), mine[a]) for a in range(3)])
    sides.append([jnp.where(left_half, mine[a], strip_block(a, after_b)) for a in range(3)])
    side_c, side_v = [], []
    for blocks in sides:
        c = [placed(blocks, k + 1) for k in range(3)]
        v = placed(blocks, 0)
        for _ in range(2):
            v = forward(v, c, [right(v, GROUP), down(v), right(v)], [left(v, GROUP), up_row(v), left(v)])
        side_c.append(c)
        side_v.append(v)

    def inserted(z, l):
        return right(z, (cols - REACH - GROUP * (l + REACH)) % cols)

    def seen_block(b, i):
        full = seen_strip[i] if b == 0 else seen_full[b - 1, i]
        return joined(full, seen_half[0, b, i], seen_half[1, b, i])

    speeds = {l: [cell(l, k + 1) for k in range(3)] for l in range(levels)}
    start = {l: cell(l, 0) for l in range(levels)}

    def lev_term(v, l):
        n = speeds[l][0]
        return jnp.abs(n) * jnp.where(n > 0.0, v[l - 1], v[l + 1])

    def within(v, l):
        result = centre_of(speeds[l]) * v[l]
        for n, minus, plus in zip(speeds[l][1:], (down(v[l]), right(v[l])), (up_row(v[l]), left(v[l]))):
            result = result + jnp.abs(n) * jnp.where(n > 0.0, minus, plus)
        return result

    begun = {l: within(start, l) for l in range(levels)}
    begun = {l: begun[l] + lev_term(start, l) if 0 < l < levels - 1 else begun[l] for l in begun}

    settle(first + second + faces, 0, send_sem)
    settle(second + faces, 1, recv_sem.at[1])
    side_q = []
    for side in range(2):
        known = []
        for i in range(2):
            if side == 0:
                known.append(jnp.where(left_half, seen_block(before_b, i), seen_block(0, i)))
            else:
                known.append(jnp.where(left_half, seen_block(0, i), seen_block(after_b, i)))
        p = known[0] * side_v[side] - known[1]
        c = side_c[side]
        low, up = shares(p, c)
        q = centre_of(c) * p + left(low[0], GROUP) + right(up[0], GROUP)
        q = q + up_row(low[1]) + down(up[1]) + left(low[2]) + right(up[2])
        low, up = shares(q, c)
        side_q.append((q, right(up[2]) if side == 0 else left(low[2])))
    fix = jnp.where(left_half, side_q[1][0], side_q[0][0])
    crossing = jnp.where(left_half, side_q[1][1], side_q[0][1])

    fix_v = jnp.where(left_half, side_v[1], side_v[0])
    fix_v = {l: inserted(fix_v, l) for l in range(2 - near - 1, levels + near - 1)}
    fix_q = {l: inserted(fix, l) for l in range(-1, levels + 1)}
    crossing = {l: inserted(crossing, l) for l in range(levels)}

    for l in (-1, levels):
        speeds[l] = [cell(l, k + 1) for k in range(3)]
        start[l] = cell(l, 0)
    beside = ((-2, -1, -3), (levels + 1, levels, levels + 2))

    def deep(s, n):
        return deep_in[s, n * high : (n + 1) * high].reshape(rows, cols)

    def kept_rows(s, places):
        plane = zero
        for n, r in places:
            plane = jnp.where(row == r, deep_in[s, 4 * high, n : n + 1, :], plane)
        return plane

    def across(c, x):
        above = jnp.where((row == 0) & (c > 0.0), down(x)[:rows], 0.0)
        below = jnp.where((row == rows - 1) & (c <= 0.0), up_row(x)[:rows], 0.0)
        return jnp.abs(c) * (above + below)

    def step(v, l, rule=forward):
        return rule(v[l], speeds[l], [v[l - 1], down(v[l]), right(v[l])], [v[l + 1], up_row(v[l]), left(v[l])])

    outside = []
    for s, (l, _, far) in enumerate(beside):
        c = [
            deep(s, 3),
            kept_rows(s, ((0, 0), (1, 1), (2, rows - 2), (3, rows - 1))),
            kept_rows(s, ((4, 0), (5, rows - 1))),
        ]
        start[l] = jnp.concatenate([deep(s, 0), halo[s, 1, 0]], axis=0)
        start[far] = jnp.concatenate([zero, halo[s, 2, 0]], axis=0)
        speeds[l] = [jnp.concatenate([c[k], halo[s, 1, k + 1]], axis=0) for k in range(3)]
        gained = across(c[1], start[l])
        further = across(kept_rows(s, ((6, 0), (7, rows - 1))), start[far])
        outside.append((c, gained, further))
    v = {l: step(start, l) for l in (-1, levels)}
    for l in range(levels):
        v[l] = begun[l] if 0 < l < levels - 1 else begun[l] + lev_term(start, l)
    for s, (l, _, _) in enumerate(beside):
        v[l] = jnp.concatenate([deep(s, 1) + outside[s][1], step(start, l)[rows:]], axis=0)
    second_v = {l: step(v, l, again) for l in range(-1, levels + 1)}
    for s, (l, by, _) in enumerate(beside):
        c, gained, further = outside[s]
        sizes = [jnp.abs(n) for n in c]
        inward, outward = v[by][:rows], further
        crossed = jnp.concatenate([gained, v[l][rows:]], axis=0)
        total = deep(s, 2) + (1.0 - sizes[0] - sizes[1] - sizes[2]) * gained
        total = total + sizes[0] * jnp.where(c[0] > 0.0, inward if s else outward, outward if s else inward)
        total = total + sizes[1] * jnp.where(c[1] > 0.0, down(crossed)[:rows], up_row(crossed)[:rows])
        total = total + sizes[2] * jnp.where(
            c[2] > 0.0, pltpu.roll(gained, 1, axis=1), pltpu.roll(gained, cols - 1, axis=1)
        )
        second_v[l] = jnp.concatenate([total, blank], axis=0)
        speeds[l] = [jnp.concatenate([c[0], blank], axis=0)]
    v = second_v
    rim = (lanes < 2) | (lanes >= cols - 2)
    v = {l: jnp.where(rim, fix_v[l], v[l]) for l in v}
    for l in range(levels):
        state_v[l] = v[l][:rows]

    def seen_cell(l, i):
        g = l + beyond
        if 0 < g < span - 1:
            return joined(seen[g, i], seen_in[0, g - 1, i], seen_in[1, g - 1, i])
        return jnp.concatenate([seen[g, i], blank], axis=0)

    p = {l: seen_cell(l, 0) * v[l] - seen_cell(l, 1) for l in v}
    low, up = {}, {}
    for l in p:
        low[l], up[l] = shares(p[l], speeds[l])
    rim = (lanes < 1) | (lanes >= cols - 1)
    q = {}
    for l in range(-1, levels + 1):
        total = centre_of(speeds[l]) * p[l] + low[l + 1][0] + up[l - 1][0]
        total = total + up_row(low[l][1]) + down(up[l][1]) + left(low[l][2]) + right(up[l][2])
        q[l] = jnp.where(rim, fix_q[l], total)
    for l in q:
        low[l], up[l] = shares(q[l], speeds[l])
    for l in range(levels):
        total = centre_of(speeds[l]) * q[l] + low[l + 1][0] + up[l - 1][0]
        total = total + up_row(low[l][1]) + down(up[l][1])
        total = total + jnp.where(rim, crossing[l], 0.0)
        total = total + jnp.where(lanes >= cols - 1, 0.0, left(low[l][2])) + jnp.where(lanes < 1, 0.0, right(up[l][2]))
        adj_v[l] = total[:rows]


def finish(state_v, adj_v, outer, state_hbm, adj_hbm, next_hbm, wide, nxt, out_sem):
    levels, rows, cols = state_v.shape
    flat_rows = levels * rows
    wide_cols = outer.shape[1]
    fine = wide_cols // cols
    outer_rows = outer.shape[0] // levels
    stores = [
        pltpu.make_async_copy(state_v, state_hbm, out_sem.at[0]),
        pltpu.make_async_copy(adj_v, adj_hbm, out_sem.at[1]),
    ]
    for store in stores:
        store.start()
    field = adj_v[...]

    table = (
        lax.broadcasted_iota(jnp.int32, (cols, wide_cols), 0)
        == lax.broadcasted_iota(jnp.int32, (cols, wide_cols), 1) // fine
    ).astype(jnp.float32).astype(jnp.bfloat16)
    halves = bf16_parts(field.reshape(flat_rows, cols), 2)
    spread = jnp.dot(
        jnp.concatenate([h.astype(jnp.bfloat16) for h in halves], axis=1),
        jnp.concatenate([table, table], axis=0),
        preferred_element_type=jnp.float32,
    )
    for k in range(fine):
        for c in range(fine):
            wide[c, pl.ds(k, flat_rows, stride=fine), :] = spread[:, c * cols : (c + 1) * cols]
    for level in range(levels):
        span = pl.ds(level * outer_rows, outer_rows)
        for c in range(fine):
            lanes = pl.ds(c * cols, cols)
            nxt[span, lanes] = (outer[span, lanes].astype(jnp.float32) - wide[c, span, :]).astype(jnp.bfloat16)
        store = pltpu.make_async_copy(nxt.at[span], next_hbm.at[span], out_sem.at[2 + level])
        store.start()
        stores.append(store)
    for store in stores:
        store.wait()


def shards(ends, outer_increment, courant, obs_column, obs_level, obs_value):
    levels, outer_rows, wide_cols = outer_increment.shape
    _, _, rows, cols = courant.shape
    flat_rows = levels * rows
    fine = wide_cols // cols
    lanes = 128
    observed = (obs_column.shape[0] // lanes, lanes)
    span = levels + 4
    assert 4 * levels * GROUP == cols and levels >= REACH and rows % TILE == 0 and ends[1] > 1
    f32, bf16 = jnp.float32, jnp.bfloat16
    outer_shape = (levels * outer_rows, wide_cols)
    vmem = pl.BlockSpec(memory_space=pltpu.VMEM)
    hbm = pl.BlockSpec(memory_space=pl.ANY)
    held = pl.pallas_call(
        functools.partial(kernel, ends),
        out_shape=(
            pltpu.VMEM((levels, rows, cols), f32),
            pltpu.VMEM((levels, rows, cols), f32),
            pltpu.VMEM(outer_shape, bf16),
        ),
        in_specs=[hbm] * 5,
        out_specs=(vmem,) * 3,
        scratch_shapes=[
            pltpu.VMEM(courant.shape, bf16),
            pltpu.VMEM(observed, jnp.int32),
            pltpu.VMEM(observed, jnp.int32),
            pltpu.VMEM(observed, f32),
            pltpu.VMEM((levels * outer_rows, cols), f32),
            pltpu.VMEM((levels, 4, rows, cols), f32),
            pltpu.VMEM((2, 4, rows, cols), f32),
            pltpu.VMEM((2, 4 * rows // TILE + 1, TILE, cols), f32),
            pltpu.VMEM((2, 4 * rows // TILE + 1, TILE, cols), f32),
            pltpu.VMEM((2, levels, 4, TILE, cols), f32),
            pltpu.VMEM((2, 2, 2 * TILE, cols), f32),
            pltpu.VMEM((2, 2, 2 * TILE, cols), f32),
            pltpu.VMEM((2, REACH - 1, 4, TILE, cols), f32),
            pltpu.VMEM((rows, cols), f32),
            pltpu.VMEM((3, 3, rows, cols), f32),
            pltpu.VMEM((3, 2, 3, TILE, cols), f32),
            pltpu.VMEM((span, 2, rows, cols), f32),
            pltpu.VMEM((2, span - 2, 2, TILE, cols), f32),
            pltpu.VMEM((2, rows, cols), f32),
            pltpu.VMEM((2, 2, rows, cols), f32),
            pltpu.VMEM((2, 3, 2, TILE, cols), f32),
            pltpu.VMEM((2048, 1, cols), f32),
            pltpu.SemaphoreType.DMA((3,)),
            pltpu.SemaphoreType.DMA,
            pltpu.SemaphoreType.DMA((2,)),
            pltpu.SemaphoreType.REGULAR((5,)),
        ],
        compiler_params=pltpu.CompilerParams(collective_id=0, has_side_effects=True),
    )(
        outer_increment.reshape(outer_shape),
        courant,
        obs_column.reshape(observed),
        obs_level.reshape(observed),
        obs_value.reshape(observed),
    )
    state, adjoint, following = pl.pallas_call(
        finish,
        out_shape=(
            jax.ShapeDtypeStruct((levels, rows, cols), f32),
            jax.ShapeDtypeStruct((levels, rows, cols), f32),
            jax.ShapeDtypeStruct(outer_shape, bf16),
        ),
        in_specs=[vmem] * 3,
        out_specs=(hbm,) * 3,
        scratch_shapes=[
            pltpu.VMEM((fine, levels * outer_rows, cols), f32),
            pltpu.VMEM(outer_shape, bf16),
            pltpu.SemaphoreType.DMA((2 + levels,)),
        ],
    )(*[pltpu.with_memory_space_constraint(x, pltpu.VMEM) for x in held])
    return state, adjoint, following.reshape(outer_increment.shape)


def solution(mesh):
    ends = tuple(mesh.shape[a] for a in ("lat", "lon", "lev"))
    block = P("lev", "lat", "lon")
    observed = P(("lat", "lon"))
    return jax.shard_map(
        functools.partial(shards, ends),
        mesh=mesh,
        in_specs=(block, P(None, "lev", "lat", "lon"), observed, observed, observed),
        out_specs=(block, block, block),
        check_vma=False,
    )
```

```python
import functools

import jax
import jax.numpy as jnp
from jax import lax
from jax.experimental import pallas as pl
from jax.experimental.pallas import tpu as pltpu
from jax.sharding import PartitionSpec as P

MESH = pl.DeviceIdType.MESH
REACH = 4
GROUP = 2 * REACH
TILE = 8


def bf16_parts(x, count):
    parts = []
    for _ in range(count):
        part = x.astype(jnp.bfloat16).astype(jnp.float32)
        parts.append(part)
        x = x - part
    return parts


def forward(v, c, minus, plus):
    sizes = [jnp.abs(n) for n in c]
    result = (1.0 - sizes[0] - sizes[1] - sizes[2]) * v
    for k in range(3):
        result = result + sizes[k] * jnp.where(c[k] > 0.0, minus[k], plus[k])
    return result


def again(v, c, minus, plus):
    result = centre_of(c) * v
    for k in range(3):
        low = jnp.maximum(c[k], 0.0)
        result = result + low * minus[k] + (low - c[k]) * plus[k]
    return result


def shares(p, c):
    low, up = [], []
    for n in c:
        low.append(jnp.maximum(n, 0.0) * p)
        up.append(low[-1] - n * p)
    return low, up


def centre_of(c):
    return 1.0 - jnp.abs(c[0]) - jnp.abs(c[1]) - jnp.abs(c[2])


def kernel(
    ends, outer_hbm, courant_hbm, col_hbm, lvl_hbm, val_hbm,
    state_v, adj_v, outer,
    courant, col, lvl, val, sums,
    own, face_in, deep_out, deep_in, side_in, edge_out, edge_in, halo,
    strip, strip_full, strip_half,
    seen, seen_in, seen_strip, seen_full, seen_half, units,
    in_sem, send_sem, recv_sem, ready,
):
    n_lat, n_lon, n_lev = ends
    levels, rows, cols = state_v.shape
    flat_rows = levels * rows
    wide_cols = outer.shape[1]
    fine = wide_cols // cols
    near = REACH - 1
    span = seen.shape[0]
    beyond = (span - levels) // 2

    loads = [
        pltpu.make_async_copy(src, dst, in_sem.at[min(i, 2)])
        for i, (src, dst) in enumerate(
            ((outer_hbm, outer), (courant_hbm, courant), (col_hbm, col), (lvl_hbm, lvl), (val_hbm, val))
        )
    ]
    for load in loads:
        load.start()

    me_lat, me_lon, me_lev = (lax.axis_index(a) for a in ("lat", "lon", "lev"))
    links = (
        ("lev", me_lev + 1, me_lev < n_lev - 1),
        ("lev", me_lev - 1, me_lev > 0),
        ("lat", me_lat + 1, me_lat < n_lat - 1),
        ("lat", me_lat - 1, me_lat > 0),
        ("lon", lax.rem(me_lon + 1, n_lon), None),
        ("lon", lax.rem(me_lon + n_lon - 1, n_lon), None),
    )
    turns = (0, 1) if n_lon > 2 else (0,)
    bands = ((rows - TILE, TILE), (0, TILE))

    def both(flags):
        return functools.reduce(jnp.logical_and, flags) if flags else None

    def guarded(exists, action):
        if exists is None:
            action()
        else:
            pl.when(exists)(action)

    def flags_of(which):
        return [links[w][2] for w in which if w < 4]

    def lon_of(which):
        return [w for w in which if w > 3]

    def is_ahead(which):
        return me_lon < links[lon_of(which)[0]][1]

    def is_behind(which):
        return me_lon > links[lon_of(which)[0]][1]

    class Message:
        def __init__(self, which, source, landing, sem, later=0):
            self.which, self.later = which, later
            self.needs = tuple(w for w in which if w < 4)
            self.target = {links[w][0]: links[w][1] for w in which}
            self.arrives = both([links[w ^ 1][2] for w in self.needs])
            self.source, self.landing, self.sem = source, landing, sem

        def start(self, flag=None):
            def begin():
                pltpu.make_async_remote_copy(
                    src_ref=self.source, dst_ref=self.landing, send_sem=send_sem, recv_sem=recv_sem.at[self.sem],
                    device_id=self.target, device_id_type=MESH,
                ).start()

            guarded(both(flags_of(self.which) + ([] if flag is None else [flag])), begin)

        def lines(self):
            total = 1
            for n in self.landing.shape:
                total = total * n
            return total // cols

    partners, first, second, faces = [], [], [], []
    for a in (2, 1, 0):
        for t in (0, 1, None):
            for u in turns + (None,):
                which = [a - 1] if a else []
                which = which + ([2 + t] if t is not None else []) + ([4 + u] if u is not None else [])
                if not which:
                    continue
                partners.append(which)
                b = 0 if u is None else u + 1
                if t is None:
                    first.append(Message(which, strip, strip_full.at[a, b], 0))
                else:
                    first.append(Message(which, strip.at[pl.ds(*bands[t])], strip_half.at[a, t, b], 0))
                if u is None:
                    if a and t is None:
                        faces.append(Message(which, own.at[levels - 1 if a == 1 else 0], face_in.at[a - 1], 1))
                        faces.append(Message(which, deep_out.at[a - 1], deep_in.at[a - 1], 1, 2))
                    elif a:
                        first.append(Message(which, edge_out.at[a - 1, t], edge_in.at[a - 1, t], 0))
                    else:
                        first.append(Message(which, own.at[:, :, pl.ds(*bands[t])], side_in.at[t], 0))
                if not a:
                    if t is None:
                        second.append(Message(which, seen_strip, seen_full.at[u], 1))
                    else:
                        second.append(Message(which, seen_strip.at[:, pl.ds(*bands[t])], seen_half.at[t, b], 1))
                    if u is None:
                        kept = pl.ds(1, span - 2)
                        second.append(Message(which, seen.at[kept, :, pl.ds(*bands[t])], seen_in.at[t], 1))
    first.sort(key=lambda m: m.lines() - 1024 * len(m.target))

    def pick(test, side=None):
        return [(which, None if side is None else side(which)) for which in partners if test(which)]

    def count(chosen):
        total = 0
        for which, flag in chosen:
            exists = both(flags_of(which) + ([] if flag is None else [flag]))
            total = total + (1 if exists is None else exists.astype(jnp.int32))
        return total

    def signal(sem, chosen):
        for which, flag in chosen:
            target = {links[w][0]: links[w][1] for w in which}
            guarded(
                both(flags_of(which) + ([] if flag is None else [flag])),
                lambda target=target: pl.semaphore_signal(sem, inc=1, device_id=target, device_id_type=MESH),
            )

    def level_lon(which):
        return lon_of(which) and not {0, 1} & set(which)

    def corner(which):
        return len(which) == 3

    lower = pick(lambda w: 1 in w and not corner(w))
    upper = pick(lambda w: 0 in w and not corner(w))
    lower_face, upper_face = [[c for c in side if len(c[0]) == 1] for side in (lower, upper)]
    lower_rest, upper_rest = [[c for c in side if len(c[0]) > 1] for side in (lower, upper)]
    lower_south = pick(lambda w: corner(w) and 1 in w and 3 in w)
    upper_north = pick(lambda w: corner(w) and 0 in w and 2 in w)
    lower_north = pick(lambda w: corner(w) and 1 in w and 2 in w, is_behind)
    upper_south = pick(lambda w: corner(w) and 0 in w and 3 in w, is_ahead)
    south, north = pick(lambda w: w == [3]), pick(lambda w: w == [2])
    behind, ahead = pick(level_lon, is_behind), pick(level_lon, is_ahead)

    barrier = pltpu.get_barrier_semaphore()
    signal(barrier, upper_rest[::-1] + upper_north + upper_face + ahead + upper_south + north)

    def settle(messages, flip, sem, known=()):
        if len(known) < 4:
            for has in (True, False):
                flag = links[len(known)][2]
                pl.when(flag if has else jnp.logical_not(flag))(
                    lambda has=has: settle(messages, flip, sem, known + (has,))
                )
            return
        total = sum(m.lines() for m in messages if all(known[w ^ flip] for w in m.needs))
        view = units.at[pl.ds(0, total)]
        pltpu.make_async_copy(view, view, sem).wait()

    def clear(ref):
        ref[...] = jnp.zeros(ref.shape, jnp.float32)

    for m in first + second + faces:
        if m.arrives is not None:
            pl.when(jnp.logical_not(m.arrives))(lambda m=m: clear(m.landing))
    clear(halo)

    lane = lax.broadcasted_iota(jnp.int32, (rows, cols), 1)
    group = lane // GROUP
    pool = (
        lax.broadcasted_iota(jnp.int32, (wide_cols, cols), 0) // fine
        == lax.broadcasted_iota(jnp.int32, (wide_cols, cols), 1)
    ).astype(jnp.float32).astype(jnp.bfloat16)

    loads[1].wait()
    for k in range(3):
        own[:, k + 1] = courant[k].astype(jnp.float32)
    loads[0].wait()
    sums[...] = jnp.dot(outer[...], pool, preferred_element_type=jnp.float32)
    coarse = sums[pl.ds(0, flat_rows, stride=fine), :]
    for k in range(1, fine):
        coarse = coarse + sums[pl.ds(k, flat_rows, stride=fine), :]
    own[:, 0] = (coarse * (1.0 / (fine * fine))).reshape(levels, rows, cols)

    ends_only = jnp.zeros((rows, cols), jnp.float32)
    for f in (1, 2, 3, 0):
        for l in range(levels):
            place = f * levels + l
            ends_only = jnp.where(group == place, pltpu.roll(own[l, f], (REACH + GROUP * place) % cols, axis=1), ends_only)
    strip[...] = ends_only

    entries = [(0, i, j) for i in range(1, REACH) for j in range(1, REACH + 1 - i)]
    entries = entries + [(f, i, j) for f in (1, 2, 3) for i in range(1, near) for j in range(1, near + 1 - i)]
    for s in range(2):
        for t in range(2):
            for n, (f, i, j) in enumerate(entries):
                l = levels - i if s == 0 else i - 1
                r = rows - j if t == 0 else j - 1
                edge_out[s, t, n : n + 1, :] = own[l, f, r : r + 1, :]

    def send(messages, test, side=None, later=0):
        for m in messages:
            if test(m.which) and m.later == later:
                m.start(None if side is None else side(m.which))

    def at_once(w):
        return (1 in w and not (corner(w) and 2 in w)) or w == [3]

    def north_corner(w):
        return corner(w) and 1 in w and 2 in w

    expected = count(lower + lower_south + lower_north + south + behind)
    pl.when(expected > 0)(lambda: pl.semaphore_wait(barrier, expected))
    signal(ready.at[4], [(w, is_behind(w)) for w, _ in lower_south])
    signal(ready.at[3], lower_rest)
    signal(ready.at[0], behind)
    signal(ready.at[2], lower_face)
    signal(ready.at[1], south)
    send(first, north_corner, is_behind)
    send(first, at_once)
    send(first, level_lon, is_behind)
    send(faces, at_once)

    row = lax.broadcasted_iota(jnp.int32, (rows, cols), 0)
    high = rows // TILE
    zero = jnp.zeros((rows, cols), jnp.float32)

    def inner(v, c, before, after):
        above = jnp.where(row == 0, 0.0, pltpu.roll(v, 1, axis=0))
        below = jnp.where(row == rows - 1, 0.0, pltpu.roll(v, rows - 1, axis=0))
        return forward(v, c, [before, above, pltpu.roll(v, 1, axis=1)], [after, below, pltpu.roll(v, cols - 1, axis=1)])

    def rim_rows(second_level, third_level):
        kept = [(second_level, 2, r) for r in (0, 1, rows - 2, rows - 1)]
        return kept + [(second_level, 3, r) for r in (0, rows - 1)] + [(third_level, 2, r) for r in (0, rows - 1)]

    view = units.at[pl.ds(0, 3 * col.shape[0])]
    pltpu.make_async_copy(view, view, in_sem.at[2]).wait()
    where_row = (lvl[...] - me_lev * levels + beyond) * rows + col[...] // cols
    where_col = col[...] % cols
    parts = bf16_parts(val[...], 2)
    pieces, width = col.shape
    row_id = lax.broadcasted_iota(jnp.int32, (span * rows, width), 0)
    col_id = lax.broadcasted_iota(jnp.int32, (cols, width), 0)
    hits = [[] for _ in range(3)]
    tables = []
    for k in range(pieces):
        match = where_row[k : k + 1] == row_id
        hits[0].append(jnp.where(match, 1.0, 0.0).astype(jnp.bfloat16))
        for i, part in enumerate(parts):
            hits[i + 1].append(jnp.where(match, part[k : k + 1], 0.0).astype(jnp.bfloat16))
        tables.append(jnp.where(where_col[k : k + 1] == col_id, 1.0, 0.0).astype(jnp.bfloat16))
    left_side = jnp.concatenate([jnp.concatenate(h, axis=1) for h in hits], axis=0)
    totals = lax.dot_general(
        left_side, jnp.concatenate(tables, axis=1), (((1,), (1,)), ((), ())),
        preferred_element_type=jnp.float32,
    )
    wide_rows = span * rows
    counted = totals[:wide_rows].reshape(span, rows, cols)
    summed = (totals[wide_rows : 2 * wide_rows] + totals[2 * wide_rows :]).reshape(span, rows, cols)
    seen[:, 0] = counted
    seen[:, 1] = summed
    for i, values in enumerate((counted, summed)):
        ends_only = jnp.zeros((rows, cols), jnp.float32)
        for g in range(span):
            place = g + REACH - beyond
            ends_only = jnp.where(group == place, pltpu.roll(values[g], (REACH + GROUP * place) % cols, axis=1), ends_only)
        seen_strip[i] = ends_only
    send(second, level_lon, is_behind)
    send(second, at_once)

    pairs = ((levels - 2, levels - 3), (1, 2))
    once = {
        l: inner(own[l, 0], [own[l, k + 1] for k in range(3)], own[l - 1, 0], own[l + 1, 0])
        for l in sorted(set(pairs[0] + pairs[1]))
    }
    for s, (l, far) in enumerate(pairs):
        c = [own[l, k + 1] for k in range(3)]
        twice = inner(once[l], c, zero if s else once[far], once[far] if s else zero)
        for n, plane in enumerate((own[l, 0], once[l], twice, c[0])):
            deep_out[s, n * high : (n + 1) * high] = plane.reshape(high, TILE, cols)
        for n, (at, f, r) in enumerate(rim_rows(l, far)):
            deep_out[s, 4 * high, n : n + 1, :] = own[at, f, r : r + 1, :]

    send(faces, at_once, later=2)

    @pl.when(links[2][2])
    def _():
        pl.semaphore_wait(ready.at[1], 1)
        send(first, north_corner, is_ahead)
        send(first + second, lambda w: w == [2])

    @pl.when(me_lon < n_lon - 1)
    def _():
        pl.semaphore_wait(ready.at[0], count(ahead))
        send(first + second, level_lon, is_ahead)

    @pl.when(links[0][2])
    def _():
        pl.semaphore_wait(ready.at[2], 1)
        send(faces, lambda w: 0 in w)
        pl.semaphore_wait(ready.at[3], count(upper_rest))
        send(first, lambda w: 0 in w and not (corner(w) and 2 in w))
        send(first, lambda w: corner(w) and 0 in w and 2 in w, is_behind)

    @pl.when(links[0][2] & links[2][2] & (me_lon < n_lon - 1))
    def _():
        pl.semaphore_wait(ready.at[4], count([(w, is_ahead(w)) for w, _ in upper_north]))
        send(first, lambda w: corner(w) and 0 in w and 2 in w, is_ahead)

    pl.when(links[0][2])(lambda: send(faces, lambda w: 0 in w, later=2))

    settle(first, 1, recv_sem.at[0])

    tall = rows + TILE
    half = lax.broadcasted_iota(jnp.int32, (TILE, cols), 0) < TILE // 2
    lanes = lax.broadcasted_iota(jnp.int32, (tall, cols), 1)
    slot = lanes % GROUP
    left_half = slot < REACH
    blank = jnp.zeros((TILE, cols), jnp.float32)

    def joined(full, before, after):
        return jnp.concatenate([full, jnp.where(half, after, before)], axis=0)

    for s in range(2):
        for t in range(2):
            for n, (f, i, j) in enumerate(entries):
                r = TILE - j if t == 0 else j - 1
                halo[s, i - 1, f, r : r + 1, :] = edge_in[s, t, n : n + 1, :]

    def cell(l, f):
        if 0 <= l < levels:
            return joined(own[l, f], side_in[0, l, f], side_in[1, l, f])
        s, i = (0, -l) if l < 0 else (1, l - levels + 1)
        return jnp.concatenate([face_in[s, f], halo[s, i - 1, f]], axis=0)

    def down(x):
        return pltpu.roll(x, 1, axis=0)

    def up_row(x):
        return pltpu.roll(x, tall - 1, axis=0)

    def right(x, by=1):
        return pltpu.roll(x, by, axis=1)

    def left(x, by=1):
        return pltpu.roll(x, cols - by, axis=1)

    before_b, after_b = 1, (2 if n_lon > 2 else 1)

    def strip_block(a, b):
        full = strip[...] if a == 0 and b == 0 else strip_full[a, b]
        return joined(full, strip_half[a, 0, b], strip_half[a, 1, b])

    def placed(blocks, f):
        turned = [right(blocks[a], (GROUP * levels * (n - f)) % cols) if n != f else blocks[a] for n, a in enumerate((1, 0, 2))]
        width = GROUP * levels
        return jnp.where(lanes < width, turned[0], jnp.where(lanes < 2 * width, turned[1], turned[2]))

    mine = [strip_block(a, 0) for a in range(3)]
    sides = []
    sides.append([jnp.where(left_half, strip_block(a, before_b), mine[a]) for a in range(3)])
    sides.append([jnp.where(left_half, mine[a], strip_block(a, after_b)) for a in range(3)])
    side_c, side_v = [], []
    for blocks in sides:
        c = [placed(blocks, k + 1) for k in range(3)]
        v = placed(blocks, 0)
        for _ in range(2):
            v = forward(v, c, [right(v, GROUP), down(v), right(v)], [left(v, GROUP), up_row(v), left(v)])
        side_c.append(c)
        side_v.append(v)

    def inserted(z, l):
        return right(z, (cols - REACH - GROUP * (l + REACH)) % cols)

    def seen_block(b, i):
        full = seen_strip[i] if b == 0 else seen_full[b - 1, i]
        return joined(full, seen_half[0, b, i], seen_half[1, b, i])

    speeds = {l: [cell(l, k + 1) for k in range(3)] for l in range(levels)}
    start = {l: cell(l, 0) for l in range(levels)}

    def lev_term(v, l):
        n = speeds[l][0]
        return jnp.abs(n) * jnp.where(n > 0.0, v[l - 1], v[l + 1])

    def within(v, l):
        result = centre_of(speeds[l]) * v[l]
        for n, minus, plus in zip(speeds[l][1:], (down(v[l]), right(v[l])), (up_row(v[l]), left(v[l]))):
            result = result + jnp.abs(n) * jnp.where(n > 0.0, minus, plus)
        return result

    begun = {l: within(start, l) for l in range(levels)}
    begun = {l: begun[l] + lev_term(start, l) if 0 < l < levels - 1 else begun[l] for l in begun}

    settle(first + second + faces, 0, send_sem)
    settle(second + faces, 1, recv_sem.at[1])
    side_q = []
    for side in range(2):
        known = []
        for i in range(2):
            if side == 0:
                known.append(jnp.where(left_half, seen_block(before_b, i), seen_block(0, i)))
            else:
                known.append(jnp.where(left_half, seen_block(0, i), seen_block(after_b, i)))
        p = known[0] * side_v[side] - known[1]
        c = side_c[side]
        low, up = shares(p, c)
        q = centre_of(c) * p + left(low[0], GROUP) + right(up[0], GROUP)
        q = q + up_row(low[1]) + down(up[1]) + left(low[2]) + right(up[2])
        low, up = shares(q, c)
        side_q.append((q, right(up[2]) if side == 0 else left(low[2])))
    fix = jnp.where(left_half, side_q[1][0], side_q[0][0])
    crossing = jnp.where(left_half, side_q[1][1], side_q[0][1])

    fix_v = jnp.where(left_half, side_v[1], side_v[0])
    fix_v = {l: inserted(fix_v, l) for l in range(2 - near - 1, levels + near - 1)}
    fix_q = {l: inserted(fix, l) for l in range(-1, levels + 1)}
    crossing = {l: inserted(crossing, l) for l in range(levels)}

    for l in (-1, levels):
        speeds[l] = [cell(l, k + 1) for k in range(3)]
        start[l] = cell(l, 0)
    beside = ((-2, -1, -3), (levels + 1, levels, levels + 2))

    def deep(s, n):
        return deep_in[s, n * high : (n + 1) * high].reshape(rows, cols)

    def kept_rows(s, places):
        plane = zero
        for n, r in places:
            plane = jnp.where(row == r, deep_in[s, 4 * high, n : n + 1, :], plane)
        return plane

    def across(c, x):
        above = jnp.where((row == 0) & (c > 0.0), down(x)[:rows], 0.0)
        below = jnp.where((row == rows - 1) & (c <= 0.0), up_row(x)[:rows], 0.0)
        return jnp.abs(c) * (above + below)

    def step(v, l, rule=forward):
        return rule(v[l], speeds[l], [v[l - 1], down(v[l]), right(v[l])], [v[l + 1], up_row(v[l]), left(v[l])])

    outside = []
    for s, (l, _, far) in enumerate(beside):
        c = [
            deep(s, 3),
            kept_rows(s, ((0, 0), (1, 1), (2, rows - 2), (3, rows - 1))),
            kept_rows(s, ((4, 0), (5, rows - 1))),
        ]
        start[l] = jnp.concatenate([deep(s, 0), halo[s, 1, 0]], axis=0)
        start[far] = jnp.concatenate([zero, halo[s, 2, 0]], axis=0)
        speeds[l] = [jnp.concatenate([c[k], halo[s, 1, k + 1]], axis=0) for k in range(3)]
        gained = across(c[1], start[l])
        further = across(kept_rows(s, ((6, 0), (7, rows - 1))), start[far])
        outside.append((c, gained, further))
    v = {l: step(start, l) for l in (-1, levels)}
    for l in range(levels):
        v[l] = begun[l] if 0 < l < levels - 1 else begun[l] + lev_term(start, l)
    for s, (l, _, _) in enumerate(beside):
        v[l] = jnp.concatenate([deep(s, 1) + outside[s][1], step(start, l)[rows:]], axis=0)
    second_v = {l: step(v, l, again) for l in range(-1, levels + 1)}
    for s, (l, by, _) in enumerate(beside):
        c, gained, further = outside[s]
        sizes = [jnp.abs(n) for n in c]
        inward, outward = v[by][:rows], further
        crossed = jnp.concatenate([gained, v[l][rows:]], axis=0)
        total = deep(s, 2) + (1.0 - sizes[0] - sizes[1] - sizes[2]) * gained
        total = total + sizes[0] * jnp.where(c[0] > 0.0, inward if s else outward, outward if s else inward)
        total = total + sizes[1] * jnp.where(c[1] > 0.0, down(crossed)[:rows], up_row(crossed)[:rows])
        total = total + sizes[2] * jnp.where(
            c[2] > 0.0, pltpu.roll(gained, 1, axis=1), pltpu.roll(gained, cols - 1, axis=1)
        )
        second_v[l] = jnp.concatenate([total, blank], axis=0)
        speeds[l] = [jnp.concatenate([c[0], blank], axis=0)]
    v = second_v
    rim = (lanes < 2) | (lanes >= cols - 2)
    v = {l: jnp.where(rim, fix_v[l], v[l]) for l in v}
    for l in range(levels):
        state_v[l] = v[l][:rows]

    def seen_cell(l, i):
        g = l + beyond
        if 0 < g < span - 1:
            return joined(seen[g, i], seen_in[0, g - 1, i], seen_in[1, g - 1, i])
        return jnp.concatenate([seen[g, i], blank], axis=0)

    p = {l: seen_cell(l, 0) * v[l] - seen_cell(l, 1) for l in v}
    low, up = {}, {}
    for l in p:
        low[l], up[l] = shares(p[l], speeds[l])
    rim = (lanes < 1) | (lanes >= cols - 1)
    q = {}
    for l in range(-1, levels + 1):
        total = centre_of(speeds[l]) * p[l] + low[l + 1][0] + up[l - 1][0]
        total = total + up_row(low[l][1]) + down(up[l][1]) + left(low[l][2]) + right(up[l][2])
        q[l] = jnp.where(rim, fix_q[l], total)
    for l in q:
        low[l], up[l] = shares(q[l], speeds[l])
    for l in range(levels):
        total = centre_of(speeds[l]) * q[l] + low[l + 1][0] + up[l - 1][0]
        total = total + up_row(low[l][1]) + down(up[l][1])
        total = total + jnp.where(rim, crossing[l], 0.0)
        total = total + jnp.where(lanes >= cols - 1, 0.0, left(low[l][2])) + jnp.where(lanes < 1, 0.0, right(up[l][2]))
        adj_v[l] = total[:rows]


def finish(state_v, adj_v, outer, state_hbm, adj_hbm, next_hbm, wide, nxt, out_sem):
    levels, rows, cols = state_v.shape
    flat_rows = levels * rows
    wide_cols = outer.shape[1]
    fine = wide_cols // cols
    outer_rows = outer.shape[0] // levels
    stores = [
        pltpu.make_async_copy(state_v, state_hbm, out_sem.at[0]),
        pltpu.make_async_copy(adj_v, adj_hbm, out_sem.at[1]),
    ]
    for store in stores:
        store.start()
    field = adj_v[...]

    table = (
        lax.broadcasted_iota(jnp.int32, (cols, wide_cols), 0)
        == lax.broadcasted_iota(jnp.int32, (cols, wide_cols), 1) // fine
    ).astype(jnp.float32).astype(jnp.bfloat16)
    halves = bf16_parts(field.reshape(flat_rows, cols), 2)
    spread = jnp.dot(
        jnp.concatenate([h.astype(jnp.bfloat16) for h in halves], axis=1),
        jnp.concatenate([table, table], axis=0),
        preferred_element_type=jnp.float32,
    )
    for k in range(fine):
        for c in range(fine):
            wide[c, pl.ds(k, flat_rows, stride=fine), :] = spread[:, c * cols : (c + 1) * cols]
    for level in range(levels):
        span = pl.ds(level * outer_rows, outer_rows)
        for c in range(fine):
            lanes = pl.ds(c * cols, cols)
            nxt[span, lanes] = (outer[span, lanes].astype(jnp.float32) - wide[c, span, :]).astype(jnp.bfloat16)
        store = pltpu.make_async_copy(nxt.at[span], next_hbm.at[span], out_sem.at[2 + level])
        store.start()
        stores.append(store)
    for store in stores:
        store.wait()


def shards(ends, outer_increment, courant, obs_column, obs_level, obs_value):
    levels, outer_rows, wide_cols = outer_increment.shape
    _, _, rows, cols = courant.shape
    flat_rows = levels * rows
    fine = wide_cols // cols
    lanes = 128
    observed = (obs_column.shape[0] // lanes, lanes)
    span = levels + 4
    assert 4 * levels * GROUP == cols and levels >= REACH and rows % TILE == 0 and ends[1] > 1
    f32, bf16 = jnp.float32, jnp.bfloat16
    outer_shape = (levels * outer_rows, wide_cols)
    vmem = pl.BlockSpec(memory_space=pltpu.VMEM)
    hbm = pl.BlockSpec(memory_space=pl.ANY)
    held = pl.pallas_call(
        functools.partial(kernel, ends),
        out_shape=(
            pltpu.VMEM((levels, rows, cols), f32),
            pltpu.VMEM((levels, rows, cols), f32),
            pltpu.VMEM(outer_shape, bf16),
        ),
        in_specs=[hbm] * 5,
        out_specs=(vmem,) * 3,
        scratch_shapes=[
            pltpu.VMEM(courant.shape, bf16),
            pltpu.VMEM(observed, jnp.int32),
            pltpu.VMEM(observed, jnp.int32),
            pltpu.VMEM(observed, f32),
            pltpu.VMEM((levels * outer_rows, cols), f32),
            pltpu.VMEM((levels, 4, rows, cols), f32),
            pltpu.VMEM((2, 4, rows, cols), f32),
            pltpu.VMEM((2, 4 * rows // TILE + 1, TILE, cols), f32),
            pltpu.VMEM((2, 4 * rows // TILE + 1, TILE, cols), f32),
            pltpu.VMEM((2, levels, 4, TILE, cols), f32),
            pltpu.VMEM((2, 2, 2 * TILE, cols), f32),
            pltpu.VMEM((2, 2, 2 * TILE, cols), f32),
            pltpu.VMEM((2, REACH - 1, 4, TILE, cols), f32),
            pltpu.VMEM((rows, cols), f32),
            pltpu.VMEM((3, 3, rows, cols), f32),
            pltpu.VMEM((3, 2, 3, TILE, cols), f32),
            pltpu.VMEM((span, 2, rows, cols), f32),
            pltpu.VMEM((2, span - 2, 2, TILE, cols), f32),
            pltpu.VMEM((2, rows, cols), f32),
            pltpu.VMEM((2, 2, rows, cols), f32),
            pltpu.VMEM((2, 3, 2, TILE, cols), f32),
            pltpu.VMEM((2048, 1, cols), f32),
            pltpu.SemaphoreType.DMA((3,)),
            pltpu.SemaphoreType.DMA,
            pltpu.SemaphoreType.DMA((2,)),
            pltpu.SemaphoreType.REGULAR((5,)),
        ],
        compiler_params=pltpu.CompilerParams(collective_id=0, has_side_effects=True),
    )(
        outer_increment.reshape(outer_shape),
        courant,
        obs_column.reshape(observed),
        obs_level.reshape(observed),
        obs_value.reshape(observed),
    )
    state, adjoint, following = pl.pallas_call(
        finish,
        out_shape=(
            jax.ShapeDtypeStruct((levels, rows, cols), f32),
            jax.ShapeDtypeStruct((levels, rows, cols), f32),
            jax.ShapeDtypeStruct(outer_shape, bf16),
        ),
        in_specs=[vmem] * 3,
        out_specs=(hbm,) * 3,
        scratch_shapes=[
            pltpu.VMEM((fine, levels * outer_rows, cols), f32),
            pltpu.VMEM(outer_shape, bf16),
            pltpu.SemaphoreType.DMA((2 + levels,)),
        ],
    )(*[pltpu.with_memory_space_constraint(x, pltpu.VMEM) for x in held])
    return state, adjoint, following.reshape(outer_increment.shape)


def solution(mesh):
    ends = tuple(mesh.shape[a] for a in ("lat", "lon", "lev"))
    block = P("lev", "lat", "lon")
    observed = P(("lat", "lon"))
    return jax.shard_map(
        functools.partial(shards, ends),
        mesh=mesh,
        in_specs=(block, P(None, "lev", "lat", "lon"), observed, observed, observed),
        out_specs=(block, block, block),
        check_vma=False,
    )
```

```python
import functools

import jax
import jax.numpy as jnp
from jax import lax
from jax.experimental import pallas as pl
from jax.experimental.pallas import tpu as pltpu
from jax.sharding import PartitionSpec as P

MESH = pl.DeviceIdType.MESH
REACH = 4
GROUP = 2 * REACH
TILE = 8


def bf16_parts(x, count):
    parts = []
    for _ in range(count):
        part = x.astype(jnp.bfloat16).astype(jnp.float32)
        parts.append(part)
        x = x - part
    return parts


def forward(v, c, minus, plus):
    sizes = [jnp.abs(n) for n in c]
    result = (1.0 - sizes[0] - sizes[1] - sizes[2]) * v
    for k in range(3):
        result = result + sizes[k] * jnp.where(c[k] > 0.0, minus[k], plus[k])
    return result


def again(v, c, minus, plus):
    result = centre_of(c) * v
    for k in range(3):
        low = jnp.maximum(c[k], 0.0)
        result = result + low * minus[k] + (low - c[k]) * plus[k]
    return result


def shares(p, c):
    low, up = [], []
    for n in c:
        low.append(jnp.maximum(n, 0.0) * p)
        up.append(low[-1] - n * p)
    return low, up


def centre_of(c):
    return 1.0 - jnp.abs(c[0]) - jnp.abs(c[1]) - jnp.abs(c[2])


def kernel(
    ends, outer_hbm, courant_hbm, col_hbm, lvl_hbm, val_hbm,
    state_v, adj_v, outer,
    courant, col, lvl, val, sums,
    own, face_in, deep_out, deep_in, side_in, edge_out, edge_in, halo,
    strip, strip_full, strip_half,
    seen, seen_in, seen_strip, seen_full, seen_half, units,
    in_sem, send_sem, recv_sem, ready,
):
    n_lat, n_lon, n_lev = ends
    levels, rows, cols = state_v.shape
    flat_rows = levels * rows
    wide_cols = outer.shape[1]
    fine = wide_cols // cols
    near = REACH - 1
    span = seen.shape[0]
    beyond = (span - levels) // 2

    loads = [
        pltpu.make_async_copy(src, dst, in_sem.at[min(i, 2)])
        for i, (src, dst) in enumerate(
            ((outer_hbm, outer), (courant_hbm, courant), (col_hbm, col), (lvl_hbm, lvl), (val_hbm, val))
        )
    ]
    for load in loads:
        load.start()

    me_lat, me_lon, me_lev = (lax.axis_index(a) for a in ("lat", "lon", "lev"))
    links = (
        ("lev", me_lev + 1, me_lev < n_lev - 1),
        ("lev", me_lev - 1, me_lev > 0),
        ("lat", me_lat + 1, me_lat < n_lat - 1),
        ("lat", me_lat - 1, me_lat > 0),
        ("lon", lax.rem(me_lon + 1, n_lon), None),
        ("lon", lax.rem(me_lon + n_lon - 1, n_lon), None),
    )
    turns = (0, 1) if n_lon > 2 else (0,)
    bands = ((rows - TILE, TILE), (0, TILE))

    def both(flags):
        return functools.reduce(jnp.logical_and, flags) if flags else None

    def guarded(exists, action):
        if exists is None:
            action()
        else:
            pl.when(exists)(action)

    def flags_of(which):
        return [links[w][2] for w in which if w < 4]

    def lon_of(which):
        return [w for w in which if w > 3]

    def is_ahead(which):
        return me_lon < links[lon_of(which)[0]][1]

    def is_behind(which):
        return me_lon > links[lon_of(which)[0]][1]

    class Message:
        def __init__(self, which, source, landing, sem, later=0):
            self.which, self.later = which, later
            self.needs = tuple(w for w in which if w < 4)
            self.target = {links[w][0]: links[w][1] for w in which}
            self.arrives = both([links[w ^ 1][2] for w in self.needs])
            self.source, self.landing, self.sem = source, landing, sem

        def start(self, flag=None):
            def begin():
                pltpu.make_async_remote_copy(
                    src_ref=self.source, dst_ref=self.landing, send_sem=send_sem, recv_sem=recv_sem.at[self.sem],
                    device_id=self.target, device_id_type=MESH,
                ).start()

            guarded(both(flags_of(self.which) + ([] if flag is None else [flag])), begin)

        def lines(self):
            total = 1
            for n in self.landing.shape:
                total = total * n
            return total // cols

    partners, first, second, faces = [], [], [], []
    for a in (2, 1, 0):
        for t in (0, 1, None):
            for u in turns + (None,):
                which = [a - 1] if a else []
                which = which + ([2 + t] if t is not None else []) + ([4 + u] if u is not None else [])
                if not which:
                    continue
                partners.append(which)
                b = 0 if u is None else u + 1
                if t is None:
                    first.append(Message(which, strip, strip_full.at[a, b], 0))
                else:
                    first.append(Message(which, strip.at[pl.ds(*bands[t])], strip_half.at[a, t, b], 0))
                if u is None:
                    if a and t is None:
                        faces.append(Message(which, own.at[levels - 1 if a == 1 else 0], face_in.at[a - 1], 1))
                        faces.append(Message(which, deep_out.at[a - 1], deep_in.at[a - 1], 1, 2))
                    elif a:
                        first.append(Message(which, edge_out.at[a - 1, t], edge_in.at[a - 1, t], 0))
                    else:
                        first.append(Message(which, own.at[:, :, pl.ds(*bands[t])], side_in.at[t], 0))
                if not a:
                    if t is None:
                        second.append(Message(which, seen_strip, seen_full.at[u], 1))
                    else:
                        second.append(Message(which, seen_strip.at[:, pl.ds(*bands[t])], seen_half.at[t, b], 1))
                    if u is None:
                        kept = pl.ds(1, span - 2)
                        second.append(Message(which, seen.at[kept, :, pl.ds(*bands[t])], seen_in.at[t], 1))
    first.sort(key=lambda m: m.lines() - 1024 * len(m.target))

    def pick(test, side=None):
        return [(which, None if side is None else side(which)) for which in partners if test(which)]

    def count(chosen):
        total = 0
        for which, flag in chosen:
            exists = both(flags_of(which) + ([] if flag is None else [flag]))
            total = total + (1 if exists is None else exists.astype(jnp.int32))
        return total

    def signal(sem, chosen):
        for which, flag in chosen:
            target = {links[w][0]: links[w][1] for w in which}
            guarded(
                both(flags_of(which) + ([] if flag is None else [flag])),
                lambda target=target: pl.semaphore_signal(sem, inc=1, device_id=target, device_id_type=MESH),
            )

    def level_lon(which):
        return lon_of(which) and not {0, 1} & set(which)

    def corner(which):
        return len(which) == 3

    lower = pick(lambda w: 1 in w and not corner(w))
    upper = pick(lambda w: 0 in w and not corner(w))
    lower_face, upper_face = [[c for c in side if len(c[0]) == 1] for side in (lower, upper)]
    lower_rest, upper_rest = [[c for c in side if len(c[0]) > 1] for side in (lower, upper)]
    lower_south = pick(lambda w: corner(w) and 1 in w and 3 in w)
    upper_north = pick(lambda w: corner(w) and 0 in w and 2 in w)
    lower_north = pick(lambda w: corner(w) and 1 in w and 2 in w, is_behind)
    upper_south = pick(lambda w: corner(w) and 0 in w and 3 in w, is_ahead)
    south, north = pick(lambda w: w == [3]), pick(lambda w: w == [2])
    behind, ahead = pick(level_lon, is_behind), pick(level_lon, is_ahead)

    barrier = pltpu.get_barrier_semaphore()
    signal(barrier, upper_rest[::-1] + upper_north + upper_face + ahead + upper_south + north)

    def settle(messages, flip, sem, known=()):
        if len(known) < 4:
            for has in (True, False):
                flag = links[len(known)][2]
                pl.when(flag if has else jnp.logical_not(flag))(
                    lambda has=has: settle(messages, flip, sem, known + (has,))
                )
            return
        total = sum(m.lines() for m in messages if all(known[w ^ flip] for w in m.needs))
        view = units.at[pl.ds(0, total)]
        pltpu.make_async_copy(view, view, sem).wait()

    def clear(ref):
        ref[...] = jnp.zeros(ref.shape, jnp.float32)

    for m in first + second + faces:
        if m.arrives is not None:
            pl.when(jnp.logical_not(m.arrives))(lambda m=m: clear(m.landing))
    clear(halo)

    lane = lax.broadcasted_iota(jnp.int32, (rows, cols), 1)
    group = lane // GROUP
    pool = (
        lax.broadcasted_iota(jnp.int32, (wide_cols, cols), 0) // fine
        == lax.broadcasted_iota(jnp.int32, (wide_cols, cols), 1)
    ).astype(jnp.float32).astype(jnp.bfloat16)

    loads[1].wait()
    for k in range(3):
        own[:, k + 1] = courant[k].astype(jnp.float32)
    loads[0].wait()
    sums[...] = jnp.dot(outer[...], pool, preferred_element_type=jnp.float32)
    coarse = sums[pl.ds(0, flat_rows, stride=fine), :]
    for k in range(1, fine):
        coarse = coarse + sums[pl.ds(k, flat_rows, stride=fine), :]
    own[:, 0] = (coarse * (1.0 / (fine * fine))).reshape(levels, rows, cols)

    ends_only = jnp.zeros((rows, cols), jnp.float32)
    for f in (1, 2, 3, 0):
        for l in range(levels):
            place = f * levels + l
            ends_only = jnp.where(group == place, pltpu.roll(own[l, f], (REACH + GROUP * place) % cols, axis=1), ends_only)
    strip[...] = ends_only

    entries = [(0, i, j) for i in range(1, REACH) for j in range(1, REACH + 1 - i)]
    entries = entries + [(f, i, j) for f in (1, 2, 3) for i in range(1, near) for j in range(1, near + 1 - i)]
    for s in range(2):
        for t in range(2):
            for n, (f, i, j) in enumerate(entries):
                l = levels - i if s == 0 else i - 1
                r = rows - j if t == 0 else j - 1
                edge_out[s, t, n : n + 1, :] = own[l, f, r : r + 1, :]

    def send(messages, test, side=None, later=0):
        for m in messages:
            if test(m.which) and m.later == later:
                m.start(None if side is None else side(m.which))

    def at_once(w):
        return (1 in w and not (corner(w) and 2 in w)) or w == [3]

    def north_corner(w):
        return corner(w) and 1 in w and 2 in w

    expected = count(lower + lower_south + lower_north + south + behind)
    pl.when(expected > 0)(lambda: pl.semaphore_wait(barrier, expected))
    signal(ready.at[4], [(w, is_behind(w)) for w, _ in lower_south])
    signal(ready.at[3], lower_rest)
    signal(ready.at[0], behind)
    signal(ready.at[2], lower_face)
    signal(ready.at[1], south)
    send(first, north_corner, is_behind)
    send(first, level_lon, is_behind)
    send(first, at_once)
    send(faces, at_once)

    row = lax.broadcasted_iota(jnp.int32, (rows, cols), 0)
    high = rows // TILE
    zero = jnp.zeros((rows, cols), jnp.float32)

    def inner(v, c, before, after):
        above = jnp.where(row == 0, 0.0, pltpu.roll(v, 1, axis=0))
        below = jnp.where(row == rows - 1, 0.0, pltpu.roll(v, rows - 1, axis=0))
        return forward(v, c, [before, above, pltpu.roll(v, 1, axis=1)], [after, below, pltpu.roll(v, cols - 1, axis=1)])

    def rim_rows(second_level, third_level):
        kept = [(second_level, 2, r) for r in (0, 1, rows - 2, rows - 1)]
        return kept + [(second_level, 3, r) for r in (0, rows - 1)] + [(third_level, 2, r) for r in (0, rows - 1)]

    view = units.at[pl.ds(0, 3 * col.shape[0])]
    pltpu.make_async_copy(view, view, in_sem.at[2]).wait()
    where_row = (lvl[...] - me_lev * levels + beyond) * rows + col[...] // cols
    where_col = col[...] % cols
    parts = bf16_parts(val[...], 2)
    pieces, width = col.shape
    row_id = lax.broadcasted_iota(jnp.int32, (span * rows, width), 0)
    col_id = lax.broadcasted_iota(jnp.int32, (cols, width), 0)
    hits = [[] for _ in range(3)]
    tables = []
    for k in range(pieces):
        match = where_row[k : k + 1] == row_id
        hits[0].append(jnp.where(match, 1.0, 0.0).astype(jnp.bfloat16))
        for i, part in enumerate(parts):
            hits[i + 1].append(jnp.where(match, part[k : k + 1], 0.0).astype(jnp.bfloat16))
        tables.append(jnp.where(where_col[k : k + 1] == col_id, 1.0, 0.0).astype(jnp.bfloat16))
    left_side = jnp.concatenate([jnp.concatenate(h, axis=1) for h in hits], axis=0)
    totals = lax.dot_general(
        left_side, jnp.concatenate(tables, axis=1), (((1,), (1,)), ((), ())),
        preferred_element_type=jnp.float32,
    )
    wide_rows = span * rows
    counted = totals[:wide_rows].reshape(span, rows, cols)
    summed = (totals[wide_rows : 2 * wide_rows] + totals[2 * wide_rows :]).reshape(span, rows, cols)
    seen[:, 0] = counted
    seen[:, 1] = summed
    for i, values in enumerate((counted, summed)):
        ends_only = jnp.zeros((rows, cols), jnp.float32)
        for g in range(span):
            place = g + REACH - beyond
            ends_only = jnp.where(group == place, pltpu.roll(values[g], (REACH + GROUP * place) % cols, axis=1), ends_only)
        seen_strip[i] = ends_only
    send(second, level_lon, is_behind)
    send(second, at_once)

    pairs = ((levels - 2, levels - 3), (1, 2))
    once = {
        l: inner(own[l, 0], [own[l, k + 1] for k in range(3)], own[l - 1, 0], own[l + 1, 0])
        for l in sorted(set(pairs[0] + pairs[1]))
    }
    for s, (l, far) in enumerate(pairs):
        c = [own[l, k + 1] for k in range(3)]
        twice = inner(once[l], c, zero if s else once[far], once[far] if s else zero)
        for n, plane in enumerate((own[l, 0], once[l], twice, c[0])):
            deep_out[s, n * high : (n + 1) * high] = plane.reshape(high, TILE, cols)
        for n, (at, f, r) in enumerate(rim_rows(l, far)):
            deep_out[s, 4 * high, n : n + 1, :] = own[at, f, r : r + 1, :]

    send(faces, at_once, later=2)

    @pl.when(links[2][2])
    def _():
        pl.semaphore_wait(ready.at[1], 1)
        send(first, north_corner, is_ahead)
        send(first + second, lambda w: w == [2])

    @pl.when(me_lon < n_lon - 1)
    def _():
        pl.semaphore_wait(ready.at[0], count(ahead))
        send(first + second, level_lon, is_ahead)

    @pl.when(links[0][2])
    def _():
        pl.semaphore_wait(ready.at[2], 1)
        send(faces, lambda w: 0 in w)
        pl.semaphore_wait(ready.at[3], count(upper_rest))
        send(first, lambda w: 0 in w and not (corner(w) and 2 in w))
        send(first, lambda w: corner(w) and 0 in w and 2 in w, is_behind)

    @pl.when(links[0][2] & links[2][2] & (me_lon < n_lon - 1))
    def _():
        pl.semaphore_wait(ready.at[4], count([(w, is_ahead(w)) for w, _ in upper_north]))
        send(first, lambda w: corner(w) and 0 in w and 2 in w, is_ahead)

    pl.when(links[0][2])(lambda: send(faces, lambda w: 0 in w, later=2))

    settle(first, 1, recv_sem.at[0])

    tall = rows + TILE
    half = lax.broadcasted_iota(jnp.int32, (TILE, cols), 0) < TILE // 2
    lanes = lax.broadcasted_iota(jnp.int32, (tall, cols), 1)
    slot = lanes % GROUP
    left_half = slot < REACH
    blank = jnp.zeros((TILE, cols), jnp.float32)

    def joined(full, before, after):
        return jnp.concatenate([full, jnp.where(half, after, before)], axis=0)

    for s in range(2):
        for t in range(2):
            for n, (f, i, j) in enumerate(entries):
                r = TILE - j if t == 0 else j - 1
                halo[s, i - 1, f, r : r + 1, :] = edge_in[s, t, n : n + 1, :]

    def cell(l, f):
        if 0 <= l < levels:
            return joined(own[l, f], side_in[0, l, f], side_in[1, l, f])
        s, i = (0, -l) if l < 0 else (1, l - levels + 1)
        return jnp.concatenate([face_in[s, f], halo[s, i - 1, f]], axis=0)

    def down(x):
        return pltpu.roll(x, 1, axis=0)

    def up_row(x):
        return pltpu.roll(x, tall - 1, axis=0)

    def right(x, by=1):
        return pltpu.roll(x, by, axis=1)

    def left(x, by=1):
        return pltpu.roll(x, cols - by, axis=1)

    before_b, after_b = 1, (2 if n_lon > 2 else 1)

    def strip_block(a, b):
        full = strip[...] if a == 0 and b == 0 else strip_full[a, b]
        return joined(full, strip_half[a, 0, b], strip_half[a, 1, b])

    def placed(blocks, f):
        turned = [right(blocks[a], (GROUP * levels * (n - f)) % cols) if n != f else blocks[a] for n, a in enumerate((1, 0, 2))]
        width = GROUP * levels
        return jnp.where(lanes < width, turned[0], jnp.where(lanes < 2 * width, turned[1], turned[2]))

    mine = [strip_block(a, 0) for a in range(3)]
    sides = []
    sides.append([jnp.where(left_half, strip_block(a, before_b), mine[a]) for a in range(3)])
    sides.append([jnp.where(left_half, mine[a], strip_block(a, after_b)) for a in range(3)])
    side_c, side_v = [], []
    for blocks in sides:
        c = [placed(blocks, k + 1) for k in range(3)]
        v = placed(blocks, 0)
        for _ in range(2):
            v = forward(v, c, [right(v, GROUP), down(v), right(v)], [left(v, GROUP), up_row(v), left(v)])
        side_c.append(c)
        side_v.append(v)

    def inserted(z, l):
        return right(z, (cols - REACH - GROUP * (l + REACH)) % cols)

    def seen_block(b, i):
        full = seen_strip[i] if b == 0 else seen_full[b - 1, i]
        return joined(full, seen_half[0, b, i], seen_half[1, b, i])

    speeds = {l: [cell(l, k + 1) for k in range(3)] for l in range(levels)}
    start = {l: cell(l, 0) for l in range(levels)}

    def lev_term(v, l):
        n = speeds[l][0]
        return jnp.abs(n) * jnp.where(n > 0.0, v[l - 1], v[l + 1])

    def within(v, l):
        result = centre_of(speeds[l]) * v[l]
        for n, minus, plus in zip(speeds[l][1:], (down(v[l]), right(v[l])), (up_row(v[l]), left(v[l]))):
            result = result + jnp.abs(n) * jnp.where(n > 0.0, minus, plus)
        return result

    begun = {l: within(start, l) for l in range(levels)}
    begun = {l: begun[l] + lev_term(start, l) if 0 < l < levels - 1 else begun[l] for l in begun}

    settle(first + second + faces, 0, send_sem)
    settle(second + faces, 1, recv_sem.at[1])
    side_q = []
    for side in range(2):
        known = []
        for i in range(2):
            if side == 0:
                known.append(jnp.where(left_half, seen_block(before_b, i), seen_block(0, i)))
            else:
                known.append(jnp.where(left_half, seen_block(0, i), seen_block(after_b, i)))
        p = known[0] * side_v[side] - known[1]
        c = side_c[side]
        low, up = shares(p, c)
        q = centre_of(c) * p + left(low[0], GROUP) + right(up[0], GROUP)
        q = q + up_row(low[1]) + down(up[1]) + left(low[2]) + right(up[2])
        low, up = shares(q, c)
        side_q.append((q, right(up[2]) if side == 0 else left(low[2])))
    fix = jnp.where(left_half, side_q[1][0], side_q[0][0])
    crossing = jnp.where(left_half, side_q[1][1], side_q[0][1])

    fix_v = jnp.where(left_half, side_v[1], side_v[0])
    fix_v = {l: inserted(fix_v, l) for l in range(2 - near - 1, levels + near - 1)}
    fix_q = {l: inserted(fix, l) for l in range(-1, levels + 1)}
    crossing = {l: inserted(crossing, l) for l in range(levels)}

    for l in (-1, levels):
        speeds[l] = [cell(l, k + 1) for k in range(3)]
        start[l] = cell(l, 0)
    beside = ((-2, -1, -3), (levels + 1, levels, levels + 2))

    def deep(s, n):
        return deep_in[s, n * high : (n + 1) * high].reshape(rows, cols)

    def kept_rows(s, places):
        plane = zero
        for n, r in places:
            plane = jnp.where(row == r, deep_in[s, 4 * high, n : n + 1, :], plane)
        return plane

    def across(c, x):
        above = jnp.where((row == 0) & (c > 0.0), down(x)[:rows], 0.0)
        below = jnp.where((row == rows - 1) & (c <= 0.0), up_row(x)[:rows], 0.0)
        return jnp.abs(c) * (above + below)

    def step(v, l, rule=forward):
        return rule(v[l], speeds[l], [v[l - 1], down(v[l]), right(v[l])], [v[l + 1], up_row(v[l]), left(v[l])])

    outside = []
    for s, (l, _, far) in enumerate(beside):
        c = [
            deep(s, 3),
            kept_rows(s, ((0, 0), (1, 1), (2, rows - 2), (3, rows - 1))),
            kept_rows(s, ((4, 0), (5, rows - 1))),
        ]
        start[l] = jnp.concatenate([deep(s, 0), halo[s, 1, 0]], axis=0)
        start[far] = jnp.concatenate([zero, halo[s, 2, 0]], axis=0)
        speeds[l] = [jnp.concatenate([c[k], halo[s, 1, k + 1]], axis=0) for k in range(3)]
        gained = across(c[1], start[l])
        further = across(kept_rows(s, ((6, 0), (7, rows - 1))), start[far])
        outside.append((c, gained, further))
    v = {l: step(start, l) for l in (-1, levels)}
    for l in range(levels):
        v[l] = begun[l] if 0 < l < levels - 1 else begun[l] + lev_term(start, l)
    for s, (l, _, _) in enumerate(beside):
        v[l] = jnp.concatenate([deep(s, 1) + outside[s][1], step(start, l)[rows:]], axis=0)
    second_v = {l: step(v, l, again) for l in range(-1, levels + 1)}
    for s, (l, by, _) in enumerate(beside):
        c, gained, further = outside[s]
        sizes = [jnp.abs(n) for n in c]
        inward, outward = v[by][:rows], further
        crossed = jnp.concatenate([gained, v[l][rows:]], axis=0)
        total = deep(s, 2) + (1.0 - sizes[0] - sizes[1] - sizes[2]) * gained
        total = total + sizes[0] * jnp.where(c[0] > 0.0, inward if s else outward, outward if s else inward)
        total = total + sizes[1] * jnp.where(c[1] > 0.0, down(crossed)[:rows], up_row(crossed)[:rows])
        total = total + sizes[2] * jnp.where(
            c[2] > 0.0, pltpu.roll(gained, 1, axis=1), pltpu.roll(gained, cols - 1, axis=1)
        )
        second_v[l] = jnp.concatenate([total, blank], axis=0)
        speeds[l] = [jnp.concatenate([c[0], blank], axis=0)]
    v = second_v
    rim = (lanes < 2) | (lanes >= cols - 2)
    v = {l: jnp.where(rim, fix_v[l], v[l]) for l in v}
    for l in range(levels):
        state_v[l] = v[l][:rows]

    def seen_cell(l, i):
        g = l + beyond
        if 0 < g < span - 1:
            return joined(seen[g, i], seen_in[0, g - 1, i], seen_in[1, g - 1, i])
        return jnp.concatenate([seen[g, i], blank], axis=0)

    p = {l: seen_cell(l, 0) * v[l] - seen_cell(l, 1) for l in v}
    low, up = {}, {}
    for l in p:
        low[l], up[l] = shares(p[l], speeds[l])
    rim = (lanes < 1) | (lanes >= cols - 1)
    q = {}
    for l in range(-1, levels + 1):
        total = centre_of(speeds[l]) * p[l] + low[l + 1][0] + up[l - 1][0]
        total = total + up_row(low[l][1]) + down(up[l][1]) + left(low[l][2]) + right(up[l][2])
        q[l] = jnp.where(rim, fix_q[l], total)
    for l in q:
        low[l], up[l] = shares(q[l], speeds[l])
    for l in range(levels):
        total = centre_of(speeds[l]) * q[l] + low[l + 1][0] + up[l - 1][0]
        total = total + up_row(low[l][1]) + down(up[l][1])
        total = total + jnp.where(rim, crossing[l], 0.0)
        total = total + jnp.where(lanes >= cols - 1, 0.0, left(low[l][2])) + jnp.where(lanes < 1, 0.0, right(up[l][2]))
        adj_v[l] = total[:rows]


def finish(state_v, adj_v, outer, state_hbm, adj_hbm, next_hbm, wide, nxt, out_sem):
    levels, rows, cols = state_v.shape
    flat_rows = levels * rows
    wide_cols = outer.shape[1]
    fine = wide_cols // cols
    outer_rows = outer.shape[0] // levels
    stores = [
        pltpu.make_async_copy(state_v, state_hbm, out_sem.at[0]),
        pltpu.make_async_copy(adj_v, adj_hbm, out_sem.at[1]),
    ]
    for store in stores:
        store.start()
    field = adj_v[...]

    table = (
        lax.broadcasted_iota(jnp.int32, (cols, wide_cols), 0)
        == lax.broadcasted_iota(jnp.int32, (cols, wide_cols), 1) // fine
    ).astype(jnp.float32).astype(jnp.bfloat16)
    halves = bf16_parts(field.reshape(flat_rows, cols), 2)
    spread = jnp.dot(
        jnp.concatenate([h.astype(jnp.bfloat16) for h in halves], axis=1),
        jnp.concatenate([table, table], axis=0),
        preferred_element_type=jnp.float32,
    )
    for k in range(fine):
        for c in range(fine):
            wide[c, pl.ds(k, flat_rows, stride=fine), :] = spread[:, c * cols : (c + 1) * cols]
    for level in range(levels):
        span = pl.ds(level * outer_rows, outer_rows)
        for c in range(fine):
            lanes = pl.ds(c * cols, cols)
            nxt[span, lanes] = (outer[span, lanes].astype(jnp.float32) - wide[c, span, :]).astype(jnp.bfloat16)
        store = pltpu.make_async_copy(nxt.at[span], next_hbm.at[span], out_sem.at[2 + level])
        store.start()
        stores.append(store)
    for store in stores:
        store.wait()


def shards(ends, outer_increment, courant, obs_column, obs_level, obs_value):
    levels, outer_rows, wide_cols = outer_increment.shape
    _, _, rows, cols = courant.shape
    flat_rows = levels * rows
    fine = wide_cols // cols
    lanes = 128
    observed = (obs_column.shape[0] // lanes, lanes)
    span = levels + 4
    assert 4 * levels * GROUP == cols and levels >= REACH and rows % TILE == 0 and ends[1] > 1
    f32, bf16 = jnp.float32, jnp.bfloat16
    outer_shape = (levels * outer_rows, wide_cols)
    vmem = pl.BlockSpec(memory_space=pltpu.VMEM)
    hbm = pl.BlockSpec(memory_space=pl.ANY)
    held = pl.pallas_call(
        functools.partial(kernel, ends),
        out_shape=(
            pltpu.VMEM((levels, rows, cols), f32),
            pltpu.VMEM((levels, rows, cols), f32),
            pltpu.VMEM(outer_shape, bf16),
        ),
        in_specs=[hbm] * 5,
        out_specs=(vmem,) * 3,
        scratch_shapes=[
            pltpu.VMEM(courant.shape, bf16),
            pltpu.VMEM(observed, jnp.int32),
            pltpu.VMEM(observed, jnp.int32),
            pltpu.VMEM(observed, f32),
            pltpu.VMEM((levels * outer_rows, cols), f32),
            pltpu.VMEM((levels, 4, rows, cols), f32),
            pltpu.VMEM((2, 4, rows, cols), f32),
            pltpu.VMEM((2, 4 * rows // TILE + 1, TILE, cols), f32),
            pltpu.VMEM((2, 4 * rows // TILE + 1, TILE, cols), f32),
            pltpu.VMEM((2, levels, 4, TILE, cols), f32),
            pltpu.VMEM((2, 2, 2 * TILE, cols), f32),
            pltpu.VMEM((2, 2, 2 * TILE, cols), f32),
            pltpu.VMEM((2, REACH - 1, 4, TILE, cols), f32),
            pltpu.VMEM((rows, cols), f32),
            pltpu.VMEM((3, 3, rows, cols), f32),
            pltpu.VMEM((3, 2, 3, TILE, cols), f32),
            pltpu.VMEM((span, 2, rows, cols), f32),
            pltpu.VMEM((2, span - 2, 2, TILE, cols), f32),
            pltpu.VMEM((2, rows, cols), f32),
            pltpu.VMEM((2, 2, rows, cols), f32),
            pltpu.VMEM((2, 3, 2, TILE, cols), f32),
            pltpu.VMEM((2048, 1, cols), f32),
            pltpu.SemaphoreType.DMA((3,)),
            pltpu.SemaphoreType.DMA,
            pltpu.SemaphoreType.DMA((2,)),
            pltpu.SemaphoreType.REGULAR((5,)),
        ],
        compiler_params=pltpu.CompilerParams(collective_id=0, has_side_effects=True),
    )(
        outer_increment.reshape(outer_shape),
        courant,
        obs_column.reshape(observed),
        obs_level.reshape(observed),
        obs_value.reshape(observed),
    )
    state, adjoint, following = pl.pallas_call(
        finish,
        out_shape=(
            jax.ShapeDtypeStruct((levels, rows, cols), f32),
            jax.ShapeDtypeStruct((levels, rows, cols), f32),
            jax.ShapeDtypeStruct(outer_shape, bf16),
        ),
        in_specs=[vmem] * 3,
        out_specs=(hbm,) * 3,
        scratch_shapes=[
            pltpu.VMEM((fine, levels * outer_rows, cols), f32),
            pltpu.VMEM(outer_shape, bf16),
            pltpu.SemaphoreType.DMA((2 + levels,)),
        ],
    )(*[pltpu.with_memory_space_constraint(x, pltpu.VMEM) for x in held])
    return state, adjoint, following.reshape(outer_increment.shape)


def solution(mesh):
    ends = tuple(mesh.shape[a] for a in ("lat", "lon", "lev"))
    block = P("lev", "lat", "lon")
    observed = P(("lat", "lon"))
    return jax.shard_map(
        functools.partial(shards, ends),
        mesh=mesh,
        in_specs=(block, P(None, "lev", "lat", "lon"), observed, observed, observed),
        out_specs=(block, block, block),
        check_vma=False,
    )
```
